8 devices in a mesh: dp: 1 (over z), tp: 8 (over y, x, core).
Axes of the slice: x: 2, y: 2, z: 1, core: 2. Of those that a mesh axis runs over, the one named last changes fastest.
Arguments:
- hidden_in: bfloat16 [12, 768, 1024], P('dp', 'tp')
- ln1_gain: bfloat16 [1024], replicated
- ln1_bias: bfloat16 [1024], replicated
- w_q: bfloat16 [1024, 1024], P(None, 'tp')
- b_q: bfloat16 [1024], P('tp')
- w_k: bfloat16 [1024, 1024], P(None, 'tp')
- w_v: bfloat16 [1024, 1024], P(None, 'tp')
- b_v: bfloat16 [1024], P('tp')
- w_o: bfloat16 [1024, 1024], P('tp')
- b_o: bfloat16 [1024], replicated
- ln2_gain: bfloat16 [1024], replicated
- ln2_bias: bfloat16 [1024], replicated
- w_fc1: bfloat16 [1024, 4096], P(None, 'tp')
- b_fc1: bfloat16 [4096], P('tp')
- w_fc2: bfloat16 [4096, 1024], P('tp')
- b_fc2: bfloat16 [1024], replicated
- post_gain: bfloat16 [1024], replicated
- post_bias: bfloat16 [1024], replicated
- w_ck: bfloat16 [2, 1024, 1024], P(None, None, 'tp')
- w_cv: bfloat16 [2, 1024, 1024], P(None, None, 'tp')
- b_cv: bfloat16 [2, 1024], P(None, 'tp')
Outputs:
- output 1: bfloat16 [12, 768, 1024], P('dp', 'tp')
- output 2: bfloat16 [2, 12, 768, 16, 64], P(None, 'dp', None, 'tp')
- output 3: bfloat16 [2, 12, 768, 16, 64], P(None, 'dp', None, 'tp')
All inputs are finite; a program needn't handle non-finite values.
Results may differ from the reference program's by a relative error of at most 0.0160126.
Values are sent between devices in bfloat16 or wider.
A program may use at most 1 GiB of HBM per device.

```python
import jax
import jax.numpy as jnp
from jax import lax

BATCH_SIZE = 12
NUM_FRAMES = 768
D_MODEL = 1024
NUM_HEADS = 16
FF_DIM = 4096
NUM_LAYERS = 2

HEAD_DIM = D_MODEL // NUM_HEADS
ATTN_SCALE = HEAD_DIM ** -0.25
LN_EPS = 1e-5


def draw_normal(key, shape, scale, offset=0.0):
    sample = jax.random.normal(key, shape, jnp.float32)
    return (offset + scale * sample).astype(jnp.bfloat16)


def setup_inputs(seed: int = 0, part: int = 0) -> dict:
    keys = jax.random.split(jax.random.key(seed), 20)
    part_key = jax.random.fold_in(jax.random.key(seed + 1), part)
    w_scale = D_MODEL ** -0.5
    ffn_scale = FF_DIM ** -0.5
    return {
        "hidden_in": draw_normal(part_key, (BATCH_SIZE, NUM_FRAMES, D_MODEL), 1.0),
        "ln1_gain": draw_normal(keys[0], (D_MODEL,), 0.2, 1.0),
        "ln1_bias": draw_normal(keys[1], (D_MODEL,), 0.3),
        "w_q": draw_normal(keys[2], (D_MODEL, D_MODEL), 1.3 * w_scale),
        "b_q": draw_normal(keys[3], (D_MODEL,), 0.5),
        "w_k": draw_normal(keys[4], (D_MODEL, D_MODEL), 1.3 * w_scale),
        "w_v": draw_normal(keys[5], (D_MODEL, D_MODEL), w_scale),
        "b_v": draw_normal(keys[6], (D_MODEL,), 0.5),
        "w_o": draw_normal(keys[7], (D_MODEL, D_MODEL), w_scale),
        "b_o": draw_normal(keys[8], (D_MODEL,), 0.3),
        "ln2_gain": draw_normal(keys[9], (D_MODEL,), 0.2, 1.0),
        "ln2_bias": draw_normal(keys[10], (D_MODEL,), 0.3),
        "w_fc1": draw_normal(keys[11], (D_MODEL, FF_DIM), w_scale),
        "b_fc1": draw_normal(keys[12], (FF_DIM,), 0.5),
        "w_fc2": draw_normal(keys[13], (FF_DIM, D_MODEL), 1.5 * ffn_scale),
        "b_fc2": draw_normal(keys[14], (D_MODEL,), 0.3),
        "post_gain": draw_normal(keys[15], (D_MODEL,), 0.2, 1.0),
        "post_bias": draw_normal(keys[16], (D_MODEL,), 0.3),
        "w_ck": draw_normal(keys[17], (NUM_LAYERS, D_MODEL, D_MODEL), w_scale),
        "w_cv": draw_normal(keys[18], (NUM_LAYERS, D_MODEL, D_MODEL), w_scale),
        "b_cv": draw_normal(keys[19], (NUM_LAYERS, D_MODEL), 0.5),
    }


def layer_norm(values, ln_gain, ln_bias):
    centered = values.astype(jnp.float32)
    centered = centered - jnp.mean(centered, axis=-1, keepdims=True)
    row_var = jnp.mean(centered * centered, axis=-1, keepdims=True)
    normed = centered * lax.rsqrt(row_var + LN_EPS)
    return (normed * ln_gain.astype(jnp.float32) + ln_bias.astype(jnp.float32)).astype(jnp.bfloat16)


def split_heads(flat):
    return flat.reshape(BATCH_SIZE, NUM_FRAMES, NUM_HEADS, HEAD_DIM).transpose(0, 2, 1, 3).reshape(BATCH_SIZE * NUM_HEADS, NUM_FRAMES, HEAD_DIM)


def head_attention(triple):
    q_head, k_head, v_head = triple
    scores = jnp.dot(q_head, k_head.T, preferred_element_type=jnp.float32)
    attn_probs = jax.nn.softmax(scores, axis=-1).astype(jnp.bfloat16)
    return jnp.dot(attn_probs, v_head, preferred_element_type=jnp.float32).astype(jnp.bfloat16)


def reference(hidden_in, ln1_gain, ln1_bias, w_q, b_q, w_k, w_v, b_v, w_o, b_o, ln2_gain, ln2_bias, w_fc1, b_fc1, w_fc2, b_fc2, post_gain, post_bias, w_ck, w_cv, b_cv):
    tok_rows = BATCH_SIZE * NUM_FRAMES
    flat_in = hidden_in.reshape(tok_rows, D_MODEL)
    normed1 = layer_norm(flat_in, ln1_gain, ln1_bias)
    q_flat = ((jnp.dot(normed1, w_q, preferred_element_type=jnp.float32) + b_q.astype(jnp.float32)) * ATTN_SCALE).astype(jnp.bfloat16)
    k_flat = (jnp.dot(normed1, w_k, preferred_element_type=jnp.float32) * ATTN_SCALE).astype(jnp.bfloat16)
    v_flat = (jnp.dot(normed1, w_v, preferred_element_type=jnp.float32) + b_v.astype(jnp.float32)).astype(jnp.bfloat16)
    attn_heads = lax.map(head_attention, (split_heads(q_flat), split_heads(k_flat), split_heads(v_flat)))
    attn_flat = attn_heads.reshape(BATCH_SIZE, NUM_HEADS, NUM_FRAMES, HEAD_DIM).transpose(0, 2, 1, 3).reshape(tok_rows, D_MODEL)
    attn_out = (jnp.dot(attn_flat, w_o, preferred_element_type=jnp.float32) + b_o.astype(jnp.float32)).astype(jnp.bfloat16)
    resid_one = (flat_in.astype(jnp.float32) + attn_out.astype(jnp.float32)).astype(jnp.bfloat16)
    normed2 = layer_norm(resid_one, ln2_gain, ln2_bias)
    hidden_act = jax.nn.gelu(jnp.dot(normed2, w_fc1, preferred_element_type=jnp.float32) + b_fc1.astype(jnp.float32), approximate=False).astype(jnp.bfloat16)
    mlp_out = (jnp.dot(hidden_act, w_fc2, preferred_element_type=jnp.float32) + b_fc2.astype(jnp.float32)).astype(jnp.bfloat16)
    resid_two = (resid_one.astype(jnp.float32) + mlp_out.astype(jnp.float32)).astype(jnp.bfloat16)
    enc_flat = layer_norm(resid_two, post_gain, post_bias)

    def cache_layer(layer_weights):
        wk_layer, wv_layer, bv_layer = layer_weights
        k_layer = jnp.dot(enc_flat, wk_layer, preferred_element_type=jnp.float32).astype(jnp.bfloat16)
        v_layer = (jnp.dot(enc_flat, wv_layer, preferred_element_type=jnp.float32) + bv_layer.astype(jnp.float32)).astype(jnp.bfloat16)
        return k_layer, v_layer

    k_all, v_all = lax.map(cache_layer, (w_ck, w_cv, b_cv))
    cache_shape = (NUM_LAYERS, BATCH_SIZE, NUM_FRAMES, NUM_HEADS, HEAD_DIM)
    return enc_flat.reshape(BATCH_SIZE, NUM_FRAMES, D_MODEL), k_all.reshape(cache_shape), v_all.reshape(cache_shape)
```

```python
import numpy as np
import jax
import jax.numpy as jnp
from jax import lax
from jax.sharding import PartitionSpec as P

HEAD_DIM = 64
ATTN_SCALE = HEAD_DIM ** -0.25
LN_EPS = 1e-5


def layer_norm(values, ln_gain, ln_bias):
    centered = values.astype(jnp.float32)
    centered = centered - jnp.mean(centered, axis=-1, keepdims=True)
    row_var = jnp.mean(centered * centered, axis=-1, keepdims=True)
    normed = centered * lax.rsqrt(row_var + LN_EPS)
    return (normed * ln_gain.astype(jnp.float32) + ln_bias.astype(jnp.float32)).astype(jnp.bfloat16)


def device_body(hidden_loc, ln1_gain, ln1_bias, w_q, b_q, w_k, w_v, b_v, w_o, b_o, ln2_gain, ln2_bias, w_fc1, b_fc1, w_fc2, b_fc2, post_gain, post_bias, w_ck, w_cv, b_cv):
    f32, bf16 = jnp.float32, jnp.bfloat16
    clips, frames, width = hidden_loc.shape
    n = lax.axis_size("tp")
    per_chip = clips // (n // 2)
    core = lax.rem(lax.axis_index("tp"), 2)
    order = [per_chip * (d // 2) + (2 * (d % 2) if j == 0 else 1) for d in range(n) for j in range(2)]
    send = jnp.stack([hidden_loc[c] for c in order]).reshape(n, 2, frames, width)
    recv = lax.all_to_all(send, "tp", split_axis=0, concat_axis=0)
    total = n * frames
    x2 = recv.transpose(1, 0, 2, 3).reshape(2, total, width)
    half = total // 2

    qkv = lax.all_gather(jnp.concatenate([w_q, w_k, w_v], axis=1), "tp", axis=0)
    wo_all = lax.all_gather(w_o, "tp", axis=0, tiled=True)
    w1_all = lax.all_gather(w_fc1, "tp", axis=0)
    w2_all = lax.all_gather(w_fc2, "tp", axis=0, tiled=True)
    bias_q = lax.all_gather(b_q, "tp", axis=0, tiled=True).astype(f32)
    bias_v = lax.all_gather(b_v, "tp", axis=0, tiled=True).astype(f32)
    bias_1 = lax.all_gather(b_fc1, "tp", axis=0, tiled=True).astype(f32)

    a2 = layer_norm(x2, ln1_gain, ln1_bias)
    a_shared = lax.dynamic_slice_in_dim(a2[1], core * half, half, 0)
    x_shared = lax.dynamic_slice_in_dim(x2[1], core * half, half, 0)
    a_own = jnp.concatenate([a2[0], a_shared]).reshape(3, half, width)
    x_own = jnp.concatenate([x2[0], x_shared]).reshape(3 * half, width)
    heads = width // HEAD_DIM
    wq = qkv[:, :, : w_q.shape[1]]
    wk = qkv[:, :, w_q.shape[1]: 2 * w_q.shape[1]]
    wv = qkv[:, :, 2 * w_q.shape[1]:]
    q = jnp.einsum("btd,ndc->btnc", a_own, wq, preferred_element_type=f32).reshape(3, half, width)
    q = ((q + bias_q) * ATTN_SCALE).astype(bf16).reshape(3, half, heads, HEAD_DIM)
    k = (jnp.einsum("btd,ndc->btnc", a2, wk, preferred_element_type=f32) * ATTN_SCALE).astype(bf16).reshape(2, total, heads, HEAD_DIM)
    v = (jnp.einsum("btd,ndc->btnc", a2, wv, preferred_element_type=f32).reshape(2, total, width) + bias_v).astype(bf16).reshape(2, total, heads, HEAD_DIM)

    def attend(qq, kk, vv):
        s = jnp.einsum("qhe,khe->hqk", qq, kk, preferred_element_type=f32)
        p = jax.nn.softmax(s, axis=-1).astype(bf16)
        return jnp.einsum("hqk,khe->qhe", p, vv, preferred_element_type=f32).astype(bf16)

    o = jnp.concatenate([attend(q[:2].reshape(total, heads, HEAD_DIM), k[0], v[0]), attend(q[2], k[1], v[1])]).reshape(3 * half, width)
    attn_out = (jnp.dot(o, wo_all, preferred_element_type=f32) + b_o.astype(f32)).astype(bf16)
    h = (x_own.astype(f32) + attn_out.astype(f32)).astype(bf16)
    m = layer_norm(h, ln2_gain, ln2_bias)
    g = jnp.einsum("td,ndc->tnc", m, w1_all, preferred_element_type=f32).reshape(3 * half, -1)
    g = jax.nn.gelu(g + bias_1, approximate=False).astype(bf16)
    mlp = (jnp.dot(g, w2_all, preferred_element_type=f32) + b_fc2.astype(f32)).astype(bf16)
    h2 = (h.astype(f32) + mlp.astype(f32)).astype(bf16)
    e = layer_norm(h2, post_gain, post_bias)
    num_layers, local = w_ck.shape[0], w_ck.shape[2]
    me = lax.axis_index("tp")
    e_parts = [lax.all_gather(e[j * half:(j + 1) * half], "tp", axis=0) for j in range(3)]
    by_clip = []
    for c in range(n // 2):
        by_clip.append(jnp.concatenate([e_parts[0][2 * c], e_parts[1][2 * c]]))
        by_clip.append(jnp.concatenate([e_parts[2][2 * c], e_parts[2][2 * c + 1]]))
        by_clip.append(jnp.concatenate([e_parts[0][2 * c + 1], e_parts[1][2 * c + 1]]))
    e_all = jnp.stack(by_clip)
    enc = lax.dynamic_slice_in_dim(e_all, me * frames, frames, 1)
    cache_shape = (num_layers, clips, total, local // HEAD_DIM, HEAD_DIM)
    k_cache = jnp.einsum("bfd,ldc->lbfc", e_all, w_ck, preferred_element_type=f32).astype(bf16).reshape(cache_shape)
    v_cache = (jnp.einsum("bfd,ldc->lbfc", e_all, w_cv, preferred_element_type=f32) + b_cv.astype(f32)[:, None, None, :]).astype(bf16).reshape(cache_shape)
    return enc, k_cache, v_cache


def solution(mesh):
    in_specs = (P("dp", "tp", None), P(), P(), P(None, "tp"), P("tp"), P(None, "tp"), P(None, "tp"), P("tp"), P("tp", None), P(), P(), P(), P(None, "tp"), P("tp"), P("tp", None), P(), P(), P(), P(None, None, "tp"), P(None, None, "tp"), P(None, "tp"))
    out_specs = (P("dp", "tp", None), P(None, "dp", None, "tp", None), P(None, "dp", None, "tp", None))
    return jax.shard_map(device_body, mesh=mesh, in_specs=in_specs, out_specs=out_specs, check_vma=False)
```

```python
import functools

import jax
import jax.numpy as jnp
from jax import lax
from jax.experimental import pallas as pl
from jax.experimental.pallas import tpu as pltpu
from jax.sharding import PartitionSpec as P

HEAD_DIM = 64
ATTN_SCALE = HEAD_DIM ** -0.25
LN_EPS = 1e-5
CLIPS = 12
PER_CHIP = 3
FR = 96
HALF = 4 * FR
FRAMES = 8 * FR
D = 1024
LOC = 128
HID = 512
NQ = 4 * LOC
NH = 4 * HID
QROWS = 256
F32, BF16 = jnp.float32, jnp.bfloat16
LN1G, LN1B, LN2G, LN2B, POSTG, POSTB, BO, BFC2 = range(8)


def ln_rows(values, gain, bias):
    centered = values - jnp.mean(values, axis=-1, keepdims=True)
    row_var = jnp.mean(centered * centered, axis=-1, keepdims=True)
    return (centered * lax.rsqrt(row_var + LN_EPS) * gain + bias).astype(BF16)


def kernel(hid, wq_h, wk_h, wv_h, wo_h, w1_h, w2_h, ck_h, cv_h, bias_h, vec,
           enc_o, kc_o, vc_o,
           xb, am, ex_s, ex_r, wqkv, wo, w1, w2, bias, qkv, kz, vz, ob, g, acc, wct, bct, ea, ost,
           x_r, x_s, w_r, w_s, b_r, b_s, am_r, am_s, ex_rs, ex_ss, ex_x, ex_y, ex_d, ex_f, es_x, es_y, es_d, es_f, o_s, enc_s, c_s):
    t = lax.axis_index("tp")
    c, k = t // 2, t % 2
    cx, cy = c % 2, c // 2
    cxn = 2 * cy + (1 - cx)
    cyn = 2 * (1 - cy) + cx
    cdg = 2 * (1 - cy) + (1 - cx)
    ks = 1 - k
    sib, xn, yn, dg = 2 * c + ks, 2 * cxn + k, 2 * cyn + k, 2 * cdg + k

    def remote(src, dst, ssem, rsem, dev):
        return pltpu.make_async_remote_copy(src_ref=src, dst_ref=dst, send_sem=ssem, recv_sem=rsem,
                                            device_id={"tp": dev}, device_id_type=pl.DeviceIdType.MESH)

    def wait_recv(ref, rsem):
        pltpu.make_async_copy(ref, ref, rsem).wait()

    barrier = pltpu.get_barrier_semaphore()
    for peer in (sib, xn, yn, dg):
        pl.semaphore_signal(barrier, inc=1, device_id={"tp": peer}, device_id_type=pl.DeviceIdType.MESH)
    pl.semaphore_wait(barrier, 4)

    def xslot(chip):
        return xb.at[:, pl.ds(chip * FR, FR), :]

    def wfull(i, chip):
        if i < 3:
            return wqkv.at[i, :, pl.ds(pl.multiple_of(chip * LOC, LOC), LOC)]
        if i == 3:
            return wo.at[pl.ds(chip * LOC, LOC)]
        if i == 4:
            return w1.at[:, pl.ds(pl.multiple_of(chip * HID, HID), HID)]
        return w2.at[pl.ds(chip * HID, HID)]

    def whalf(i, chip, hf):
        if i < 3:
            return wqkv.at[i, pl.ds(hf * (D // 2), D // 2), pl.ds(pl.multiple_of(chip * LOC, LOC), LOC)]
        if i == 3:
            return wo.at[pl.ds(chip * LOC + hf * (LOC // 2), LOC // 2)]
        if i == 4:
            return w1.at[pl.ds(hf * (D // 2), D // 2), pl.ds(pl.multiple_of(chip * HID, HID), HID)]
        return w2.at[pl.ds(chip * HID + hf * (HID // 2), HID // 2)]

    w_hbm = (wq_h, wk_h, wv_h, wo_h, w1_h, w2_h)
    sends = []

    def go(src, dst, ssem, rsem, dev):
        cp = remote(src, dst, ssem, rsem, dev)
        cp.start()
        sends.append(cp)

    def send_direct(i):
        go(w_hbm[i], wfull(i, c), w_s.at[i, 0], w_r.at[i, 1], xn)
        go(w_hbm[i], wfull(i, c), w_s.at[i, 1], w_r.at[i, 2], yn)

    def relay(i):
        wait_recv(wfull(i, cxn), w_r.at[i, 1])
        go(whalf(i, cxn, 0), whalf(i, cxn, 0), w_s.at[i, 2], w_r.at[i, 3], yn)
        wait_recv(wfull(i, cyn), w_r.at[i, 2])
        go(whalf(i, cyn, 1), whalf(i, cyn, 1), w_s.at[i, 3], w_r.at[i, 4], xn)

    def wait_rest(i):
        wait_recv(wfull(i, c), w_r.at[i, 0])
        wait_recv(whalf(i, cdg, 0), w_r.at[i, 3])
        wait_recv(whalf(i, cdg, 1), w_r.at[i, 4])

    for r, (dev, chip) in enumerate(((xn, cxn), (yn, cyn), (dg, cdg))):
        go(bias_h, bias.at[c], b_s.at[r], b_r.at[1 + r], dev)
    for r, (dev, chip) in ((2, (dg, cdg)), (0, (xn, cxn)), (1, (yn, cyn))):
        go(hid.at[pl.ds(chip * PER_CHIP, PER_CHIP)], xslot(c), x_s.at[r], x_r.at[1 + r], dev)
    for i in range(3):
        send_direct(i)
    pltpu.make_async_copy(hid.at[pl.ds(c * PER_CHIP, PER_CHIP)], xslot(c), x_r.at[0]).start()
    pltpu.make_async_copy(bias_h, bias.at[c], b_r.at[0]).start()
    wc_copies = []
    for i, src in enumerate((ck_h.at[0], ck_h.at[1], cv_h.at[0], cv_h.at[1])):
        cp = pltpu.make_async_copy(src, wct.at[i], c_s.at[i])
        cp.start()
        wc_copies.append(cp)
    for i in range(6):
        pltpu.make_async_copy(w_hbm[i], wfull(i, c), w_r.at[i, 0]).start()

    for r, chip in ((0, c), (1, cxn), (2, cyn), (3, cdg)):
        wait_recv(xslot(chip), x_r.at[r])
    own = pl.ds(k * HALF, HALF)
    oth = pl.ds(ks * HALF, HALF)
    for j in range(PER_CHIP):
        def ln1(b, _, j=j):
            vals = xb[j, pl.ds(b * FR, FR), :].astype(F32)
            am[j, pl.ds(k * HALF + b * FR, FR), :] = ln_rows(vals, vec[LN1G:LN1G + 1, :], vec[LN1B:LN1B + 1, :])
            return 0
        lax.fori_loop(0, 4, ln1, 0)
    a_sends = []
    for j in range(PER_CHIP):
        cp = remote(am.at[j, own], am.at[j, own], am_s.at[0, j], am_r.at[0, j], sib)
        cp.start()
        a_sends.append(cp)

    send_direct(3)
    for cp in wc_copies:
        cp.wait()
    for r, chip in ((0, c), (1, cxn), (2, cyn), (3, cdg)):
        wait_recv(bias.at[chip], b_r.at[r])
    for l in range(2):
        bct[l] = jnp.transpose(jnp.broadcast_to(bias[c, 6 + l:7 + l, :], (LOC, LOC)))
    for i in range(3):
        relay(i)
    relay(3)
    send_direct(4)
    send_direct(5)
    for i in range(3):
        wait_rest(i)

    def row_of(r):
        return jnp.concatenate([bias[n, r:r + 1, :] for n in range(4)], axis=1)

    lane = lax.broadcasted_iota(jnp.int32, (FRAMES, LOC), 1)

    def attention_stage(j):
        wait_recv(am.at[j, oth], am_r.at[0, j])
        bq, bv = row_of(0), row_of(1)

        def project(r, _):
            rows = pl.ds(r * HALF, HALF)
            a = am[j, rows, :]
            qkv[0, rows, :] = ((jnp.dot(a, wqkv[0], preferred_element_type=F32) + bq) * ATTN_SCALE).astype(BF16)
            qkv[1, rows, :] = (jnp.dot(a, wqkv[1], preferred_element_type=F32) * ATTN_SCALE).astype(BF16)
            qkv[2, rows, :] = (jnp.dot(a, wqkv[2], preferred_element_type=F32) + bv).astype(BF16)
            return 0
        lax.fori_loop(0, 2, project, 0)

        for p in range(4):
            cols = slice(p * LOC, (p + 1) * LOC)
            kp, vp = qkv[1, :, cols], qkv[2, :, cols]
            zero = jnp.zeros_like(kp)
            kz[0] = jnp.where(lane < HEAD_DIM, kp, zero)
            kz[1] = jnp.where(lane < HEAD_DIM, zero, kp)
            vz[0] = jnp.where(lane < HEAD_DIM, vp, zero)
            vz[1] = jnp.where(lane < HEAD_DIM, zero, vp)

            def attend(r, _, cols=cols):
                rows = pl.ds(r * QROWS, QROWS)
                qb = qkv[0, rows, cols]
                out = None
                for hh in range(2):
                    s = lax.dot_general(qb, kz[hh], (((1,), (1,)), ((), ())), preferred_element_type=F32)
                    e = jnp.exp(s - jnp.max(s, axis=-1, keepdims=True))
                    prob = (e * (1.0 / jnp.sum(e, axis=-1, keepdims=True))).astype(BF16)
                    part = jnp.dot(prob, vz[hh], preferred_element_type=F32)
                    out = part if out is None else out + part
                ob[rows, cols] = out.astype(BF16)
                return 0
            lax.fori_loop(0, FRAMES // QROWS, attend, 0)

    def swap_partials(phase, j, lhs, weight):
        for n in range(2):
            cols = slice(n * 512, (n + 1) * 512)
            ex_s[j, :, cols] = jnp.dot(lhs[oth, :], weight[:, cols], preferred_element_type=F32).astype(BF16)
        cp = remote(ex_s.at[j], ex_r.at[j], ex_ss.at[phase, j], ex_rs.at[phase, j], sib)
        cp.start()
        for n in range(2):
            cols = slice(n * 512, (n + 1) * 512)
            acc[:, cols] = jnp.dot(lhs[own, :], weight[:, cols], preferred_element_type=F32)
        wait_recv(ex_r.at[j], ex_rs.at[phase, j])
        cp.wait_send()

    m_sends = []
    for j in range(PER_CHIP):
        attention_stage(j)
        if j == 0:
            wait_rest(3)
        swap_partials(0, j, ob, wo)
        a_sends[j].wait_send()

        def ln2(b, _, j=j):
            rows = pl.ds(b * FR, FR)
            out = (acc[rows, :] + ex_r[j, rows, :].astype(F32) + vec[BO:BO + 1, :]).astype(BF16)
            h = (xb[j, rows, :].astype(F32) + out.astype(F32)).astype(BF16)
            xb[j, rows, :] = h
            am[j, pl.ds(k * HALF + b * FR, FR), :] = ln_rows(h.astype(F32), vec[LN2G:LN2G + 1, :], vec[LN2B:LN2B + 1, :])
            return 0
        lax.fori_loop(0, 4, ln2, 0)
        cp = remote(am.at[j, own], am.at[j, own], am_s.at[1, j], am_r.at[1, j], sib)
        cp.start()
        m_sends.append(cp)
        if j == 1:
            relay(4)
    relay(5)

    def epiece(clip, core, hf):
        return ea.at[clip, pl.ds(2 * hf, 2), core]

    for j in range(PER_CHIP):
        wait_recv(am.at[j, oth], am_r.at[1, j])
        if j == 0:
            wait_rest(4)

        for n in range(4):
            b1 = jnp.concatenate([bias[n, 2 + q:3 + q, :] for q in range(4)], axis=1)

            def up(r, _, j=j, n=n, b1=b1):
                rows = pl.ds(r * HALF, HALF)
                u = jnp.dot(am[j, rows, :], w1[:, n * HID:(n + 1) * HID], preferred_element_type=F32) + b1
                g[rows, n * HID:(n + 1) * HID] = (0.5 * u * (1.0 + lax.erf(u * (2.0 ** -0.5)))).astype(BF16)
                return 0
            lax.fori_loop(0, 2, up, 0)
        if j == 0:
            wait_rest(5)
        swap_partials(1, j, g, w2)
        clip = PER_CHIP * c + j

        def post(b, _, j=j, clip=clip):
            rows = pl.ds(b * FR, FR)
            out = (acc[rows, :] + ex_r[j, rows, :].astype(F32) + vec[BFC2:BFC2 + 1, :]).astype(BF16)
            h2 = (xb[j, rows, :].astype(F32) + out.astype(F32)).astype(BF16)
            ea[clip, b, k] = ln_rows(h2.astype(F32), vec[POSTG:POSTG + 1, :], vec[POSTB:POSTB + 1, :])
            return 0
        lax.fori_loop(0, 4, post, 0)
        for hf in range(2):
            go(epiece(clip, k, hf), epiece(clip, k, hf), es_x.at[j, hf], ex_x.at[j, hf], xn)
            go(epiece(clip, k, 1 - hf), epiece(clip, k, 1 - hf), es_y.at[j, 1 - hf], ex_y.at[j, 1 - hf], yn)
        for hf in range(2):
            go(epiece(clip, k, hf), epiece(clip, k, hf), es_f.at[0, j, hf], ex_f.at[0, j, hf], sib)

    def out_copies(slot, clip):
        return [pltpu.make_async_copy(ost.at[slot, pl.ds(i * LOC, LOC)], (kc_o, vc_o)[i // 2].at[i % 2, clip], o_s.at[slot, i])
                for i in range(4)]

    def caches(group, chip):
        def one(j, _):
            clip = chip * PER_CHIP + j
            for hf in range(2):
                wait_recv(epiece(clip, ks, hf), ex_f.at[group, j, hf])
            pltpu.make_async_copy(ea.at[clip, c, k], enc_o.at[clip], enc_s.at[clip]).start()
            step = group * PER_CHIP + j
            slot = step % 2

            @pl.when(step >= 2)
            def _():
                for cp in out_copies(slot, clip):
                    cp.wait()
            ec = ea[clip].reshape(FRAMES, D)
            for i in range(4):
                r = lax.dot_general(wct[i], ec, (((0,), (1,)), ((), ())), preferred_element_type=F32)
                if i >= 2:
                    r = r + jnp.concatenate([bct[i - 2]] * 6, axis=1)
                ost[slot, i * LOC:(i + 1) * LOC, :] = r.astype(BF16)
            for cp in out_copies(slot, clip):
                cp.start()
            return 0
        lax.fori_loop(0, PER_CHIP, one, 0)

    caches(0, c)
    for j in range(PER_CHIP):
        clx, cly = PER_CHIP * cxn + j, PER_CHIP * cyn + j
        for hf in range(2):
            wait_recv(epiece(clx, k, hf), ex_x.at[j, hf])
            if hf == 0:
                go(epiece(clx, k, 0), epiece(clx, k, 0), es_d.at[j, 0], ex_d.at[j, 0], yn)
            go(epiece(clx, k, hf), epiece(clx, k, hf), es_f.at[1, j, hf], ex_f.at[1, j, hf], sib)
            wait_recv(epiece(cly, k, 1 - hf), ex_y.at[j, 1 - hf])
            if hf == 0:
                go(epiece(cly, k, 1), epiece(cly, k, 1), es_d.at[j, 1], ex_d.at[j, 1], xn)
            go(epiece(cly, k, 1 - hf), epiece(cly, k, 1 - hf), es_f.at[2, j, 1 - hf], ex_f.at[2, j, 1 - hf], sib)
    caches(1, cxn)
    caches(2, cyn)
    for j in range(PER_CHIP):
        cld = PER_CHIP * cdg + j
        for hf in range(2):
            wait_recv(epiece(cld, k, hf), ex_d.at[j, hf])
            go(epiece(cld, k, hf), epiece(cld, k, hf), es_f.at[3, j, hf], ex_f.at[3, j, hf], sib)
    caches(3, cdg)

    for slot in range(2):
        for cp in out_copies(slot, 0):
            cp.wait()
    for clip in range(CLIPS):
        pltpu.make_async_copy(ea.at[clip, c, k], enc_o.at[clip], enc_s.at[clip]).wait()
    for cp in sends + m_sends:
        cp.wait_send()


def device_body(hidden_loc, ln1_gain, ln1_bias, w_q, b_q, w_k, w_v, b_v, w_o, b_o, ln2_gain, ln2_bias, w_fc1, b_fc1, w_fc2, b_fc2, post_gain, post_bias, w_ck, w_cv, b_cv):
    vec = jnp.stack([ln1_gain, ln1_bias, ln2_gain, ln2_bias, post_gain, post_bias, b_o, b_fc2]).astype(F32)
    bias = jnp.concatenate([b_q[None], b_v[None], b_fc1.reshape(4, LOC), b_cv]).astype(F32)
    anyspec = pl.BlockSpec(memory_space=pl.ANY)
    dma = pltpu.SemaphoreType.DMA
    cache = jax.ShapeDtypeStruct((2, CLIPS, LOC, FRAMES), BF16)
    enc, kc, vc = pl.pallas_call(
        kernel,
        out_shape=(jax.ShapeDtypeStruct((CLIPS, FR, D), BF16), cache, cache),
        in_specs=[anyspec] * 10 + [pl.BlockSpec(memory_space=pltpu.VMEM)],
        out_specs=(anyspec, anyspec, anyspec),
        scratch_shapes=[
            pltpu.VMEM((PER_CHIP, HALF, D), BF16),
            pltpu.VMEM((PER_CHIP, FRAMES, D), BF16),
            pltpu.VMEM((PER_CHIP, HALF, D), BF16),
            pltpu.VMEM((PER_CHIP, HALF, D), BF16),
            pltpu.VMEM((3, D, NQ), BF16),
            pltpu.VMEM((NQ, D), BF16),
            pltpu.VMEM((D, NH), BF16),
            pltpu.VMEM((NH, D), BF16),
            pltpu.VMEM((4, 8, LOC), F32),
            pltpu.VMEM((3, FRAMES, NQ), BF16),
            pltpu.VMEM((2, FRAMES, LOC), BF16),
            pltpu.VMEM((2, FRAMES, LOC), BF16),
            pltpu.VMEM((FRAMES, NQ), BF16),
            pltpu.VMEM((FRAMES, NH), BF16),
            pltpu.VMEM((HALF, D), F32),
            pltpu.VMEM((4, D, LOC), BF16),
            pltpu.VMEM((2, LOC, LOC), F32),
            pltpu.VMEM((CLIPS, 4, 2, FR, D), BF16),
            pltpu.VMEM((2, 4 * LOC, FRAMES), BF16),
            dma((4,)), dma((3,)), dma((6, 5)), dma((6, 4)), dma((4,)), dma((3,)),
            dma((2, 3)), dma((2, 3)), dma((2, 3)), dma((2, 3)),
            dma((3, 2)), dma((3, 2)), dma((3, 2)), dma((4, 3, 2)),
            dma((3, 2)), dma((3, 2)), dma((3, 2)), dma((4, 3, 2)),
            dma((2, 4)), dma((CLIPS,)), dma((4,)),
        ],
        compiler_params=pltpu.CompilerParams(collective_id=0, has_side_effects=True, vmem_limit_bytes=67043328),
        name="encoder_layer",
    )(hidden_loc, w_q, w_k, w_v, w_o, w_fc1, w_fc2, w_ck, w_cv, bias, vec)

    def heads_last(cached):
        return cached.reshape(2, CLIPS, LOC // HEAD_DIM, HEAD_DIM, FRAMES).transpose(0, 1, 4, 2, 3)
    return enc, heads_last(kc), heads_last(vc)


def solution(mesh):
    in_specs = (P("dp", "tp", None), P(), P(), P(None, "tp"), P("tp"), P(None, "tp"), P(None, "tp"), P("tp"), P("tp", None), P(), P(), P(), P(None, "tp"), P("tp"), P("tp", None), P(), P(), P(), P(None, None, "tp"), P(None, None, "tp"), P(None, "tp"))
    out_specs = (P("dp", "tp", None), P(None, "dp", None, "tp", None), P(None, "dp", None, "tp", None))
    return jax.shard_map(device_body, mesh=mesh, in_specs=in_specs, out_specs=out_specs, check_vma=False)
```

```python
import functools

import jax
import jax.numpy as jnp
from jax import lax
from jax.experimental import pallas as pl
from jax.experimental.pallas import tpu as pltpu
from jax.sharding import PartitionSpec as P

HEAD_DIM = 64
ATTN_SCALE = HEAD_DIM ** -0.25
LN_EPS = 1e-5
CLIPS = 12
PER_CHIP = 3
FR = 96
HALF = 4 * FR
FRAMES = 8 * FR
D = 1024
LOC = 128
HID = 512
NQ = 4 * LOC
NH = 4 * HID
QROWS = 256
F32, BF16 = jnp.float32, jnp.bfloat16


def ln_rows(values, gain, bias):
    centered = values - jnp.mean(values, axis=-1, keepdims=True)
    row_var = jnp.mean(centered * centered, axis=-1, keepdims=True)
    return (centered * lax.rsqrt(row_var + LN_EPS) * gain + bias).astype(BF16)


def kernel(hid, wq_h, wk_h, wv_h, wo_h, w1_h, w2_h, ck_h, cv_h,
           bq_v, bv_v, b1_v, bcv_v, ln1g, ln1b, ln2g, ln2b, postg, postb, bo_v, bfc2,
           enc_o, kc_o, vc_o,
           xb, am, ex_s, ex_r, wqkv, wo, w1, w2, bias, qkv, kz, vz, ob, g, acc, wct, bct, ea,
           x_r, x_s, w_r, w_s, b_r, b_s, am_r, am_s, ex_rs, ex_ss, ex_x, ex_y, ex_d, ex_f, es_x, es_y, es_d, es_f, c_s, free):
    t = lax.axis_index("tp")
    c, k = t // 2, t % 2
    cx, cy = c % 2, c // 2
    cxn = 2 * cy + (1 - cx)
    cyn = 2 * (1 - cy) + cx
    cdg = 2 * (1 - cy) + (1 - cx)
    ks = 1 - k
    sib, xn, yn, dg = 2 * c + ks, 2 * cxn + k, 2 * cyn + k, 2 * cdg + k

    def remote(src, dst, ssem, rsem, dev):
        return pltpu.make_async_remote_copy(src_ref=src, dst_ref=dst, send_sem=ssem, recv_sem=rsem,
                                            device_id={"tp": dev}, device_id_type=pl.DeviceIdType.MESH)

    def wait_recv(ref, rsem):
        pltpu.make_async_copy(ref, ref, rsem).wait()

    def row(ref):
        return ref[...].astype(F32).reshape(1, ref.shape[0])

    bias[c, 0:1, :] = row(bq_v)
    bias[c, 1:2, :] = row(bv_v)
    b1_row = row(b1_v)
    for q in range(4):
        bias[c, 2 + q:3 + q, :] = b1_row[:, q * LOC:(q + 1) * LOC]
    for l in range(2):
        bct[l] = jnp.transpose(jnp.broadcast_to(bcv_v[l:l + 1, :].astype(F32), (LOC, LOC)))

    barrier = pltpu.get_barrier_semaphore()
    for peer in (sib, xn, yn, dg):
        pl.semaphore_signal(barrier, inc=1, device_id={"tp": peer}, device_id_type=pl.DeviceIdType.MESH)
    pl.semaphore_wait(barrier, 4)

    def xslot(chip, late):
        return xb.at[pl.ds(2, 1) if late else pl.ds(0, 2), pl.ds(chip * FR, FR), :]

    def xsource(chip, late):
        return hid.at[pl.ds(chip * PER_CHIP + 2, 1) if late else pl.ds(chip * PER_CHIP, 2)]

    def wfull(i, chip):
        if i < 3:
            return wqkv.at[i, :, pl.ds(pl.multiple_of(chip * LOC, LOC), LOC)]
        if i == 3:
            return wo.at[pl.ds(chip * LOC, LOC)]
        if i == 4:
            return w1.at[:, pl.ds(pl.multiple_of(chip * HID, HID), HID)]
        return w2.at[pl.ds(chip * HID, HID)]

    def whalf(i, chip, hf):
        if i < 3:
            return wqkv.at[i, pl.ds(hf * (D // 2), D // 2), pl.ds(pl.multiple_of(chip * LOC, LOC), LOC)]
        if i == 3:
            return wo.at[pl.ds(chip * LOC + hf * (LOC // 2), LOC // 2)]
        if i == 4:
            return w1.at[pl.ds(hf * (D // 2), D // 2), pl.ds(pl.multiple_of(chip * HID, HID), HID)]
        return w2.at[pl.ds(chip * HID + hf * (HID // 2), HID // 2)]

    w_hbm = (wq_h, wk_h, wv_h, wo_h, w1_h, w2_h)
    sends = []

    def go(src, dst, ssem, rsem, dev):
        cp = remote(src, dst, ssem, rsem, dev)
        cp.start()
        sends.append(cp)

    def send_direct(i):
        go(w_hbm[i], wfull(i, c), w_s.at[i, 0], w_r.at[i, 1], xn)
        go(w_hbm[i], wfull(i, c), w_s.at[i, 1], w_r.at[i, 2], yn)

    def relay(i):
        wait_recv(wfull(i, cxn), w_r.at[i, 1])
        go(whalf(i, cxn, 0), whalf(i, cxn, 0), w_s.at[i, 2], w_r.at[i, 3], yn)
        wait_recv(wfull(i, cyn), w_r.at[i, 2])
        go(whalf(i, cyn, 1), whalf(i, cyn, 1), w_s.at[i, 3], w_r.at[i, 4], xn)

    def wait_rest(i):
        wait_recv(wfull(i, c), w_r.at[i, 0])
        wait_recv(whalf(i, cdg, 0), w_r.at[i, 3])
        wait_recv(whalf(i, cdg, 1), w_r.at[i, 4])

    def send_x(late):
        for r, (dev, chip) in ((2, (dg, cdg)), (0, (xn, cxn)), (1, (yn, cyn))):
            go(xsource(chip, late), xslot(c, late), x_s.at[late, r], x_r.at[late, 1 + r], dev)

    def ln1_stage(j):
        def body(b, _):
            vals = xb[j, pl.ds(b * FR, FR), :].astype(F32)
            am[j, k, b] = ln_rows(vals, row(ln1g), row(ln1b))
            return 0
        lax.fori_loop(0, 4, body, 0)
        cp = remote(am.at[j, k], am.at[j, k], am_s.at[0, j], am_r.at[0, j], sib)
        cp.start()
        a_sends.append(cp)

    def wait_x(late):
        for r, chip in ((0, c), (1, cxn), (2, cyn), (3, cdg)):
            wait_recv(xslot(chip, late), x_r.at[late, r])

    for r, dev in enumerate((xn, yn, dg)):
        go(bias.at[c], bias.at[c], b_s.at[r], b_r.at[r], dev)
    send_x(0)
    for i in range(3):
        send_direct(i)
    for late in range(2):
        pltpu.make_async_copy(xsource(c, late), xslot(c, late), x_r.at[late, 0]).start()
    wc_copies = []
    for i, src in enumerate((ck_h.at[0], ck_h.at[1], cv_h.at[0], cv_h.at[1])):
        cp = pltpu.make_async_copy(src, wct.at[i], c_s.at[i])
        cp.start()
        wc_copies.append(cp)
    for i in range(6):
        pltpu.make_async_copy(w_hbm[i], wfull(i, c), w_r.at[i, 0]).start()

    a_sends = []
    wait_x(0)
    for j in range(2):
        ln1_stage(j)
    send_direct(3)
    for cp in wc_copies:
        cp.wait()
    for r, chip in enumerate((cxn, cyn, cdg)):
        wait_recv(bias.at[chip], b_r.at[r])
    for i in range(4):
        relay(i)
    send_direct(4)
    send_direct(5)
    for i in range(3):
        wait_rest(i)

    def row_of(r):
        return jnp.concatenate([bias[n, r:r + 1, :] for n in range(4)], axis=1)

    lane = lax.broadcasted_iota(jnp.int32, (FRAMES, LOC), 1)

    def attention_stage(j):
        wait_recv(am.at[j, ks], am_r.at[0, j])
        bq, bv = row_of(0), row_of(1)

        def project(r, _):
            rows = pl.ds(r * HALF, HALF)
            a = am[j, r].reshape(HALF, D)
            qkv[0, rows, :] = ((jnp.dot(a, wqkv[0], preferred_element_type=F32) + bq) * ATTN_SCALE).astype(BF16)
            qkv[1, rows, :] = (jnp.dot(a, wqkv[1], preferred_element_type=F32) * ATTN_SCALE).astype(BF16)
            qkv[2, rows, :] = (jnp.dot(a, wqkv[2], preferred_element_type=F32) + bv).astype(BF16)
            return 0
        lax.fori_loop(0, 2, project, 0)

        def pair(p, _):
            cols = pl.ds(pl.multiple_of(p * LOC, LOC), LOC)
            kp, vp = qkv[1, :, cols], qkv[2, :, cols]
            zero = jnp.zeros_like(kp)
            kz[0] = jnp.where(lane < HEAD_DIM, kp, zero)
            kz[1] = jnp.where(lane < HEAD_DIM, zero, kp)
            vz[0] = jnp.where(lane < HEAD_DIM, vp, zero)
            vz[1] = jnp.where(lane < HEAD_DIM, zero, vp)

            def attend(r, _):
                rows = pl.ds(r * QROWS, QROWS)
                qb = qkv[0, rows, cols]
                out = None
                for hh in range(2):
                    s = lax.dot_general(qb, kz[hh], (((1,), (1,)), ((), ())), preferred_element_type=F32)
                    e = jnp.exp(s - jnp.max(s, axis=-1, keepdims=True))
                    prob = (e * (1.0 / jnp.sum(e, axis=-1, keepdims=True))).astype(BF16)
                    part = jnp.dot(prob, vz[hh], preferred_element_type=F32)
                    out = part if out is None else out + part
                ob[rows, cols] = out.astype(BF16)
                return 0
            lax.fori_loop(0, FRAMES // QROWS, attend, 0)
            return 0
        lax.fori_loop(0, 4, pair, 0)

    own = pl.ds(k * HALF, HALF)
    oth = pl.ds(ks * HALF, HALF)

    def swap_partials(phase, j, lhs, weight):
        for n in range(2):
            cols = slice(n * 512, (n + 1) * 512)
            ex_s[j, :, cols] = jnp.dot(lhs[oth, :], weight[:, cols], preferred_element_type=F32).astype(BF16)
        cp = remote(ex_s.at[j], ex_r.at[j], ex_ss.at[phase, j], ex_rs.at[phase, j], sib)
        cp.start()
        for n in range(2):
            cols = slice(n * 512, (n + 1) * 512)
            acc[:, cols] = jnp.dot(lhs[own, :], weight[:, cols], preferred_element_type=F32)
        wait_recv(ex_r.at[j], ex_rs.at[phase, j])
        cp.wait_send()

    m_sends = []

    def output_stage(j):
        swap_partials(0, j, ob, wo)
        a_sends[j].wait_send()

        def body(b, _):
            rows = pl.ds(b * FR, FR)
            out = (acc[rows, :] + ex_r[j, rows, :].astype(F32) + row(bo_v)).astype(BF16)
            h = (xb[j, rows, :].astype(F32) + out.astype(F32)).astype(BF16)
            xb[j, rows, :] = h
            am[j, k, b] = ln_rows(h.astype(F32), row(ln2g), row(ln2b))
            return 0
        lax.fori_loop(0, 4, body, 0)
        cp = remote(am.at[j, k], am.at[j, k], am_s.at[1, j], am_r.at[1, j], sib)
        cp.start()
        m_sends.append(cp)

    def epiece(group, j, core, hf):
        if group == 3:
            return am.at[j, core, pl.ds(2 * hf, 2)]
        return ea.at[3 * group + j, pl.ds(2 * hf, 2), core]

    def mlp_stage(j):
        wait_recv(am.at[j, ks], am_r.at[1, j])
        if j == 0:
            wait_rest(4)

        def up(i, _):
            n, r = i // 2, i % 2
            rows = pl.ds(r * HALF, HALF)
            cols = pl.ds(pl.multiple_of(n * HID, HID), HID)
            b1 = jnp.concatenate([bias[n, 2 + q:3 + q, :] for q in range(4)], axis=1)
            u = jnp.dot(am[j, r].reshape(HALF, D), w1[:, cols], preferred_element_type=F32) + b1
            g[rows, cols] = (0.5 * u * (1.0 + lax.erf(u * (2.0 ** -0.5)))).astype(BF16)
            return 0
        lax.fori_loop(0, 8, up, 0)
        m_sends[j].wait_send()
        for peer in (sib, xn, yn):
            pl.semaphore_signal(free.at[j], inc=1, device_id={"tp": peer}, device_id_type=pl.DeviceIdType.MESH)
        if j == 0:
            wait_rest(5)
        swap_partials(1, j, g, w2)

        def post(b, _):
            rows = pl.ds(b * FR, FR)
            out = (acc[rows, :] + ex_r[j, rows, :].astype(F32) + row(bfc2)).astype(BF16)
            h2 = (xb[j, rows, :].astype(F32) + out.astype(F32)).astype(BF16)
            ea[j, b, k] = ln_rows(h2.astype(F32), row(postg), row(postb))
            return 0
        lax.fori_loop(0, 4, post, 0)
        for hf in range(2):
            go(epiece(0, j, k, hf), epiece(1, j, k, hf), es_x.at[j, hf], ex_x.at[j, hf], xn)
            go(epiece(0, j, k, 1 - hf), epiece(2, j, k, 1 - hf), es_y.at[j, 1 - hf], ex_y.at[j, 1 - hf], yn)
        for hf in range(2):
            go(epiece(0, j, k, hf), epiece(0, j, k, hf), es_f.at[0, j, hf], ex_f.at[0, j, hf], sib)

    def forward(group, j, hf):
        go(epiece(group, j, k, hf), epiece(group, j, k, hf), es_f.at[group, j, hf], ex_f.at[group, j, hf], sib)

    def relay_e(j):
        pl.semaphore_wait(free.at[j], 3)
        wait_recv(epiece(1, j, k, 0), ex_x.at[j, 0])
        go(epiece(1, j, k, 0), epiece(3, j, k, 0), es_d.at[j, 0], ex_d.at[j, 0], yn)
        forward(1, j, 0)
        wait_recv(epiece(2, j, k, 1), ex_y.at[j, 1])
        go(epiece(2, j, k, 1), epiece(3, j, k, 1), es_d.at[j, 1], ex_d.at[j, 1], xn)
        forward(2, j, 1)
        wait_recv(epiece(1, j, k, 1), ex_x.at[j, 1])
        forward(1, j, 1)
        wait_recv(epiece(2, j, k, 0), ex_y.at[j, 0])
        forward(2, j, 0)

    def take_diagonal(j):
        for hf in range(2):
            wait_recv(epiece(3, j, k, hf), ex_d.at[j, hf])
            forward(3, j, hf)

    def write_caches(clip, ec):
        for i in range(4):
            r = lax.dot_general(wct[i], ec, (((0,), (1,)), ((), ())), preferred_element_type=F32)
            if i >= 2:
                r = r + jnp.concatenate([bct[i - 2]] * 6, axis=1)
            (kc_o, vc_o)[i // 2][i % 2, clip] = r.astype(BF16)

    def near_cache(group, j):
        chip = jnp.where(group == 0, c, jnp.where(group == 1, cxn, cyn))
        clip = chip * PER_CHIP + j
        for hf in range(2):
            wait_recv(ea.at[3 * group + j, pl.ds(2 * hf, 2), ks], ex_f.at[group, j, hf])
        enc_o[clip] = ea[3 * group + j, c, k]
        write_caches(clip, ea[3 * group + j].reshape(FRAMES, D))

    def far_cache(j, _):
        clip = cdg * PER_CHIP + j
        for hf in range(2):
            wait_recv(epiece(3, j, ks, hf), ex_f.at[3, j, hf])
        enc_o[clip] = am[j, k, c]
        write_caches(clip, jnp.concatenate([am[j, core, b] for b in range(4) for core in range(2)], axis=0))
        return 0

    attention_stage(0)
    wait_rest(3)
    output_stage(0)
    attention_stage(1)
    relay(4)
    output_stage(1)
    relay(5)
    send_x(1)
    mlp_stage(0)
    mlp_stage(1)
    wait_x(1)
    ln1_stage(2)
    attention_stage(2)
    relay_e(0)
    output_stage(2)
    mlp_stage(2)
    relay_e(1)

    def first(i, _):
        near_cache(jnp.where(i < 3, 0, 1 + (i + 1) % 2), jnp.where(i < 3, i, (i - 3) // 2))
        return 0
    lax.fori_loop(0, 7, first, 0)
    take_diagonal(0)
    far_cache(0, 0)
    relay_e(2)

    def second(i, _):
        near_cache(1 + i, 2)
        return 0
    lax.fori_loop(0, 2, second, 0)
    take_diagonal(1)
    take_diagonal(2)
    lax.fori_loop(1, 3, far_cache, 0)
    for cp in sends:
        cp.wait_send()


def device_body(hidden_loc, ln1_gain, ln1_bias, w_q, b_q, w_k, w_v, b_v, w_o, b_o, ln2_gain, ln2_bias, w_fc1, b_fc1, w_fc2, b_fc2, post_gain, post_bias, w_ck, w_cv, b_cv):
    anyspec = pl.BlockSpec(memory_space=pl.ANY)
    vspec = pl.BlockSpec(memory_space=pltpu.VMEM)
    dma = pltpu.SemaphoreType.DMA
    cache = pltpu.VMEM((2, CLIPS, LOC, FRAMES), BF16)
    enc, kc, vc = pl.pallas_call(
        kernel,
        out_shape=(pltpu.VMEM((CLIPS, FR, D), BF16), cache, cache),
        in_specs=[anyspec] * 9 + [vspec] * 12,
        out_specs=(vspec, vspec, vspec),
        scratch_shapes=[
            pltpu.VMEM((PER_CHIP, HALF, D), BF16),
            pltpu.VMEM((PER_CHIP, 2, 4, FR, D), BF16),
            pltpu.VMEM((PER_CHIP, HALF, D), BF16),
            pltpu.VMEM((PER_CHIP, HALF, D), BF16),
            pltpu.VMEM((3, D, NQ), BF16),
            pltpu.VMEM((NQ, D), BF16),
            pltpu.VMEM((D, NH), BF16),
            pltpu.VMEM((NH, D), BF16),
            pltpu.VMEM((4, 8, LOC), F32),
            pltpu.VMEM((3, FRAMES, NQ), BF16),
            pltpu.VMEM((2, FRAMES, LOC), BF16),
            pltpu.VMEM((2, FRAMES, LOC), BF16),
            pltpu.VMEM((FRAMES, NQ), BF16),
            pltpu.VMEM((FRAMES, NH), BF16),
            pltpu.VMEM((HALF, D), F32),
            pltpu.VMEM((4, D, LOC), BF16),
            pltpu.VMEM((2, LOC, LOC), F32),
            pltpu.VMEM((9, 4, 2, FR, D), BF16),
            dma((2, 4)), dma((2, 3)), dma((6, 5)), dma((6, 4)), dma((3,)), dma((3,)),
            dma((2, 3)), dma((2, 3)), dma((2, 3)), dma((2, 3)),
            dma((3, 2)), dma((3, 2)), dma((3, 2)), dma((4, 3, 2)),
            dma((3, 2)), dma((3, 2)), dma((3, 2)), dma((4, 3, 2)),
            dma((4,)), pltpu.SemaphoreType.REGULAR((3,)),
        ],
        compiler_params=pltpu.CompilerParams(collective_id=0, has_side_effects=True, vmem_limit_bytes=55000000),
        name="encoder_layer",
    )(hidden_loc, w_q, w_k, w_v, w_o, w_fc1, w_fc2, w_ck, w_cv,
      b_q, b_v, b_fc1, b_cv, ln1_gain, ln1_bias, ln2_gain, ln2_bias, post_gain, post_bias, b_o, b_fc2)

    def heads_last(cached):
        return cached.reshape(2, CLIPS, LOC // HEAD_DIM, HEAD_DIM, FRAMES).transpose(0, 1, 4, 2, 3)
    return enc, heads_last(kc), heads_last(vc)


def solution(mesh):
    in_specs = (P("dp", "tp", None), P(), P(), P(None, "tp"), P("tp"), P(None, "tp"), P(None, "tp"), P("tp"), P("tp", None), P(), P(), P(), P(None, "tp"), P("tp"), P("tp", None), P(), P(), P(), P(None, None, "tp"), P(None, None, "tp"), P(None, "tp"))
    out_specs = (P("dp", "tp", None), P(None, "dp", None, "tp", None), P(None, "dp", None, "tp", None))
    return jax.shard_map(device_body, mesh=mesh, in_specs=in_specs, out_specs=out_specs, check_vma=False)
```

```python
import functools

import jax
import jax.numpy as jnp
from jax import lax
from jax.experimental import pallas as pl
from jax.experimental.pallas import tpu as pltpu
from jax.sharding import PartitionSpec as P

HEAD_DIM = 64
ATTN_SCALE = HEAD_DIM ** -0.25
LN_EPS = 1e-5
CLIPS = 12
PER_CHIP = 3
FR = 96
HALF = 4 * FR
FRAMES = 8 * FR
D = 1024
LOC = 128
HID = 512
NQ = 4 * LOC
NH = 4 * HID
QROWS = 256
F32, BF16 = jnp.float32, jnp.bfloat16


def ln_rows(values, gain, bias):
    centered = values - jnp.mean(values, axis=-1, keepdims=True)
    row_var = jnp.mean(centered * centered, axis=-1, keepdims=True)
    return (centered * lax.rsqrt(row_var + LN_EPS) * gain + bias).astype(BF16)


def kernel(hid, wq_h, wk_h, wv_h, wo_h, w1_h, w2_h, ck_h, cv_h,
           bq_v, bv_v, b1_v, bcv_v, ln1g, ln1b, ln2g, ln2b, postg, postb, bo_v, bfc2,
           enc_o, kc_o, vc_o, am, wct, bct,
           xb, ex_s, ex_r, wqkv, wo, w1, w2, bias, qkv, kz, vz, ob, g, acc, wc, ea,
           x_r, x_s, w_r, w_s, b_r, b_s, am_r, am_s, ex_rs, ex_ss, ex_x, ex_y, ex_d, ex_f, es_x, es_y, es_d, es_f, c_s, free):
    t = lax.axis_index("tp")
    c, k = t // 2, t % 2
    cx, cy = c % 2, c // 2
    cxn = 2 * cy + (1 - cx)
    cyn = 2 * (1 - cy) + cx
    cdg = 2 * (1 - cy) + (1 - cx)
    ks = 1 - k
    sib, xn, yn, dg = 2 * c + ks, 2 * cxn + k, 2 * cyn + k, 2 * cdg + k

    def remote(src, dst, ssem, rsem, dev):
        return pltpu.make_async_remote_copy(src_ref=src, dst_ref=dst, send_sem=ssem, recv_sem=rsem,
                                            device_id={"tp": dev}, device_id_type=pl.DeviceIdType.MESH)

    def wait_recv(ref, rsem):
        pltpu.make_async_copy(ref, ref, rsem).wait()

    def row(ref):
        return ref[...].astype(F32).reshape(1, ref.shape[0])

    bias[c, 0:1, :] = row(bq_v)
    bias[c, 1:2, :] = row(bv_v)
    b1_row = row(b1_v)
    for q in range(4):
        bias[c, 2 + q:3 + q, :] = b1_row[:, q * LOC:(q + 1) * LOC]
    for l in range(2):
        bct[l] = jnp.transpose(jnp.broadcast_to(bcv_v[l:l + 1, :].astype(F32), (LOC, LOC)))

    barrier = pltpu.get_barrier_semaphore()
    for peer in (sib, xn, yn, dg):
        pl.semaphore_signal(barrier, inc=1, device_id={"tp": peer}, device_id_type=pl.DeviceIdType.MESH)
    pl.semaphore_wait(barrier, 4)

    def xslot(chip, late):
        return xb.at[pl.ds(2, 1) if late else pl.ds(0, 2), pl.ds(chip * FR, FR), :]

    def xsource(chip, late):
        return hid.at[pl.ds(chip * PER_CHIP + 2, 1) if late else pl.ds(chip * PER_CHIP, 2)]

    def wfull(i, chip):
        if i < 3:
            return wqkv.at[i, :, pl.ds(pl.multiple_of(chip * LOC, LOC), LOC)]
        if i == 3:
            return wo.at[pl.ds(chip * LOC, LOC)]
        if i == 4:
            return w1.at[:, pl.ds(pl.multiple_of(chip * HID, HID), HID)]
        return w2.at[pl.ds(chip * HID, HID)]

    def whalf(i, chip, hf):
        if i < 3:
            return wqkv.at[i, pl.ds(hf * (D // 2), D // 2), pl.ds(pl.multiple_of(chip * LOC, LOC), LOC)]
        if i == 3:
            return wo.at[pl.ds(chip * LOC + hf * (LOC // 2), LOC // 2)]
        if i == 4:
            return w1.at[pl.ds(hf * (D // 2), D // 2), pl.ds(pl.multiple_of(chip * HID, HID), HID)]
        return w2.at[pl.ds(chip * HID + hf * (HID // 2), HID // 2)]

    w_hbm = (wq_h, wk_h, wv_h, wo_h, w1_h, w2_h)
    sends = []

    def go(src, dst, ssem, rsem, dev):
        cp = remote(src, dst, ssem, rsem, dev)
        cp.start()
        sends.append(cp)

    def send_direct(i):
        go(w_hbm[i], wfull(i, c), w_s.at[i, 0], w_r.at[i, 1], xn)
        go(w_hbm[i], wfull(i, c), w_s.at[i, 1], w_r.at[i, 2], yn)

    def relay(i):
        wait_recv(wfull(i, cxn), w_r.at[i, 1])
        go(whalf(i, cxn, 0), whalf(i, cxn, 0), w_s.at[i, 2], w_r.at[i, 3], yn)
        wait_recv(wfull(i, cyn), w_r.at[i, 2])
        go(whalf(i, cyn, 1), whalf(i, cyn, 1), w_s.at[i, 3], w_r.at[i, 4], xn)

    def wait_rest(i):
        wait_recv(wfull(i, c), w_r.at[i, 0])
        wait_recv(whalf(i, cdg, 0), w_r.at[i, 3])
        wait_recv(whalf(i, cdg, 1), w_r.at[i, 4])

    def send_x(late):
        for r, (dev, chip) in ((2, (dg, cdg)), (0, (xn, cxn)), (1, (yn, cyn))):
            go(xsource(chip, late), xslot(c, late), x_s.at[late, r], x_r.at[late, 1 + r], dev)

    def ln1_stage(j):
        def body(b, _):
            vals = xb[j, pl.ds(b * FR, FR), :].astype(F32)
            am[j, k, b] = ln_rows(vals, row(ln1g), row(ln1b))
            return 0
        lax.fori_loop(0, 4, body, 0)
        cp = remote(am.at[j, k], am.at[j, k], am_s.at[0, j], am_r.at[0, j], sib)
        cp.start()
        a_sends.append(cp)

    def wait_x(late):
        for r, chip in ((0, c), (1, cxn), (2, cyn), (3, cdg)):
            wait_recv(xslot(chip, late), x_r.at[late, r])

    for r, dev in enumerate((xn, yn, dg)):
        go(bias.at[c], bias.at[c], b_s.at[r], b_r.at[r], dev)
    send_x(0)
    for i in range(3):
        send_direct(i)
    for late in range(2):
        pltpu.make_async_copy(xsource(c, late), xslot(c, late), x_r.at[late, 0]).start()
    wc_copies = []
    for i, src in enumerate((ck_h.at[0], ck_h.at[1], cv_h.at[0], cv_h.at[1])):
        cp = pltpu.make_async_copy(src, wc.at[i], c_s.at[i])
        cp.start()
        wc_copies.append(cp)
    for i in range(6):
        pltpu.make_async_copy(w_hbm[i], wfull(i, c), w_r.at[i, 0]).start()

    a_sends = []
    wait_x(0)
    for j in range(2):
        ln1_stage(j)
    send_direct(3)
    for cp in wc_copies:
        cp.wait()
    for i in range(4):
        wct[i * LOC:(i + 1) * LOC, :] = jnp.transpose(wc[i])
    for r, chip in enumerate((cxn, cyn, cdg)):
        wait_recv(bias.at[chip], b_r.at[r])
    for i in range(4):
        relay(i)
    send_direct(4)
    send_direct(5)
    for i in range(3):
        wait_rest(i)

    def row_of(r):
        return jnp.concatenate([bias[n, r:r + 1, :] for n in range(4)], axis=1)

    lane = lax.broadcasted_iota(jnp.int32, (FRAMES, LOC), 1)

    def attention_stage(j):
        wait_recv(am.at[j, ks], am_r.at[0, j])
        bq, bv = row_of(0), row_of(1)

        def project(r, _):
            rows = pl.ds(r * HALF, HALF)
            a = am[j, r].reshape(HALF, D)
            qkv[0, rows, :] = ((jnp.dot(a, wqkv[0], preferred_element_type=F32) + bq) * ATTN_SCALE).astype(BF16)
            qkv[1, rows, :] = (jnp.dot(a, wqkv[1], preferred_element_type=F32) * ATTN_SCALE).astype(BF16)
            qkv[2, rows, :] = (jnp.dot(a, wqkv[2], preferred_element_type=F32) + bv).astype(BF16)
            return 0
        lax.fori_loop(0, 2, project, 0)

        def pair(p, _):
            cols = pl.ds(pl.multiple_of(p * LOC, LOC), LOC)
            kp, vp = qkv[1, :, cols], qkv[2, :, cols]
            zero = jnp.zeros_like(kp)
            kz[0] = jnp.where(lane < HEAD_DIM, kp, zero)
            kz[1] = jnp.where(lane < HEAD_DIM, zero, kp)
            vz[0] = jnp.where(lane < HEAD_DIM, vp, zero)
            vz[1] = jnp.where(lane < HEAD_DIM, zero, vp)

            def attend(r, _):
                rows = pl.ds(r * QROWS, QROWS)
                qb = qkv[0, rows, cols]
                out = None
                for hh in range(2):
                    s = lax.dot_general(qb, kz[hh], (((1,), (1,)), ((), ())), preferred_element_type=F32)
                    e = jnp.exp(s - jnp.max(s, axis=-1, keepdims=True))
                    prob = (e * (1.0 / jnp.sum(e, axis=-1, keepdims=True))).astype(BF16)
                    part = jnp.dot(prob, vz[hh], preferred_element_type=F32)
                    out = part if out is None else out + part
                ob[rows, cols] = out.astype(BF16)
                return 0
            lax.fori_loop(0, FRAMES // QROWS, attend, 0)
            return 0
        lax.fori_loop(0, 4, pair, 0)

    own = pl.ds(k * HALF, HALF)
    oth = pl.ds(ks * HALF, HALF)

    def swap_partials(phase, j, lhs, weight):
        for n in range(2):
            cols = slice(n * 512, (n + 1) * 512)
            ex_s[j, :, cols] = jnp.dot(lhs[oth, :], weight[:, cols], preferred_element_type=F32).astype(BF16)
        cp = remote(ex_s.at[j], ex_r.at[j], ex_ss.at[phase, j], ex_rs.at[phase, j], sib)
        cp.start()
        for n in range(2):
            cols = slice(n * 512, (n + 1) * 512)
            acc[:, cols] = jnp.dot(lhs[own, :], weight[:, cols], preferred_element_type=F32)
        wait_recv(ex_r.at[j], ex_rs.at[phase, j])
        cp.wait_send()

    m_sends = []

    def output_stage(j):
        swap_partials(0, j, ob, wo)
        a_sends[j].wait_send()

        def body(b, _):
            rows = pl.ds(b * FR, FR)
            out = (acc[rows, :] + ex_r[j, rows, :].astype(F32) + row(bo_v)).astype(BF16)
            h = (xb[j, rows, :].astype(F32) + out.astype(F32)).astype(BF16)
            xb[j, rows, :] = h
            am[j, k, b] = ln_rows(h.astype(F32), row(ln2g), row(ln2b))
            return 0
        lax.fori_loop(0, 4, body, 0)
        cp = remote(am.at[j, k], am.at[j, k], am_s.at[1, j], am_r.at[1, j], sib)
        cp.start()
        m_sends.append(cp)

    def epiece(group, j, core, hf):
        if group == 3:
            return am.at[j, core, pl.ds(2 * hf, 2)]
        return ea.at[3 * group + j, pl.ds(2 * hf, 2), core]

    def mlp_stage(j):
        wait_recv(am.at[j, ks], am_r.at[1, j])
        if j == 0:
            wait_rest(4)

        def up(i, _):
            n, r = i // 2, i % 2
            rows = pl.ds(r * HALF, HALF)
            cols = pl.ds(pl.multiple_of(n * HID, HID), HID)
            b1 = jnp.concatenate([bias[n, 2 + q:3 + q, :] for q in range(4)], axis=1)
            u = jnp.dot(am[j, r].reshape(HALF, D), w1[:, cols], preferred_element_type=F32) + b1
            g[rows, cols] = (0.5 * u * (1.0 + lax.erf(u * (2.0 ** -0.5)))).astype(BF16)
            return 0
        lax.fori_loop(0, 8, up, 0)
        m_sends[j].wait_send()
        for peer in (sib, xn, yn):
            pl.semaphore_signal(free.at[j], inc=1, device_id={"tp": peer}, device_id_type=pl.DeviceIdType.MESH)
        if j == 0:
            wait_rest(5)
        swap_partials(1, j, g, w2)

        def post(b, _):
            rows = pl.ds(b * FR, FR)
            out = (acc[rows, :] + ex_r[j, rows, :].astype(F32) + row(bfc2)).astype(BF16)
            h2 = (xb[j, rows, :].astype(F32) + out.astype(F32)).astype(BF16)
            ea[j, b, k] = ln_rows(h2.astype(F32), row(postg), row(postb))
            return 0
        lax.fori_loop(0, 4, post, 0)
        for hf in range(2):
            go(epiece(0, j, k, hf), epiece(1, j, k, hf), es_x.at[j, hf], ex_x.at[j, hf], xn)
            go(epiece(0, j, k, 1 - hf), epiece(2, j, k, 1 - hf), es_y.at[j, 1 - hf], ex_y.at[j, 1 - hf], yn)
        for hf in range(2):
            go(epiece(0, j, k, hf), epiece(0, j, k, hf), es_f.at[0, j, hf], ex_f.at[0, j, hf], sib)

    def forward(group, j, hf):
        go(epiece(group, j, k, hf), epiece(group, j, k, hf), es_f.at[group, j, hf], ex_f.at[group, j, hf], sib)

    def relay_e(j):
        pl.semaphore_wait(free.at[j], 3)
        wait_recv(epiece(1, j, k, 0), ex_x.at[j, 0])
        go(epiece(1, j, k, 0), epiece(3, j, k, 0), es_d.at[j, 0], ex_d.at[j, 0], yn)
        forward(1, j, 0)
        wait_recv(epiece(2, j, k, 1), ex_y.at[j, 1])
        go(epiece(2, j, k, 1), epiece(3, j, k, 1), es_d.at[j, 1], ex_d.at[j, 1], xn)
        forward(2, j, 1)
        wait_recv(epiece(1, j, k, 1), ex_x.at[j, 1])
        forward(1, j, 1)
        wait_recv(epiece(2, j, k, 0), ex_y.at[j, 0])
        forward(2, j, 0)

    def take_diagonal(j):
        for hf in range(2):
            wait_recv(epiece(3, j, k, hf), ex_d.at[j, hf])
            forward(3, j, hf)

    def write_caches(clip, ec):
        cache_rows(clip, ec, wct, bct, kc_o, vc_o)

    def near_cache(group, j):
        chip = jnp.where(group == 0, c, jnp.where(group == 1, cxn, cyn))
        clip = chip * PER_CHIP + j
        for hf in range(2):
            wait_recv(ea.at[3 * group + j, pl.ds(2 * hf, 2), ks], ex_f.at[group, j, hf])
        enc_o[clip] = ea[3 * group + j, c, k]
        write_caches(clip, ea[3 * group + j].reshape(FRAMES, D))

    def far_cache(j):
        clip = cdg * PER_CHIP + j
        for hf in range(2):
            wait_recv(epiece(3, j, ks, hf), ex_f.at[3, j, hf])
        enc_o[clip] = am[j, k, c]
        write_caches(clip, natural_order(am, j))

    attention_stage(0)
    wait_rest(3)
    output_stage(0)
    attention_stage(1)
    relay(4)
    output_stage(1)
    relay(5)
    send_x(1)
    mlp_stage(0)
    mlp_stage(1)
    wait_x(1)
    ln1_stage(2)
    attention_stage(2)
    relay_e(0)
    output_stage(2)
    mlp_stage(2)
    relay_e(1)

    def first(i, _):
        near_cache(jnp.where(i < 3, 0, 1 + (i + 1) % 2), jnp.where(i < 3, i, (i - 3) // 2))
        return 0
    lax.fori_loop(0, 7, first, 0)
    take_diagonal(0)
    far_cache(0)
    relay_e(2)

    def second(i, _):
        near_cache(1 + i, 2)
        return 0
    lax.fori_loop(0, 2, second, 0)
    take_diagonal(1)
    far_cache(1)
    take_diagonal(2)
    for hf in range(2):
        wait_recv(epiece(3, 2, ks, hf), ex_f.at[3, 2, hf])
    for cp in sends:
        cp.wait_send()


def natural_order(am, j):
    return jnp.concatenate([am[j, core, b] for b in range(4) for core in range(2)], axis=0)


def cache_rows(clip, ec, wct, bct, k_ref, v_ref):
    r = lax.dot_general(wct[...], ec, (((1,), (1,)), ((), ())), preferred_element_type=F32)
    for i in range(4):
        part = r[i * LOC:(i + 1) * LOC, :]
        if i >= 2:
            part = part + jnp.concatenate([bct[i - 2]] * 6, axis=1)
        (k_ref, v_ref)[i // 2][i % 2, clip] = part.astype(BF16)


def writer(enc_v, kc_v, vc_v, am, wct, bct, enc_o, kc_o, vc_o, kl, vl, sem, last_sem):
    t = lax.axis_index("tp")
    c, k = t // 2, t % 2
    cx, cy = c % 2, c // 2
    cdg = 2 * (1 - cy) + (1 - cx)
    last = cdg * PER_CHIP + 2

    def copies(clip):
        cps = [pltpu.make_async_copy(kc_v.at[l, clip], kc_o.at[l, clip], sem) for l in range(2)]
        cps += [pltpu.make_async_copy(vc_v.at[l, clip], vc_o.at[l, clip], sem) for l in range(2)]
        return cps + [pltpu.make_async_copy(enc_v.at[clip], enc_o.at[clip], sem)]

    def start(i, _):
        for cp in copies(lax.rem(last + 1 + i, CLIPS)):
            cp.start()
        return 0
    lax.fori_loop(0, CLIPS - 1, start, 0)
    cps = [pltpu.make_async_copy(am.at[2, k, c], enc_o.at[last], last_sem)]
    cps[0].start()
    cache_rows(0, natural_order(am, 2), wct, bct, kl, vl)
    for l in range(2):
        cps.append(pltpu.make_async_copy(kl.at[l, 0], kc_o.at[l, last], last_sem))
        cps.append(pltpu.make_async_copy(vl.at[l, 0], vc_o.at[l, last], last_sem))
    for cp in cps[1:]:
        cp.start()

    def finish(i, _):
        for cp in copies(lax.rem(last + 1 + i, CLIPS)):
            cp.wait()
        return 0
    lax.fori_loop(0, CLIPS - 1, finish, 0)
    for cp in cps:
        cp.wait()


def device_body(hidden_loc, ln1_gain, ln1_bias, w_q, b_q, w_k, w_v, b_v, w_o, b_o, ln2_gain, ln2_bias, w_fc1, b_fc1, w_fc2, b_fc2, post_gain, post_bias, w_ck, w_cv, b_cv):
    anyspec = pl.BlockSpec(memory_space=pl.ANY)
    vspec = pl.BlockSpec(memory_space=pltpu.VMEM)
    dma = pltpu.SemaphoreType.DMA
    cache = (2, CLIPS, LOC, FRAMES)
    parts = pl.pallas_call(
        kernel,
        out_shape=(
            pltpu.VMEM((CLIPS, FR, D), BF16), pltpu.VMEM(cache, BF16), pltpu.VMEM(cache, BF16),
            pltpu.VMEM((PER_CHIP, 2, 4, FR, D), BF16),
            pltpu.VMEM((4 * LOC, D), BF16),
            pltpu.VMEM((2, LOC, LOC), F32),
        ),
        in_specs=[anyspec] * 9 + [vspec] * 12,
        out_specs=(vspec,) * 6,
        scratch_shapes=[
            pltpu.VMEM((PER_CHIP, HALF, D), BF16),
            pltpu.VMEM((PER_CHIP, HALF, D), BF16),
            pltpu.VMEM((PER_CHIP, HALF, D), BF16),
            pltpu.VMEM((3, D, NQ), BF16),
            pltpu.VMEM((NQ, D), BF16),
            pltpu.VMEM((D, NH), BF16),
            pltpu.VMEM((NH, D), BF16),
            pltpu.VMEM((4, 8, LOC), F32),
            pltpu.VMEM((3, FRAMES, NQ), BF16),
            pltpu.VMEM((2, FRAMES, LOC), BF16),
            pltpu.VMEM((2, FRAMES, LOC), BF16),
            pltpu.VMEM((FRAMES, NQ), BF16),
            pltpu.VMEM((FRAMES, NH), BF16),
            pltpu.VMEM((HALF, D), F32),
            pltpu.VMEM((4, D, LOC), BF16),
            pltpu.VMEM((9, 4, 2, FR, D), BF16),
            dma((2, 4)), dma((2, 3)), dma((6, 5)), dma((6, 4)), dma((3,)), dma((3,)),
            dma((2, 3)), dma((2, 3)), dma((2, 3)), dma((2, 3)),
            dma((3, 2)), dma((3, 2)), dma((3, 2)), dma((4, 3, 2)),
            dma((3, 2)), dma((3, 2)), dma((3, 2)), dma((4, 3, 2)),
            dma((4,)), pltpu.SemaphoreType.REGULAR((3,)),
        ],
        compiler_params=pltpu.CompilerParams(collective_id=0, has_side_effects=True, vmem_limit_bytes=48500000),
        name="encoder_layer",
    )(hidden_loc, w_q, w_k, w_v, w_o, w_fc1, w_fc2, w_ck, w_cv,
      b_q, b_v, b_fc1, b_cv, ln1_gain, ln1_bias, ln2_gain, ln2_bias, post_gain, post_bias, b_o, b_fc2)

    enc, kc, vc = pl.pallas_call(
        writer,
        out_shape=(jax.ShapeDtypeStruct((CLIPS, FR, D), BF16), jax.ShapeDtypeStruct(cache, BF16), jax.ShapeDtypeStruct(cache, BF16)),
        in_specs=[vspec] * 6,
        out_specs=(anyspec,) * 3,
        scratch_shapes=[pltpu.VMEM((2, 1, LOC, FRAMES), BF16), pltpu.VMEM((2, 1, LOC, FRAMES), BF16), dma, dma],
        compiler_params=pltpu.CompilerParams(vmem_limit_bytes=8000000),
        name="writer",
    )(*parts)

    def heads_last(cached):
        return cached.reshape(2, CLIPS, LOC // HEAD_DIM, HEAD_DIM, FRAMES).transpose(0, 1, 4, 2, 3)
    return enc, heads_last(kc), heads_last(vc)


def solution(mesh):
    in_specs = (P("dp", "tp", None), P(), P(), P(None, "tp"), P("tp"), P(None, "tp"), P(None, "tp"), P("tp"), P("tp", None), P(), P(), P(), P(None, "tp"), P("tp"), P("tp", None), P(), P(), P(), P(None, None, "tp"), P(None, None, "tp"), P(None, "tp"))
    out_specs = (P("dp", "tp", None), P(None, "dp", None, "tp", None), P(None, "dp", None, "tp", None))
    return jax.shard_map(device_body, mesh=mesh, in_specs=in_specs, out_specs=out_specs, check_vma=False)
```

```python
import functools

import jax
import jax.numpy as jnp
from jax import lax
from jax.experimental import pallas as pl
from jax.experimental.pallas import tpu as pltpu
from jax.sharding import PartitionSpec as P

HEAD_DIM = 64
ATTN_SCALE = HEAD_DIM ** -0.25
LN_EPS = 1e-5
CLIPS = 12
PER_CHIP = 3
FR = 96
HALF = 4 * FR
FRAMES = 8 * FR
D = 1024
LOC = 128
HID = 512
NQ = 4 * LOC
NH = 4 * HID
QROWS = 256
F32, BF16 = jnp.float32, jnp.bfloat16


def ln_rows(values, gain, bias):
    centered = values - jnp.mean(values, axis=-1, keepdims=True)
    row_var = jnp.mean(centered * centered, axis=-1, keepdims=True)
    return (centered * lax.rsqrt(row_var + LN_EPS) * gain + bias).astype(BF16)


def kernel(hid, wq_h, wk_h, wv_h, wo_h, w1_h, w2_h, ck_h, cv_h,
           bq_v, bv_v, b1_v, bcv_v, ln1g, ln1b, ln2g, ln2b, postg, postb, bo_v, bfc2,
           enc_o, kc_o, vc_o, am, wct, bct,
           xb, xrel, ex_s, ex_r, wqkv, wo, w1, w2, bias, qkv, kz, vz, g, acc, ea,
           x_r, x_s, xrel_r, w_r, w_s, b_r, b_s, am_r, am_s, ex_rs, ex_ss, ex_x, ex_y, ex_d, ex_f, es_x, es_y, es_d, es_f, c_s, free):
    t = lax.axis_index("tp")
    c, k = t // 2, t % 2
    cx, cy = c % 2, c // 2
    cxn = 2 * cy + (1 - cx)
    cyn = 2 * (1 - cy) + cx
    cdg = 2 * (1 - cy) + (1 - cx)
    ks = 1 - k
    sib, xn, yn, dg = 2 * c + ks, 2 * cxn + k, 2 * cyn + k, 2 * cdg + k

    def remote(src, dst, ssem, rsem, dev):
        return pltpu.make_async_remote_copy(src_ref=src, dst_ref=dst, send_sem=ssem, recv_sem=rsem,
                                            device_id={"tp": dev}, device_id_type=pl.DeviceIdType.MESH)

    def wait_recv(ref, rsem):
        pltpu.make_async_copy(ref, ref, rsem).wait()

    def row(ref):
        return ref[...].astype(F32).reshape(1, ref.shape[0])

    barrier = pltpu.get_barrier_semaphore()
    for peer in (sib, xn, yn, dg):
        pl.semaphore_signal(barrier, inc=1, device_id={"tp": peer}, device_id_type=pl.DeviceIdType.MESH)
    pl.semaphore_wait(barrier, 4)

    def xclips(late):
        return pl.ds(2, 1) if late else pl.ds(0, 2)

    def xslot(chip, late):
        return xb.at[xclips(late), pl.ds(chip * FR, FR), :]

    def xhalf(chip, late, hf):
        return xb.at[xclips(late), pl.ds(chip * FR + hf * (FR // 2), FR // 2), :]

    def xsource(chip, late):
        return hid.at[pl.ds(chip * PER_CHIP + 2, 1) if late else pl.ds(chip * PER_CHIP, 2)]

    def wfull(i, chip):
        if i < 3:
            return wqkv.at[i, :, pl.ds(pl.multiple_of(chip * LOC, LOC), LOC)]
        if i == 3:
            return wo.at[pl.ds(chip * LOC, LOC)]
        if i == 4:
            return w1.at[:, pl.ds(pl.multiple_of(chip * HID, HID), HID)]
        return w2.at[pl.ds(chip * HID, HID)]

    def whalf(i, chip, hf):
        if i < 3:
            return wqkv.at[i, pl.ds(hf * (D // 2), D // 2), pl.ds(pl.multiple_of(chip * LOC, LOC), LOC)]
        if i == 3:
            return wo.at[pl.ds(chip * LOC + hf * (LOC // 2), LOC // 2)]
        if i == 4:
            return w1.at[pl.ds(hf * (D // 2), D // 2), pl.ds(pl.multiple_of(chip * HID, HID), HID)]
        return w2.at[pl.ds(chip * HID + hf * (HID // 2), HID // 2)]

    w_hbm = (wq_h, wk_h, wv_h, wo_h, w1_h, w2_h)
    sends = []

    def go(src, dst, ssem, rsem, dev):
        cp = remote(src, dst, ssem, rsem, dev)
        cp.start()
        sends.append(cp)

    def send_direct(i):
        wait_recv(wfull(i, c), w_r.at[i, 0])
        go(wfull(i, c), wfull(i, c), w_s.at[i, 0], w_r.at[i, 1], xn)
        go(wfull(i, c), wfull(i, c), w_s.at[i, 1], w_r.at[i, 2], yn)

    def relay(i):
        wait_recv(wfull(i, cxn), w_r.at[i, 1])
        go(whalf(i, cxn, 0), whalf(i, cxn, 0), w_s.at[i, 2], w_r.at[i, 3], yn)
        wait_recv(wfull(i, cyn), w_r.at[i, 2])
        go(whalf(i, cyn, 1), whalf(i, cyn, 1), w_s.at[i, 3], w_r.at[i, 4], xn)

    def wait_rest(i):
        wait_recv(whalf(i, cdg, 0), w_r.at[i, 3])
        wait_recv(whalf(i, cdg, 1), w_r.at[i, 4])

    def send_x(late):
        for hf, dev in enumerate((xn, yn)):
            src = xsource(cdg, late).at[:, pl.ds(hf * (FR // 2), FR // 2), :]
            go(src, xrel.at[hf, xclips(late)], x_s.at[late, hf], xrel_r.at[late, hf], dev)
        go(xsource(cxn, late), xslot(c, late), x_s.at[late, 2], x_r.at[late, 1], xn)
        go(xsource(cyn, late), xslot(c, late), x_s.at[late, 3], x_r.at[late, 2], yn)

    def relay_x(late):
        for hf, (chip, dev) in enumerate(((cxn, yn), (cyn, xn))):
            piece = xrel.at[hf, xclips(late)]
            wait_recv(piece, xrel_r.at[late, hf])
            go(piece, xhalf(chip, late, hf), x_s.at[late, 4 + hf], x_r.at[late, 3 + hf], dev)

    def ln1_stage(j):
        def body(b, _):
            vals = xb[j, pl.ds(b * FR, FR), :].astype(F32)
            am[j, k, b] = ln_rows(vals, row(ln1g), row(ln1b))
            return 0
        lax.fori_loop(0, 4, body, 0)
        cp = remote(am.at[j, k], am.at[j, k], am_s.at[0, j], am_r.at[0, j], sib)
        cp.start()
        a_sends.append(cp)

    def wait_x(late):
        for r, chip in ((0, c), (1, cxn), (2, cyn)):
            wait_recv(xslot(chip, late), x_r.at[late, r])
        for hf in range(2):
            wait_recv(xhalf(cdg, late, hf), x_r.at[late, 3 + hf])

    send_x(0)
    for i in range(3):
        pltpu.make_async_copy(w_hbm[i], wfull(i, c), w_r.at[i, 0]).start()
    for late in range(2):
        pltpu.make_async_copy(xsource(c, late), xslot(c, late), x_r.at[late, 0]).start()
    for i in range(3, 6):
        pltpu.make_async_copy(w_hbm[i], wfull(i, c), w_r.at[i, 0]).start()
    wc_copies = []
    for i, src in enumerate((ck_h.at[0], ck_h.at[1], cv_h.at[0], cv_h.at[1])):
        for hf in range(2):
            cp = pltpu.make_async_copy(src.at[pl.ds(hf * 512, 512)], qkv.at[i, pl.ds(0, 512), pl.ds(hf * LOC, LOC)], c_s.at[i, hf])
            cp.start()
            wc_copies.append(cp)
    bias[c, 0:1, :] = row(bq_v)
    bias[c, 1:2, :] = row(bv_v)
    b1_row = row(b1_v)
    for q in range(4):
        bias[c, 2 + q:3 + q, :] = b1_row[:, q * LOC:(q + 1) * LOC]
    for l in range(2):
        bct[l] = jnp.transpose(jnp.broadcast_to(bcv_v[l:l + 1, :].astype(F32), (LOC, LOC)))
    relay_x(0)
    for r, dev in enumerate((xn, yn, dg)):
        go(bias.at[c], bias.at[c], b_s.at[r], b_r.at[r], dev)
    for i in range(3):
        send_direct(i)

    a_sends = []
    wait_x(0)
    for j in range(2):
        ln1_stage(j)
    send_direct(3)
    for cp in wc_copies:
        cp.wait()
    for i in range(4):
        for hf in range(2):
            wct[i * LOC:(i + 1) * LOC, hf * 512:(hf + 1) * 512] = jnp.transpose(qkv[i, 0:512, hf * LOC:(hf + 1) * LOC])
    for r, chip in enumerate((cxn, cyn, cdg)):
        wait_recv(bias.at[chip], b_r.at[r])
    for i in range(4):
        relay(i)
    send_direct(4)
    send_direct(5)
    for i in range(3):
        wait_rest(i)

    def row_of(r):
        return jnp.concatenate([bias[n, r:r + 1, :] for n in range(4)], axis=1)

    lane = lax.broadcasted_iota(jnp.int32, (FRAMES, LOC), 1)

    def attention_stage(j):
        wait_recv(am.at[j, ks], am_r.at[0, j])
        bq, bv = row_of(0), row_of(1)

        def project(r, _):
            rows = pl.ds(r * HALF, HALF)
            a = am[j, r].reshape(HALF, D)
            qkv[0, rows, :] = ((jnp.dot(a, wqkv[0], preferred_element_type=F32) + bq) * ATTN_SCALE).astype(BF16)
            qkv[1, rows, :] = (jnp.dot(a, wqkv[1], preferred_element_type=F32) * ATTN_SCALE).astype(BF16)
            qkv[2, rows, :] = (jnp.dot(a, wqkv[2], preferred_element_type=F32) + bv).astype(BF16)
            return 0
        lax.fori_loop(0, 2, project, 0)

        def pair(p, _):
            cols = pl.ds(pl.multiple_of(p * LOC, LOC), LOC)
            kp, vp = qkv[1, :, cols], qkv[2, :, cols]
            zero = jnp.zeros_like(kp)
            kz[0] = jnp.where(lane < HEAD_DIM, kp, zero)
            kz[1] = jnp.where(lane < HEAD_DIM, zero, kp)
            vz[0] = jnp.where(lane < HEAD_DIM, vp, zero)
            vz[1] = jnp.where(lane < HEAD_DIM, zero, vp)

            def attend(r, _):
                rows = pl.ds(r * QROWS, QROWS)
                qb = qkv[0, rows, cols]
                out = None
                for hh in range(2):
                    s = lax.dot_general(qb, kz[hh], (((1,), (1,)), ((), ())), preferred_element_type=F32)
                    e = jnp.exp(s - jnp.max(s, axis=-1, keepdims=True))
                    prob = (e * (1.0 / jnp.sum(e, axis=-1, keepdims=True))).astype(BF16)
                    part = jnp.dot(prob, vz[hh], preferred_element_type=F32)
                    out = part if out is None else out + part
                qkv[3, rows, cols] = out.astype(BF16)
                return 0
            lax.fori_loop(0, FRAMES // QROWS, attend, 0)
            return 0
        lax.fori_loop(0, 4, pair, 0)

    own = pl.ds(k * HALF, HALF)
    oth = pl.ds(ks * HALF, HALF)

    def swap_partials(phase, j, lhs, weight):
        for n in range(2):
            cols = slice(n * 512, (n + 1) * 512)
            ex_s[j, :, cols] = jnp.dot(lhs(oth), weight[:, cols], preferred_element_type=F32).astype(BF16)
        cp = remote(ex_s.at[j], ex_r.at[j], ex_ss.at[phase, j], ex_rs.at[phase, j], sib)
        cp.start()
        for n in range(2):
            cols = slice(n * 512, (n + 1) * 512)
            acc[:, cols] = jnp.dot(lhs(own), weight[:, cols], preferred_element_type=F32)
        wait_recv(ex_r.at[j], ex_rs.at[phase, j])
        cp.wait_send()

    m_sends = []

    def output_stage(j):
        swap_partials(0, j, lambda rows: qkv[3, rows, :], wo)
        a_sends[j].wait_send()

        def body(b, _):
            rows = pl.ds(b * FR, FR)
            out = (acc[rows, :] + ex_r[j, rows, :].astype(F32) + row(bo_v)).astype(BF16)
            h = (xb[j, rows, :].astype(F32) + out.astype(F32)).astype(BF16)
            xb[j, rows, :] = h
            am[j, k, b] = ln_rows(h.astype(F32), row(ln2g), row(ln2b))
            return 0
        lax.fori_loop(0, 4, body, 0)
        cp = remote(am.at[j, k], am.at[j, k], am_s.at[1, j], am_r.at[1, j], sib)
        cp.start()
        m_sends.append(cp)

    def epiece(group, j, core, hf):
        if group == 3:
            return am.at[j, core, pl.ds(2 * hf, 2)]
        return ea.at[3 * group + j, pl.ds(2 * hf, 2), core]

    def up_stage(j):
        wait_recv(am.at[j, ks], am_r.at[1, j])

        def up(i, _):
            n, r = i // 2, i % 2
            rows = pl.ds(r * HALF, HALF)
            cols = pl.ds(pl.multiple_of(n * HID, HID), HID)
            b1 = jnp.concatenate([bias[n, 2 + q:3 + q, :] for q in range(4)], axis=1)
            u = jnp.dot(am[j, r].reshape(HALF, D), w1[:, cols], preferred_element_type=F32) + b1
            act = (0.5 * u * (1.0 + lax.erf(u * (2.0 ** -0.5)))).astype(BF16)
            if j == 1:
                qkv[n, rows, :] = act
            else:
                g[n, rows, :] = act
            return 0
        lax.fori_loop(0, 8, up, 0)
        m_sends[j].wait_send()
        for peer in (sib, xn, yn):
            pl.semaphore_signal(free.at[j], inc=1, device_id={"tp": peer}, device_id_type=pl.DeviceIdType.MESH)

    def down_stage(j):
        hidden = qkv if j == 1 else g
        swap_partials(1, j, lambda rows: jnp.concatenate([hidden[n, rows, :] for n in range(4)], axis=1), w2)
        if j == 0:
            relay_x(1)

        def post(b, _):
            rows = pl.ds(b * FR, FR)
            out = (acc[rows, :] + ex_r[j, rows, :].astype(F32) + row(bfc2)).astype(BF16)
            h2 = (xb[j, rows, :].astype(F32) + out.astype(F32)).astype(BF16)
            ea[j, b, k] = ln_rows(h2.astype(F32), row(postg), row(postb))
            return 0
        lax.fori_loop(0, 4, post, 0)
        for hf in range(2):
            go(epiece(0, j, k, hf), epiece(1, j, k, hf), es_x.at[j, hf], ex_x.at[j, hf], xn)
            go(epiece(0, j, k, 1 - hf), epiece(2, j, k, 1 - hf), es_y.at[j, 1 - hf], ex_y.at[j, 1 - hf], yn)
        for hf in range(2):
            go(epiece(0, j, k, hf), epiece(0, j, k, hf), es_f.at[0, j, hf], ex_f.at[0, j, hf], sib)

    def forward(group, j, hf):
        go(epiece(group, j, k, hf), epiece(group, j, k, hf), es_f.at[group, j, hf], ex_f.at[group, j, hf], sib)

    def relay_e(j):
        pl.semaphore_wait(free.at[j], 3)
        wait_recv(epiece(1, j, k, 0), ex_x.at[j, 0])
        go(epiece(1, j, k, 0), epiece(3, j, k, 0), es_d.at[j, 0], ex_d.at[j, 0], yn)
        forward(1, j, 0)
        wait_recv(epiece(2, j, k, 1), ex_y.at[j, 1])
        go(epiece(2, j, k, 1), epiece(3, j, k, 1), es_d.at[j, 1], ex_d.at[j, 1], xn)
        forward(2, j, 1)
        wait_recv(epiece(1, j, k, 1), ex_x.at[j, 1])
        forward(1, j, 1)
        wait_recv(epiece(2, j, k, 0), ex_y.at[j, 0])
        forward(2, j, 0)

    def take_diagonal(j):
        for hf in range(2):
            wait_recv(epiece(3, j, k, hf), ex_d.at[j, hf])
            forward(3, j, hf)

    def write_caches(clip, ec):
        cache_rows(clip, ec, wct, bct, kc_o, vc_o)

    def near_cache(group, j):
        chip = jnp.where(group == 0, c, jnp.where(group == 1, cxn, cyn))
        clip = chip * PER_CHIP + j
        for hf in range(2):
            wait_recv(ea.at[3 * group + j, pl.ds(2 * hf, 2), ks], ex_f.at[group, j, hf])
        enc_o[clip] = ea[3 * group + j, c, k]
        write_caches(clip, ea[3 * group + j].reshape(FRAMES, D))

    def far_cache(j):
        clip = cdg * PER_CHIP + j
        for hf in range(2):
            wait_recv(epiece(3, j, ks, hf), ex_f.at[3, j, hf])
        enc_o[clip] = am[j, k, c]
        write_caches(clip, natural_order(am, j))

    attention_stage(0)
    wait_rest(3)
    output_stage(0)
    attention_stage(1)
    relay(4)
    output_stage(1)
    relay(5)
    send_x(1)
    wait_rest(4)
    up_stage(0)
    up_stage(1)
    wait_rest(5)
    down_stage(0)
    down_stage(1)
    wait_x(1)
    ln1_stage(2)
    attention_stage(2)
    relay_e(0)
    output_stage(2)
    up_stage(2)
    down_stage(2)
    relay_e(1)

    def first(i, _):
        near_cache(jnp.where(i < 3, 0, 1 + (i + 1) % 2), jnp.where(i < 3, i, (i - 3) // 2))
        return 0
    lax.fori_loop(0, 7, first, 0)
    take_diagonal(0)
    far_cache(0)
    relay_e(2)

    def second(i, _):
        near_cache(1 + i, 2)
        return 0
    lax.fori_loop(0, 2, second, 0)
    take_diagonal(1)
    far_cache(1)
    take_diagonal(2)
    for hf in range(2):
        wait_recv(epiece(3, 2, ks, hf), ex_f.at[3, 2, hf])
    for cp in sends:
        cp.wait_send()


def natural_order(am, j):
    return jnp.concatenate([am[j, core, b] for b in range(4) for core in range(2)], axis=0)


def cache_rows(clip, ec, wct, bct, k_ref, v_ref):
    r = lax.dot_general(wct[...], ec, (((1,), (1,)), ((), ())), preferred_element_type=F32)
    for i in range(4):
        part = r[i * LOC:(i + 1) * LOC, :]
        if i >= 2:
            part = part + jnp.concatenate([bct[i - 2]] * 6, axis=1)
        (k_ref, v_ref)[i // 2][i % 2, clip] = part.astype(BF16)


def writer(enc_v, kc_v, vc_v, am, wct, bct, enc_o, kc_o, vc_o, kl, vl, sem, last_sem):
    t = lax.axis_index("tp")
    c, k = t // 2, t % 2
    cx, cy = c % 2, c // 2
    cdg = 2 * (1 - cy) + (1 - cx)
    last = cdg * PER_CHIP + 2

    def copies(clip):
        cps = [pltpu.make_async_copy(kc_v.at[l, clip], kc_o.at[l, clip], sem) for l in range(2)]
        cps += [pltpu.make_async_copy(vc_v.at[l, clip], vc_o.at[l, clip], sem) for l in range(2)]
        return cps + [pltpu.make_async_copy(enc_v.at[clip], enc_o.at[clip], sem)]

    def start(i, _):
        for cp in copies(lax.rem(last + 1 + i, CLIPS)):
            cp.start()
        return 0
    lax.fori_loop(0, CLIPS - 1, start, 0)
    cps = [pltpu.make_async_copy(am.at[2, k, c], enc_o.at[last], last_sem)]
    cps[0].start()
    cache_rows(0, natural_order(am, 2), wct, bct, kl, vl)
    for l in range(2):
        cps.append(pltpu.make_async_copy(kl.at[l, 0], kc_o.at[l, last], last_sem))
        cps.append(pltpu.make_async_copy(vl.at[l, 0], vc_o.at[l, last], last_sem))
    for cp in cps[1:]:
        cp.start()

    def finish(i, _):
        for cp in copies(lax.rem(last + 1 + i, CLIPS)):
            cp.wait()
        return 0
    lax.fori_loop(0, CLIPS - 1, finish, 0)
    for cp in cps:
        cp.wait()


def device_body(hidden_loc, ln1_gain, ln1_bias, w_q, b_q, w_k, w_v, b_v, w_o, b_o, ln2_gain, ln2_bias, w_fc1, b_fc1, w_fc2, b_fc2, post_gain, post_bias, w_ck, w_cv, b_cv):
    anyspec = pl.BlockSpec(memory_space=pl.ANY)
    vspec = pl.BlockSpec(memory_space=pltpu.VMEM)
    dma = pltpu.SemaphoreType.DMA
    cache = (2, CLIPS, LOC, FRAMES)
    parts = pl.pallas_call(
        kernel,
        out_shape=(
            pltpu.VMEM((CLIPS, FR, D), BF16), pltpu.VMEM(cache, BF16), pltpu.VMEM(cache, BF16),
            pltpu.VMEM((PER_CHIP, 2, 4, FR, D), BF16),
            pltpu.VMEM((4 * LOC, D), BF16),
            pltpu.VMEM((2, LOC, LOC), F32),
        ),
        in_specs=[anyspec] * 9 + [vspec] * 12,
        out_specs=(vspec,) * 6,
        scratch_shapes=[
            pltpu.VMEM((PER_CHIP, HALF, D), BF16),
            pltpu.VMEM((2, PER_CHIP, FR // 2, D), BF16),
            pltpu.VMEM((PER_CHIP, HALF, D), BF16),
            pltpu.VMEM((PER_CHIP, HALF, D), BF16),
            pltpu.VMEM((3, D, NQ), BF16),
            pltpu.VMEM((NQ, D), BF16),
            pltpu.VMEM((D, NH), BF16),
            pltpu.VMEM((NH, D), BF16),
            pltpu.VMEM((4, 8, LOC), F32),
            pltpu.VMEM((4, FRAMES, NQ), BF16),
            pltpu.VMEM((2, FRAMES, LOC), BF16),
            pltpu.VMEM((2, FRAMES, LOC), BF16),
            pltpu.VMEM((4, FRAMES, HID), BF16),
            pltpu.VMEM((HALF, D), F32),
            pltpu.VMEM((9, 4, 2, FR, D), BF16),
            dma((2, 5)), dma((2, 6)), dma((2, 2)), dma((6, 5)), dma((6, 4)), dma((3,)), dma((3,)),
            dma((2, 3)), dma((2, 3)), dma((2, 3)), dma((2, 3)),
            dma((3, 2)), dma((3, 2)), dma((3, 2)), dma((4, 3, 2)),
            dma((3, 2)), dma((3, 2)), dma((3, 2)), dma((4, 3, 2)),
            dma((4, 2)), pltpu.SemaphoreType.REGULAR((3,)),
        ],
        compiler_params=pltpu.CompilerParams(collective_id=0, has_side_effects=True, vmem_limit_bytes=48500000),
        name="encoder_layer",
    )(hidden_loc, w_q, w_k, w_v, w_o, w_fc1, w_fc2, w_ck, w_cv,
      b_q, b_v, b_fc1, b_cv, ln1_gain, ln1_bias, ln2_gain, ln2_bias, post_gain, post_bias, b_o, b_fc2)

    enc, kc, vc = pl.pallas_call(
        writer,
        out_shape=(jax.ShapeDtypeStruct((CLIPS, FR, D), BF16), jax.ShapeDtypeStruct(cache, BF16), jax.ShapeDtypeStruct(cache, BF16)),
        in_specs=[vspec] * 6,
        out_specs=(anyspec,) * 3,
        scratch_shapes=[pltpu.VMEM((2, 1, LOC, FRAMES), BF16), pltpu.VMEM((2, 1, LOC, FRAMES), BF16), dma, dma],
        compiler_params=pltpu.CompilerParams(vmem_limit_bytes=8000000),
        name="writer",
    )(*parts)

    def heads_last(cached):
        return cached.reshape(2, CLIPS, LOC // HEAD_DIM, HEAD_DIM, FRAMES).transpose(0, 1, 4, 2, 3)
    return enc, heads_last(kc), heads_last(vc)


def solution(mesh):
    in_specs = (P("dp", "tp", None), P(), P(), P(None, "tp"), P("tp"), P(None, "tp"), P(None, "tp"), P("tp"), P("tp", None), P(), P(), P(), P(None, "tp"), P("tp"), P("tp", None), P(), P(), P(), P(None, None, "tp"), P(None, None, "tp"), P(None, "tp"))
    out_specs = (P("dp", "tp", None), P(None, "dp", None, "tp", None), P(None, "dp", None, "tp", None))
    return jax.shard_map(device_body, mesh=mesh, in_specs=in_specs, out_specs=out_specs, check_vma=False)
```

```python
import functools

import jax
import jax.numpy as jnp
from jax import lax
from jax.experimental import pallas as pl
from jax.experimental.pallas import tpu as pltpu
from jax.sharding import PartitionSpec as P

HEAD_DIM = 64
ATTN_SCALE = HEAD_DIM ** -0.25
LN_EPS = 1e-5
CLIPS = 12
PER_CHIP = 3
FR = 96
HALF = 4 * FR
FRAMES = 8 * FR
D = 1024
LOC = 128
HID = 512
NQ = 4 * LOC
NH = 4 * HID
QROWS = 256
F32, BF16 = jnp.float32, jnp.bfloat16


def ln_rows(values, gain, bias):
    centered = values - jnp.mean(values, axis=-1, keepdims=True)
    row_var = jnp.mean(centered * centered, axis=-1, keepdims=True)
    return (centered * lax.rsqrt(row_var + LN_EPS) * gain + bias).astype(BF16)


def kernel(hid, wq_h, wk_h, wv_h, wo_h, w1_h, w2_h, ck_h, cv_h,
           bq_h, bv_h, b1_h, bcv_h, ln1g_h, ln1b_h, ln2g_h, ln2b_h, postg_h, postb_h, bo_h, bfc2_h,
           enc_o, kc_o, vc_o, am, wct, bct,
           bq_v, bv_v, b1_v, bcv_v, ln1g, ln1b, ln2g, ln2b, postg, postb, bo_v, bfc2, xb, xrel, ex_s, ex_r, wqkv, wo, w1, w2, bias, qkv, kz, vz, g, acc, ea,
           x_r, x_s, xrel_r, w_r, w_s, b_r, b_s, am_r, am_s, ex_rs, ex_ss, ex_x, ex_y, ex_d, ex_f, ex_g, es_x, es_y, es_d, es_f, es_g, c_s, v_s, free):
    t = lax.axis_index("tp")
    c, k = t // 2, t % 2
    cx, cy = c % 2, c // 2
    cxn = 2 * cy + (1 - cx)
    cyn = 2 * (1 - cy) + cx
    cdg = 2 * (1 - cy) + (1 - cx)
    ks = 1 - k
    sib, xn, yn = 2 * c + ks, 2 * cxn + k, 2 * cyn + k

    def remote(src, dst, ssem, rsem, dev):
        return pltpu.make_async_remote_copy(src_ref=src, dst_ref=dst, send_sem=ssem, recv_sem=rsem,
                                            device_id={"tp": dev}, device_id_type=pl.DeviceIdType.MESH)

    def wait_recv(ref, rsem):
        pltpu.make_async_copy(ref, ref, rsem).wait()

    def row(ref):
        return ref[...].astype(F32).reshape(1, ref.shape[0])

    barrier = pltpu.get_barrier_semaphore()
    for peer in (sib, xn, yn):
        pl.semaphore_signal(barrier, inc=1, device_id={"tp": peer}, device_id_type=pl.DeviceIdType.MESH)
    pl.semaphore_wait(barrier, 3)

    def xclips(late):
        return pl.ds(2, 1) if late else pl.ds(0, 2)

    def xslot(chip, late):
        return xb.at[xclips(late), pl.ds(chip * FR, FR), :]

    def xhalf(chip, late, hf):
        return xb.at[xclips(late), pl.ds(chip * FR + hf * (FR // 2), FR // 2), :]

    def xsource(chip, late):
        return hid.at[pl.ds(chip * PER_CHIP + 2, 1) if late else pl.ds(chip * PER_CHIP, 2)]

    def wfull(i, chip):
        if i < 3:
            return wqkv.at[i, :, pl.ds(pl.multiple_of(chip * LOC, LOC), LOC)]
        if i == 3:
            return wo.at[pl.ds(chip * LOC, LOC)]
        if i == 4:
            return w1.at[:, pl.ds(pl.multiple_of(chip * HID, HID), HID)]
        return w2.at[pl.ds(chip * HID, HID)]

    def whalf(i, chip, hf):
        if i < 3:
            return wqkv.at[i, pl.ds(hf * (D // 2), D // 2), pl.ds(pl.multiple_of(chip * LOC, LOC), LOC)]
        if i == 3:
            return wo.at[pl.ds(chip * LOC + hf * (LOC // 2), LOC // 2)]
        if i == 4:
            return w1.at[pl.ds(hf * (D // 2), D // 2), pl.ds(pl.multiple_of(chip * HID, HID), HID)]
        return w2.at[pl.ds(chip * HID + hf * (HID // 2), HID // 2)]

    w_hbm = (wq_h, wk_h, wv_h, wo_h, w1_h, w2_h)
    sends = []

    def go(src, dst, ssem, rsem, dev):
        cp = remote(src, dst, ssem, rsem, dev)
        cp.start()
        sends.append(cp)

    def send_direct(i):
        wait_recv(wfull(i, c), w_r.at[i, 0])
        go(wfull(i, c), wfull(i, c), w_s.at[i, 0], w_r.at[i, 1], xn)
        go(wfull(i, c), wfull(i, c), w_s.at[i, 1], w_r.at[i, 2], yn)

    def relay(i):
        wait_recv(wfull(i, cxn), w_r.at[i, 1])
        go(whalf(i, cxn, 0), whalf(i, cxn, 0), w_s.at[i, 2], w_r.at[i, 3], yn)
        wait_recv(wfull(i, cyn), w_r.at[i, 2])
        go(whalf(i, cyn, 1), whalf(i, cyn, 1), w_s.at[i, 3], w_r.at[i, 4], xn)

    def wait_rest(i):
        wait_recv(whalf(i, cdg, 0), w_r.at[i, 3])
        wait_recv(whalf(i, cdg, 1), w_r.at[i, 4])

    def send_x(late):
        for hf, dev in enumerate((xn, yn)):
            src = xsource(cdg, late).at[:, pl.ds(hf * (FR // 2), FR // 2), :]
            go(src, xrel.at[hf, xclips(late)], x_s.at[late, hf], xrel_r.at[late, hf], dev)
        go(xsource(cxn, late), xslot(c, late), x_s.at[late, 2], x_r.at[late, 1], xn)
        go(xsource(cyn, late), xslot(c, late), x_s.at[late, 3], x_r.at[late, 2], yn)

    def relay_x(late):
        for hf, (chip, dev) in enumerate(((cxn, yn), (cyn, xn))):
            piece = xrel.at[hf, xclips(late)]
            wait_recv(piece, xrel_r.at[late, hf])
            go(piece, xhalf(chip, late, hf), x_s.at[late, 4 + hf], x_r.at[late, 3 + hf], dev)

    def ln1_stage(j):
        def body(b, _):
            vals = xb[j, pl.ds(b * FR, FR), :].astype(F32)
            am[j, k, b] = ln_rows(vals, row(ln1g), row(ln1b))
            return 0
        lax.fori_loop(0, 4, body, 0)
        cp = remote(am.at[j, k], am.at[j, k], am_s.at[0, j], am_r.at[0, j], sib)
        cp.start()
        a_sends.append(cp)

    def wait_x(late):
        for r, chip in ((0, c), (1, cxn), (2, cyn)):
            wait_recv(xslot(chip, late), x_r.at[late, r])
        for hf in range(2):
            wait_recv(xhalf(cdg, late, hf), x_r.at[late, 3 + hf])

    send_x(0)
    vec_copies = [pltpu.make_async_copy(src, dst, v_s.at[i]) for i, (src, dst) in enumerate((
        (bq_h, bq_v), (bv_h, bv_v), (b1_h, b1_v), (bcv_h, bcv_v), (ln1g_h, ln1g), (ln1b_h, ln1b),
        (ln2g_h, ln2g), (ln2b_h, ln2b), (postg_h, postg), (postb_h, postb), (bo_h, bo_v), (bfc2_h, bfc2)))]
    for cp in vec_copies:
        cp.start()
    for i in range(3):
        pltpu.make_async_copy(w_hbm[i], wfull(i, c), w_r.at[i, 0]).start()
    for late in range(2):
        pltpu.make_async_copy(xsource(c, late), xslot(c, late), x_r.at[late, 0]).start()
    for i in range(3, 6):
        pltpu.make_async_copy(w_hbm[i], wfull(i, c), w_r.at[i, 0]).start()
    wc_copies = []
    for i, src in enumerate((ck_h.at[0], ck_h.at[1], cv_h.at[0], cv_h.at[1])):
        for hf in range(2):
            cp = pltpu.make_async_copy(src.at[pl.ds(hf * 512, 512)], qkv.at[i, pl.ds(0, 512), pl.ds(hf * LOC, LOC)], c_s.at[i, hf])
            cp.start()
            wc_copies.append(cp)
    for cp in vec_copies:
        cp.wait()
    bias[c, 0:1, :] = row(bq_v)
    bias[c, 1:2, :] = row(bv_v)
    b1_row = row(b1_v)
    for q in range(4):
        bias[c, 2 + q:3 + q, :] = b1_row[:, q * LOC:(q + 1) * LOC]
    for l in range(2):
        bct[l] = jnp.transpose(jnp.broadcast_to(bcv_v[l:l + 1, :].astype(F32), (LOC, LOC)))
    relay_x(0)
    for r, dev in enumerate((xn, yn)):
        go(bias.at[c], bias.at[c], b_s.at[r], b_r.at[r], dev)
    for i in range(3):
        send_direct(i)

    a_sends = []
    wait_x(0)
    for j in range(2):
        ln1_stage(j)
    send_direct(3)
    for cp in wc_copies:
        cp.wait()
    for i in range(4):
        for hf in range(2):
            wct[i * LOC:(i + 1) * LOC, hf * 512:(hf + 1) * 512] = jnp.transpose(qkv[i, 0:512, hf * LOC:(hf + 1) * LOC])
    for r, chip in enumerate((cxn, cyn, cdg)):
        wait_recv(bias.at[chip], b_r.at[r])
        if r == 0:
            go(bias.at[cxn], bias.at[cxn], b_s.at[2], b_r.at[2], yn)
    for i in range(4):
        relay(i)
    send_direct(4)
    send_direct(5)
    for i in range(3):
        wait_rest(i)

    def row_of(r):
        return jnp.concatenate([bias[n, r:r + 1, :] for n in range(4)], axis=1)

    lane = lax.broadcasted_iota(jnp.int32, (FRAMES, LOC), 1)

    def attention_stage(j):
        wait_recv(am.at[j, ks], am_r.at[0, j])
        bq, bv = row_of(0), row_of(1)

        def project(r, _):
            rows = pl.ds(r * HALF, HALF)
            a = am[j, r].reshape(HALF, D)
            qkv[0, rows, :] = ((jnp.dot(a, wqkv[0], preferred_element_type=F32) + bq) * ATTN_SCALE).astype(BF16)
            qkv[1, rows, :] = (jnp.dot(a, wqkv[1], preferred_element_type=F32) * ATTN_SCALE).astype(BF16)
            qkv[2, rows, :] = (jnp.dot(a, wqkv[2], preferred_element_type=F32) + bv).astype(BF16)
            return 0
        lax.fori_loop(0, 2, project, 0)

        def pair(p, _):
            cols = pl.ds(pl.multiple_of(p * LOC, LOC), LOC)
            kp, vp = qkv[1, :, cols], qkv[2, :, cols]
            zero = jnp.zeros_like(kp)
            kz[0] = jnp.where(lane < HEAD_DIM, kp, zero)
            kz[1] = jnp.where(lane < HEAD_DIM, zero, kp)
            vz[0] = jnp.where(lane < HEAD_DIM, vp, zero)
            vz[1] = jnp.where(lane < HEAD_DIM, zero, vp)

            def attend(r, _):
                rows = pl.ds(r * QROWS, QROWS)
                qb = qkv[0, rows, cols]
                out = None
                for hh in range(2):
                    s = lax.dot_general(qb, kz[hh], (((1,), (1,)), ((), ())), preferred_element_type=F32)
                    e = jnp.exp(s - jnp.max(s, axis=-1, keepdims=True))
                    prob = (e * (1.0 / jnp.sum(e, axis=-1, keepdims=True))).astype(BF16)
                    part = jnp.dot(prob, vz[hh], preferred_element_type=F32)
                    out = part if out is None else out + part
                qkv[3, rows, cols] = out.astype(BF16)
                return 0
            lax.fori_loop(0, FRAMES // QROWS, attend, 0)
            return 0
        lax.fori_loop(0, 4, pair, 0)

    own = pl.ds(k * HALF, HALF)
    oth = pl.ds(ks * HALF, HALF)

    def swap_partials(phase, j, lhs, weight):
        for n in range(2):
            cols = slice(n * 512, (n + 1) * 512)
            ex_s[j, :, cols] = jnp.dot(lhs(oth), weight[:, cols], preferred_element_type=F32).astype(BF16)
        cp = remote(ex_s.at[j], ex_r.at[j], ex_ss.at[phase, j], ex_rs.at[phase, j], sib)
        cp.start()
        for n in range(2):
            cols = slice(n * 512, (n + 1) * 512)
            acc[:, cols] = jnp.dot(lhs(own), weight[:, cols], preferred_element_type=F32)
        wait_recv(ex_r.at[j], ex_rs.at[phase, j])
        cp.wait_send()

    m_sends = []

    def output_stage(j):
        swap_partials(0, j, lambda rows: qkv[3, rows, :], wo)
        a_sends[j].wait_send()

        def body(b, _):
            rows = pl.ds(b * FR, FR)
            out = (acc[rows, :] + ex_r[j, rows, :].astype(F32) + row(bo_v)).astype(BF16)
            h = (xb[j, rows, :].astype(F32) + out.astype(F32)).astype(BF16)
            xb[j, rows, :] = h
            am[j, k, b] = ln_rows(h.astype(F32), row(ln2g), row(ln2b))
            return 0
        lax.fori_loop(0, 4, body, 0)
        cp = remote(am.at[j, k], am.at[j, k], am_s.at[1, j], am_r.at[1, j], sib)
        cp.start()
        m_sends.append(cp)

    def epiece(group, j, core, hf):
        return ea.at[3 * group + j, pl.ds(2 * hf, 2), core]

    def up_stage(j):
        wait_recv(am.at[j, ks], am_r.at[1, j])

        def up(i, _):
            n, r = i // 2, i % 2
            rows = pl.ds(r * HALF, HALF)
            cols = pl.ds(pl.multiple_of(n * HID, HID), HID)
            b1 = jnp.concatenate([bias[n, 2 + q:3 + q, :] for q in range(4)], axis=1)
            u = jnp.dot(am[j, r].reshape(HALF, D), w1[:, cols], preferred_element_type=F32) + b1
            act = (0.5 * u * (1.0 + lax.erf(u * (2.0 ** -0.5)))).astype(BF16)
            if j == 1:
                qkv[n, rows, :] = act
            else:
                g[n, rows, :] = act
            return 0
        lax.fori_loop(0, 8, up, 0)
        m_sends[j].wait_send()
        for peer in (sib, xn, yn):
            pl.semaphore_signal(free.at[j], inc=1, device_id={"tp": peer}, device_id_type=pl.DeviceIdType.MESH)

    def down_stage(j):
        hidden = qkv if j == 1 else g
        swap_partials(1, j, lambda rows: jnp.concatenate([hidden[n, rows, :] for n in range(4)], axis=1), w2)
        if j == 0:
            relay_x(1)

        def post(b, _):
            rows = pl.ds(b * FR, FR)
            out = (acc[rows, :] + ex_r[j, rows, :].astype(F32) + row(bfc2)).astype(BF16)
            h2 = (xb[j, rows, :].astype(F32) + out.astype(F32)).astype(BF16)
            ea[j, b, k] = ln_rows(h2.astype(F32), row(postg), row(postb))
            return 0
        lax.fori_loop(0, 4, post, 0)
        for hf in range(2):
            go(epiece(0, j, k, hf), epiece(1, j, k, hf), es_x.at[j, hf], ex_x.at[j, hf], xn)
            go(epiece(0, j, k, 1 - hf), epiece(2, j, k, 1 - hf), es_y.at[j, 1 - hf], ex_y.at[j, 1 - hf], yn)
        for hf in range(2):
            go(epiece(0, j, k, hf), epiece(0, j, k, hf), es_f.at[0, j, hf], ex_f.at[0, j, hf], sib)

    def forward(group, j, hf):
        go(epiece(group, j, k, hf), epiece(group, j, k, hf), es_f.at[group, j, hf], ex_f.at[group, j, hf], sib)

    def relay_e(j):
        pl.semaphore_wait(free.at[j], 3)
        wait_recv(epiece(1, j, k, 0), ex_x.at[j, 0])
        for b in range(2):
            go(ea.at[PER_CHIP + j, b, k], am.at[j, k, b], es_d.at[j, b], ex_d.at[j, b], yn)
        forward(1, j, 0)
        wait_recv(epiece(2, j, k, 1), ex_y.at[j, 1])
        for b in range(2, 4):
            go(ea.at[2 * PER_CHIP + j, b, k], am.at[j, k, b], es_d.at[j, b], ex_d.at[j, b], xn)
        forward(2, j, 1)
        wait_recv(epiece(1, j, k, 1), ex_x.at[j, 1])
        forward(1, j, 1)
        wait_recv(epiece(2, j, k, 0), ex_y.at[j, 0])
        forward(2, j, 0)

    def take_diagonal(j):
        for b in (0, 2, 1, 3):
            piece = am.at[j, k, b]
            wait_recv(piece, ex_d.at[j, b])
            go(piece, piece, es_g.at[j, b], ex_g.at[j, b], sib)

    def wait_diagonal(j):
        for b in range(4):
            wait_recv(am.at[j, ks, b], ex_g.at[j, b])

    def write_caches(clip, ec):
        cache_rows(clip, ec, wct, bct, kc_o, vc_o)

    def near_cache(group, j):
        chip = jnp.where(group == 0, c, jnp.where(group == 1, cxn, cyn))
        clip = chip * PER_CHIP + j
        for hf in range(2):
            wait_recv(ea.at[3 * group + j, pl.ds(2 * hf, 2), ks], ex_f.at[group, j, hf])
        enc_o[clip] = ea[3 * group + j, c, k]
        write_caches(clip, ea[3 * group + j].reshape(FRAMES, D))

    def far_cache(j):
        clip = cdg * PER_CHIP + j
        wait_diagonal(j)
        enc_o[clip] = am[j, k, c]
        write_caches(clip, natural_order(am, j))

    attention_stage(0)
    wait_rest(3)
    output_stage(0)
    attention_stage(1)
    relay(4)
    output_stage(1)
    relay(5)
    send_x(1)
    wait_rest(4)
    up_stage(0)
    up_stage(1)
    wait_rest(5)
    down_stage(0)
    down_stage(1)
    wait_x(1)
    ln1_stage(2)
    attention_stage(2)
    relay_e(0)
    output_stage(2)
    up_stage(2)
    down_stage(2)
    relay_e(1)

    def first(i, _):
        near_cache(jnp.where(i < 3, 0, 1 + (i + 1) % 2), jnp.where(i < 3, i, (i - 3) // 2))
        return 0
    lax.fori_loop(0, 7, first, 0)
    take_diagonal(0)
    far_cache(0)
    relay_e(2)

    def second(i, _):
        near_cache(1 + i, 2)
        return 0
    lax.fori_loop(0, 2, second, 0)
    take_diagonal(1)
    far_cache(1)
    take_diagonal(2)
    wait_diagonal(2)
    for cp in sends:
        cp.wait_send()


def natural_order(am, j):
    return jnp.concatenate([am[j, core, b] for b in range(4) for core in range(2)], axis=0)


def cache_rows(clip, ec, wct, bct, k_ref, v_ref):
    r = lax.dot_general(wct[...], ec, (((1,), (1,)), ((), ())), preferred_element_type=F32)
    for i in range(4):
        part = r[i * LOC:(i + 1) * LOC, :]
        if i >= 2:
            part = part + jnp.concatenate([bct[i - 2]] * 6, axis=1)
        (k_ref, v_ref)[i // 2][i % 2, clip] = part.astype(BF16)


def writer(enc_v, kc_v, vc_v, am, wct, bct, enc_o, kc_o, vc_o, kl, vl, sem, last_sem):
    t = lax.axis_index("tp")
    c, k = t // 2, t % 2
    cx, cy = c % 2, c // 2
    cdg = 2 * (1 - cy) + (1 - cx)
    last = cdg * PER_CHIP + 2

    def copies(clip):
        cps = [pltpu.make_async_copy(kc_v.at[l, clip], kc_o.at[l, clip], sem) for l in range(2)]
        cps += [pltpu.make_async_copy(vc_v.at[l, clip], vc_o.at[l, clip], sem) for l in range(2)]
        return cps + [pltpu.make_async_copy(enc_v.at[clip], enc_o.at[clip], sem)]

    def start(i, _):
        for cp in copies(lax.rem(last + 1 + i, CLIPS)):
            cp.start()
        return 0
    lax.fori_loop(0, CLIPS - 1, start, 0)
    cps = [pltpu.make_async_copy(am.at[2, k, c], enc_o.at[last], last_sem)]
    cps[0].start()
    cache_rows(0, natural_order(am, 2), wct, bct, kl, vl)
    for l in range(2):
        cps.append(pltpu.make_async_copy(kl.at[l, 0], kc_o.at[l, last], last_sem))
        cps.append(pltpu.make_async_copy(vl.at[l, 0], vc_o.at[l, last], last_sem))
    for cp in cps[1:]:
        cp.start()

    def finish(i, _):
        for cp in copies(lax.rem(last + 1 + i, CLIPS)):
            cp.wait()
        return 0
    lax.fori_loop(0, CLIPS - 1, finish, 0)
    for cp in cps:
        cp.wait()


def device_body(hidden_loc, ln1_gain, ln1_bias, w_q, b_q, w_k, w_v, b_v, w_o, b_o, ln2_gain, ln2_bias, w_fc1, b_fc1, w_fc2, b_fc2, post_gain, post_bias, w_ck, w_cv, b_cv):
    anyspec = pl.BlockSpec(memory_space=pl.ANY)
    vspec = pl.BlockSpec(memory_space=pltpu.VMEM)
    dma = pltpu.SemaphoreType.DMA
    cache = (2, CLIPS, LOC, FRAMES)
    parts = pl.pallas_call(
        kernel,
        out_shape=(
            pltpu.VMEM((CLIPS, FR, D), BF16), pltpu.VMEM(cache, BF16), pltpu.VMEM(cache, BF16),
            pltpu.VMEM((PER_CHIP, 2, 4, FR, D), BF16),
            pltpu.VMEM((4 * LOC, D), BF16),
            pltpu.VMEM((2, LOC, LOC), F32),
        ),
        in_specs=[anyspec] * 21,
        out_specs=(vspec,) * 6,
        scratch_shapes=[
            pltpu.VMEM((LOC,), BF16), pltpu.VMEM((LOC,), BF16), pltpu.VMEM((HID,), BF16), pltpu.VMEM((2, LOC), BF16),
            *([pltpu.VMEM((D,), BF16)] * 8),
            pltpu.VMEM((PER_CHIP, HALF, D), BF16),
            pltpu.VMEM((2, PER_CHIP, FR // 2, D), BF16),
            pltpu.VMEM((PER_CHIP, HALF, D), BF16),
            pltpu.VMEM((PER_CHIP, HALF, D), BF16),
            pltpu.VMEM((3, D, NQ), BF16),
            pltpu.VMEM((NQ, D), BF16),
            pltpu.VMEM((D, NH), BF16),
            pltpu.VMEM((NH, D), BF16),
            pltpu.VMEM((4, 8, LOC), F32),
            pltpu.VMEM((4, FRAMES, NQ), BF16),
            pltpu.VMEM((2, FRAMES, LOC), BF16),
            pltpu.VMEM((2, FRAMES, LOC), BF16),
            pltpu.VMEM((4, FRAMES, HID), BF16),
            pltpu.VMEM((HALF, D), F32),
            pltpu.VMEM((9, 4, 2, FR, D), BF16),
            dma((2, 5)), dma((2, 6)), dma((2, 2)), dma((6, 5)), dma((6, 4)), dma((3,)), dma((3,)),
            dma((2, 3)), dma((2, 3)), dma((2, 3)), dma((2, 3)),
            dma((3, 2)), dma((3, 2)), dma((3, 4)), dma((3, 3, 2)), dma((3, 4)),
            dma((3, 2)), dma((3, 2)), dma((3, 4)), dma((3, 3, 2)), dma((3, 4)),
            dma((4, 2)), dma((12,)), pltpu.SemaphoreType.REGULAR((3,)),
        ],
        compiler_params=pltpu.CompilerParams(collective_id=0, has_side_effects=True, vmem_limit_bytes=48500000),
        name="encoder_layer",
    )(hidden_loc, w_q, w_k, w_v, w_o, w_fc1, w_fc2, w_ck, w_cv,
      b_q, b_v, b_fc1, b_cv, ln1_gain, ln1_bias, ln2_gain, ln2_bias, post_gain, post_bias, b_o, b_fc2)

    enc, kc, vc = pl.pallas_call(
        writer,
        out_shape=(jax.ShapeDtypeStruct((CLIPS, FR, D), BF16), jax.ShapeDtypeStruct(cache, BF16), jax.ShapeDtypeStruct(cache, BF16)),
        in_specs=[vspec] * 6,
        out_specs=(anyspec,) * 3,
        scratch_shapes=[pltpu.VMEM((2, 1, LOC, FRAMES), BF16), pltpu.VMEM((2, 1, LOC, FRAMES), BF16), dma, dma],
        compiler_params=pltpu.CompilerParams(vmem_limit_bytes=8000000),
        name="writer",
    )(*parts)

    def heads_last(cached):
        return cached.reshape(2, CLIPS, LOC // HEAD_DIM, HEAD_DIM, FRAMES).transpose(0, 1, 4, 2, 3)
    return enc, heads_last(kc), heads_last(vc)


def solution(mesh):
    in_specs = (P("dp", "tp", None), P(), P(), P(None, "tp"), P("tp"), P(None, "tp"), P(None, "tp"), P("tp"), P("tp", None), P(), P(), P(), P(None, "tp"), P("tp"), P("tp", None), P(), P(), P(), P(None, None, "tp"), P(None, None, "tp"), P(None, "tp"))
    out_specs = (P("dp", "tp", None), P(None, "dp", None, "tp", None), P(None, "dp", None, "tp", None))
    return jax.shard_map(device_body, mesh=mesh, in_specs=in_specs, out_specs=out_specs, check_vma=False)
```

```python
import functools

import jax
import jax.numpy as jnp
from jax import lax
from jax.experimental import pallas as pl
from jax.experimental.pallas import tpu as pltpu
from jax.sharding import PartitionSpec as P

HEAD_DIM = 64
ATTN_SCALE = HEAD_DIM ** -0.25
LN_EPS = 1e-5
CLIPS = 12
PER_CHIP = 3
FR = 96
HALF = 4 * FR
FRAMES = 8 * FR
D = 1024
LOC = 128
HID = 512
NQ = 4 * LOC
NH = 4 * HID
QROWS = 256
F32, BF16 = jnp.float32, jnp.bfloat16


def ln_rows(values, gain, bias):
    centered = values - jnp.mean(values, axis=-1, keepdims=True)
    row_var = jnp.mean(centered * centered, axis=-1, keepdims=True)
    return (centered * lax.rsqrt(row_var + LN_EPS) * gain + bias).astype(BF16)


def kernel(hid, wq_h, wk_h, wv_h, wo_h, w1_h, w2_h, ck_h, cv_h,
           bq_h, bv_h, b1_h, bcv_h, ln1g_h, ln1b_h, ln2g_h, ln2b_h, postg_h, postb_h, bo_h, bfc2_h,
           enc_o, kc_o, vc_o, am, wct, bct,
           bq_v, bv_v, b1_v, bcv_v, ln1g, ln1b, ln2g, ln2b, postg, postb, bo_v, bfc2, xb, xrel, ex_s, ex_r, wqkv, wo, w1, w2, bias, qkv, kz, vz, g, acc, ea,
           x_r, x_s, xrel_r, w_r, w_s, b_r, b_s, am_r, am_s, ex_rs, ex_ss, ex_x, ex_y, ex_d, ex_f, ex_g, es_x, es_y, es_d, es_f, es_g, c_s, v_s, free):
    t = lax.axis_index("tp")
    c, k = t // 2, t % 2
    cx, cy = c % 2, c // 2
    cxn = 2 * cy + (1 - cx)
    cyn = 2 * (1 - cy) + cx
    cdg = 2 * (1 - cy) + (1 - cx)
    ks = 1 - k
    sib, xn, yn = 2 * c + ks, 2 * cxn + k, 2 * cyn + k

    def remote(src, dst, ssem, rsem, dev):
        return pltpu.make_async_remote_copy(src_ref=src, dst_ref=dst, send_sem=ssem, recv_sem=rsem,
                                            device_id={"tp": dev}, device_id_type=pl.DeviceIdType.MESH)

    def wait_recv(ref, rsem):
        pltpu.make_async_copy(ref, ref, rsem).wait()

    def row(ref):
        return ref[...].astype(F32).reshape(1, ref.shape[0])

    barrier = pltpu.get_barrier_semaphore()
    for peer in (sib, xn, yn):
        pl.semaphore_signal(barrier, inc=1, device_id={"tp": peer}, device_id_type=pl.DeviceIdType.MESH)
    pl.semaphore_wait(barrier, 3)

    def xclips(late):
        return pl.ds(2, 1) if late else pl.ds(0, 2)

    def xslot(chip, late):
        return xb.at[xclips(late), pl.ds(chip * FR, FR), :]

    def xhalf(chip, late, hf):
        return xb.at[xclips(late), pl.ds(chip * FR + hf * (FR // 2), FR // 2), :]

    def xsource(chip, late):
        return hid.at[pl.ds(chip * PER_CHIP + 2, 1) if late else pl.ds(chip * PER_CHIP, 2)]

    def wfull(i, chip):
        if i < 3:
            return wqkv.at[i, :, pl.ds(pl.multiple_of(chip * LOC, LOC), LOC)]
        if i == 3:
            return wo.at[pl.ds(chip * LOC, LOC)]
        if i == 4:
            return w1.at[:, pl.ds(pl.multiple_of(chip * HID, HID), HID)]
        return w2.at[pl.ds(chip * HID, HID)]

    def whalf(i, chip, hf):
        if i < 3:
            return wqkv.at[i, pl.ds(hf * (D // 2), D // 2), pl.ds(pl.multiple_of(chip * LOC, LOC), LOC)]
        if i == 3:
            return wo.at[pl.ds(chip * LOC + hf * (LOC // 2), LOC // 2)]
        if i == 4:
            return w1.at[pl.ds(hf * (D // 2), D // 2), pl.ds(pl.multiple_of(chip * HID, HID), HID)]
        return w2.at[pl.ds(chip * HID + hf * (HID // 2), HID // 2)]

    w_hbm = (wq_h, wk_h, wv_h, wo_h, w1_h, w2_h)
    sends = []

    def go(src, dst, ssem, rsem, dev):
        cp = remote(src, dst, ssem, rsem, dev)
        cp.start()
        sends.append(cp)

    def send_direct(i):
        wait_recv(wfull(i, c), w_r.at[i, 0])
        go(wfull(i, c), wfull(i, c), w_s.at[i, 0], w_r.at[i, 1], xn)
        go(wfull(i, c), wfull(i, c), w_s.at[i, 1], w_r.at[i, 2], yn)

    def send_halves(i, part):
        if part == 0:
            wait_recv(wfull(i, c), w_r.at[i, 0])
        mine_x, mine_y = whalf(i, c, part), whalf(i, c, 1 - part)
        go(mine_x, mine_x, w_s.at[i, 4 * part], w_r.at[i, 1 + 4 * part], xn)
        go(mine_y, mine_y, w_s.at[i, 4 * part + 1], w_r.at[i, 2 + 4 * part], yn)

    def relay(i):
        wait_recv(wfull(i, cxn) if i < 4 else whalf(i, cxn, 0), w_r.at[i, 1])
        go(whalf(i, cxn, 0), whalf(i, cxn, 0), w_s.at[i, 2], w_r.at[i, 3], yn)
        wait_recv(wfull(i, cyn) if i < 4 else whalf(i, cyn, 1), w_r.at[i, 2])
        go(whalf(i, cyn, 1), whalf(i, cyn, 1), w_s.at[i, 3], w_r.at[i, 4], xn)

    def wait_rest(i):
        if i >= 4:
            wait_recv(whalf(i, cxn, 1), w_r.at[i, 5])
            wait_recv(whalf(i, cyn, 0), w_r.at[i, 6])
        wait_recv(whalf(i, cdg, 0), w_r.at[i, 3])
        wait_recv(whalf(i, cdg, 1), w_r.at[i, 4])

    def send_x(late):
        for hf, dev in enumerate((xn, yn)):
            src = xsource(cdg, late).at[:, pl.ds(hf * (FR // 2), FR // 2), :]
            go(src, xrel.at[hf, xclips(late)], x_s.at[late, hf], xrel_r.at[late, hf], dev)
        go(xsource(cxn, late), xslot(c, late), x_s.at[late, 2], x_r.at[late, 1], xn)
        go(xsource(cyn, late), xslot(c, late), x_s.at[late, 3], x_r.at[late, 2], yn)

    def relay_x(late):
        for hf, (chip, dev) in enumerate(((cxn, yn), (cyn, xn))):
            piece = xrel.at[hf, xclips(late)]
            wait_recv(piece, xrel_r.at[late, hf])
            go(piece, xhalf(chip, late, hf), x_s.at[late, 4 + hf], x_r.at[late, 3 + hf], dev)

    def ln1_stage(j):
        def body(b, _):
            vals = xb[j, pl.ds(b * FR, FR), :].astype(F32)
            am[j, k, b] = ln_rows(vals, row(ln1g), row(ln1b))
            return 0
        lax.fori_loop(0, 4, body, 0)
        cp = remote(am.at[j, k], am.at[j, k], am_s.at[0, j], am_r.at[0, j], sib)
        cp.start()
        a_sends.append(cp)

    def wait_x(late):
        for r, chip in ((0, c), (1, cxn), (2, cyn)):
            wait_recv(xslot(chip, late), x_r.at[late, r])
        for hf in range(2):
            wait_recv(xhalf(cdg, late, hf), x_r.at[late, 3 + hf])

    send_x(0)
    vec_copies = [pltpu.make_async_copy(src, dst, v_s.at[i]) for i, (src, dst) in enumerate((
        (bq_h, bq_v), (bv_h, bv_v), (b1_h, b1_v), (bcv_h, bcv_v), (ln1g_h, ln1g), (ln1b_h, ln1b),
        (ln2g_h, ln2g), (ln2b_h, ln2b), (postg_h, postg), (postb_h, postb), (bo_h, bo_v), (bfc2_h, bfc2)))]
    for cp in vec_copies:
        cp.start()
    for i in range(3):
        pltpu.make_async_copy(w_hbm[i], wfull(i, c), w_r.at[i, 0]).start()
    for late in range(2):
        pltpu.make_async_copy(xsource(c, late), xslot(c, late), x_r.at[late, 0]).start()
    for i in range(3, 6):
        pltpu.make_async_copy(w_hbm[i], wfull(i, c), w_r.at[i, 0]).start()
    wc_copies = []
    for i, src in enumerate((ck_h.at[0], ck_h.at[1], cv_h.at[0], cv_h.at[1])):
        for hf in range(2):
            cp = pltpu.make_async_copy(src.at[pl.ds(hf * 512, 512)], qkv.at[i, pl.ds(0, 512), pl.ds(hf * LOC, LOC)], c_s.at[i, hf])
            cp.start()
            wc_copies.append(cp)
    for cp in vec_copies:
        cp.wait()
    bias[c, 0:1, :] = row(bq_v)
    bias[c, 1:2, :] = row(bv_v)
    b1_row = row(b1_v)
    for q in range(4):
        bias[c, 2 + q:3 + q, :] = b1_row[:, q * LOC:(q + 1) * LOC]
    for l in range(2):
        bct[l] = jnp.transpose(jnp.broadcast_to(bcv_v[l:l + 1, :].astype(F32), (LOC, LOC)))
    send_direct(0)
    relay_x(0)
    for r, dev in enumerate((xn, yn)):
        go(bias.at[c], bias.at[c], b_s.at[r], b_r.at[r], dev)
    for i in range(1, 3):
        send_direct(i)

    a_sends = []
    wait_x(0)
    for j in range(2):
        ln1_stage(j)
    send_direct(3)
    for cp in wc_copies:
        cp.wait()
    for i in range(4):
        for hf in range(2):
            wct[i * LOC:(i + 1) * LOC, hf * 512:(hf + 1) * 512] = jnp.transpose(qkv[i, 0:512, hf * LOC:(hf + 1) * LOC])
    for r, chip in enumerate((cxn, cyn, cdg)):
        wait_recv(bias.at[chip], b_r.at[r])
        if r == 0:
            go(bias.at[cxn], bias.at[cxn], b_s.at[2], b_r.at[2], yn)
    for i in range(3):
        relay(i)
    send_halves(4, 0)
    relay(3)
    send_halves(4, 1)
    send_halves(5, 0)
    send_halves(5, 1)
    for i in range(3):
        wait_rest(i)

    def row_of(r):
        return jnp.concatenate([bias[n, r:r + 1, :] for n in range(4)], axis=1)

    lane = lax.broadcasted_iota(jnp.int32, (FRAMES, LOC), 1)

    def attention_stage(j):
        wait_recv(am.at[j, ks], am_r.at[0, j])
        bq, bv = row_of(0), row_of(1)

        def project(r, _):
            rows = pl.ds(r * HALF, HALF)
            a = am[j, r].reshape(HALF, D)
            qkv[0, rows, :] = ((jnp.dot(a, wqkv[0], preferred_element_type=F32) + bq) * ATTN_SCALE).astype(BF16)
            qkv[1, rows, :] = (jnp.dot(a, wqkv[1], preferred_element_type=F32) * ATTN_SCALE).astype(BF16)
            qkv[2, rows, :] = (jnp.dot(a, wqkv[2], preferred_element_type=F32) + bv).astype(BF16)
            return 0
        lax.fori_loop(0, 2, project, 0)

        def pair(p, _):
            cols = pl.ds(pl.multiple_of(p * LOC, LOC), LOC)
            kp, vp = qkv[1, :, cols], qkv[2, :, cols]
            zero = jnp.zeros_like(kp)
            kz[0] = jnp.where(lane < HEAD_DIM, kp, zero)
            kz[1] = jnp.where(lane < HEAD_DIM, zero, kp)
            vz[0] = jnp.where(lane < HEAD_DIM, vp, zero)
            vz[1] = jnp.where(lane < HEAD_DIM, zero, vp)

            def attend(r, _):
                rows = pl.ds(r * QROWS, QROWS)
                qb = qkv[0, rows, cols]
                out = None
                for hh in range(2):
                    s = lax.dot_general(qb, kz[hh], (((1,), (1,)), ((), ())), preferred_element_type=F32)
                    e = jnp.exp(s - jnp.max(s, axis=-1, keepdims=True))
                    prob = (e * (1.0 / jnp.sum(e, axis=-1, keepdims=True))).astype(BF16)
                    part = jnp.dot(prob, vz[hh], preferred_element_type=F32)
                    out = part if out is None else out + part
                qkv[3, rows, cols] = out.astype(BF16)
                return 0
            lax.fori_loop(0, FRAMES // QROWS, attend, 0)
            return 0
        lax.fori_loop(0, 4, pair, 0)

    own = pl.ds(k * HALF, HALF)
    oth = pl.ds(ks * HALF, HALF)

    def swap_partials(phase, j, lhs, weight):
        for n in range(2):
            cols = slice(n * 512, (n + 1) * 512)
            ex_s[j, :, cols] = jnp.dot(lhs(oth), weight[:, cols], preferred_element_type=F32).astype(BF16)
        cp = remote(ex_s.at[j], ex_r.at[j], ex_ss.at[phase, j], ex_rs.at[phase, j], sib)
        cp.start()
        for n in range(2):
            cols = slice(n * 512, (n + 1) * 512)
            acc[:, cols] = jnp.dot(lhs(own), weight[:, cols], preferred_element_type=F32)
        wait_recv(ex_r.at[j], ex_rs.at[phase, j])
        cp.wait_send()

    m_sends = []

    def output_stage(j):
        swap_partials(0, j, lambda rows: qkv[3, rows, :], wo)
        a_sends[j].wait_send()

        def body(b, _):
            rows = pl.ds(b * FR, FR)
            out = (acc[rows, :] + ex_r[j, rows, :].astype(F32) + row(bo_v)).astype(BF16)
            h = (xb[j, rows, :].astype(F32) + out.astype(F32)).astype(BF16)
            xb[j, rows, :] = h
            am[j, k, b] = ln_rows(h.astype(F32), row(ln2g), row(ln2b))
            return 0
        lax.fori_loop(0, 4, body, 0)
        cp = remote(am.at[j, k], am.at[j, k], am_s.at[1, j], am_r.at[1, j], sib)
        cp.start()
        m_sends.append(cp)

    def epiece(group, j, core, hf):
        return ea.at[3 * group + j, pl.ds(2 * hf, 2), core]

    def up_stage(j):
        wait_recv(am.at[j, ks], am_r.at[1, j])

        def up(i, _):
            n, r = i // 2, i % 2
            rows = pl.ds(r * HALF, HALF)
            cols = pl.ds(pl.multiple_of(n * HID, HID), HID)
            b1 = jnp.concatenate([bias[n, 2 + q:3 + q, :] for q in range(4)], axis=1)
            u = jnp.dot(am[j, r].reshape(HALF, D), w1[:, cols], preferred_element_type=F32) + b1
            act = (0.5 * u * (1.0 + lax.erf(u * (2.0 ** -0.5)))).astype(BF16)
            if j == 1:
                qkv[n, rows, :] = act
            else:
                g[n, rows, :] = act
            return 0
        lax.fori_loop(0, 8, up, 0)
        m_sends[j].wait_send()
        for peer in (sib, xn, yn):
            pl.semaphore_signal(free.at[j], inc=1, device_id={"tp": peer}, device_id_type=pl.DeviceIdType.MESH)

    def down_stage(j):
        hidden = qkv if j == 1 else g
        swap_partials(1, j, lambda rows: jnp.concatenate([hidden[n, rows, :] for n in range(4)], axis=1), w2)
        if j == 0:
            relay_x(1)

        def post(b, _):
            rows = pl.ds(b * FR, FR)
            out = (acc[rows, :] + ex_r[j, rows, :].astype(F32) + row(bfc2)).astype(BF16)
            h2 = (xb[j, rows, :].astype(F32) + out.astype(F32)).astype(BF16)
            ea[j, b, k] = ln_rows(h2.astype(F32), row(postg), row(postb))
            return 0
        lax.fori_loop(0, 4, post, 0)
        for hf in range(2):
            go(epiece(0, j, k, hf), epiece(1, j, k, hf), es_x.at[j, hf], ex_x.at[j, hf], xn)
            go(epiece(0, j, k, 1 - hf), epiece(2, j, k, 1 - hf), es_y.at[j, 1 - hf], ex_y.at[j, 1 - hf], yn)
        for hf in range(2):
            go(epiece(0, j, k, hf), epiece(0, j, k, hf), es_f.at[0, j, hf], ex_f.at[0, j, hf], sib)

    def forward(group, j, hf):
        go(epiece(group, j, k, hf), epiece(group, j, k, hf), es_f.at[group, j, hf], ex_f.at[group, j, hf], sib)

    def relay_e(j):
        pl.semaphore_wait(free.at[j], 3)
        wait_recv(epiece(1, j, k, 0), ex_x.at[j, 0])
        for b in range(2):
            go(ea.at[PER_CHIP + j, b, k], am.at[j, k, b], es_d.at[j, b], ex_d.at[j, b], yn)
        forward(1, j, 0)
        wait_recv(epiece(2, j, k, 1), ex_y.at[j, 1])
        for b in range(2, 4):
            go(ea.at[2 * PER_CHIP + j, b, k], am.at[j, k, b], es_d.at[j, b], ex_d.at[j, b], xn)
        forward(2, j, 1)
        wait_recv(epiece(1, j, k, 1), ex_x.at[j, 1])
        forward(1, j, 1)
        wait_recv(epiece(2, j, k, 0), ex_y.at[j, 0])
        forward(2, j, 0)

    def take_diagonal(j):
        for b in (0, 2, 1, 3):
            piece = am.at[j, k, b]
            wait_recv(piece, ex_d.at[j, b])
            go(piece, piece, es_g.at[j, b], ex_g.at[j, b], sib)

    def wait_diagonal(j):
        for b in range(4):
            wait_recv(am.at[j, ks, b], ex_g.at[j, b])

    def write_caches(clip, ec):
        cache_rows(clip, ec, wct, bct, kc_o, vc_o)

    def near_cache(group, j):
        chip = jnp.where(group == 0, c, jnp.where(group == 1, cxn, cyn))
        clip = chip * PER_CHIP + j
        for hf in range(2):
            wait_recv(ea.at[3 * group + j, pl.ds(2 * hf, 2), ks], ex_f.at[group, j, hf])
        enc_o[clip] = ea[3 * group + j, c, k]
        write_caches(clip, ea[3 * group + j].reshape(FRAMES, D))

    def far_cache(j):
        clip = cdg * PER_CHIP + j
        wait_diagonal(j)
        enc_o[clip] = am[j, k, c]
        write_caches(clip, natural_order(am, j))

    attention_stage(0)
    wait_rest(3)
    output_stage(0)
    attention_stage(1)
    relay(4)
    output_stage(1)
    relay(5)
    send_x(1)
    wait_rest(4)
    up_stage(0)
    up_stage(1)
    wait_rest(5)
    down_stage(0)
    down_stage(1)
    wait_x(1)
    ln1_stage(2)
    attention_stage(2)
    relay_e(0)
    output_stage(2)
    up_stage(2)
    down_stage(2)
    relay_e(1)

    def first(i, _):
        near_cache(jnp.where(i < 3, 0, 1 + (i + 1) % 2), jnp.where(i < 3, i, (i - 3) // 2))
        return 0
    lax.fori_loop(0, 7, first, 0)
    take_diagonal(0)
    far_cache(0)
    relay_e(2)

    def second(i, _):
        near_cache(1 + i, 2)
        return 0
    lax.fori_loop(0, 2, second, 0)
    take_diagonal(1)
    far_cache(1)
    take_diagonal(2)
    wait_diagonal(2)
    for cp in sends:
        cp.wait_send()


def natural_order(am, j):
    return jnp.concatenate([am[j, core, b] for b in range(4) for core in range(2)], axis=0)


def cache_rows(clip, ec, wct, bct, k_ref, v_ref):
    r = lax.dot_general(wct[...], ec, (((1,), (1,)), ((), ())), preferred_element_type=F32)
    for i in range(4):
        part = r[i * LOC:(i + 1) * LOC, :]
        if i >= 2:
            part = part + jnp.concatenate([bct[i - 2]] * 6, axis=1)
        (k_ref, v_ref)[i // 2][i % 2, clip] = part.astype(BF16)


def writer(enc_v, kc_v, vc_v, am, wct, bct, enc_o, kc_o, vc_o, kl, vl, sem, last_sem):
    t = lax.axis_index("tp")
    c, k = t // 2, t % 2
    cx, cy = c % 2, c // 2
    cdg = 2 * (1 - cy) + (1 - cx)
    last = cdg * PER_CHIP + 2

    def copies(clip):
        cps = [pltpu.make_async_copy(kc_v.at[l, clip], kc_o.at[l, clip], sem) for l in range(2)]
        cps += [pltpu.make_async_copy(vc_v.at[l, clip], vc_o.at[l, clip], sem) for l in range(2)]
        return cps + [pltpu.make_async_copy(enc_v.at[clip], enc_o.at[clip], sem)]

    def start(i, _):
        for cp in copies(lax.rem(last + 1 + i, CLIPS)):
            cp.start()
        return 0
    lax.fori_loop(0, CLIPS - 1, start, 0)
    cps = [pltpu.make_async_copy(am.at[2, k, c], enc_o.at[last], last_sem)]
    cps[0].start()
    cache_rows(0, natural_order(am, 2), wct, bct, kl, vl)
    for l in range(2):
        cps.append(pltpu.make_async_copy(kl.at[l, 0], kc_o.at[l, last], last_sem))
        cps.append(pltpu.make_async_copy(vl.at[l, 0], vc_o.at[l, last], last_sem))
    for cp in cps[1:]:
        cp.start()

    def finish(i, _):
        for cp in copies(lax.rem(last + 1 + i, CLIPS)):
            cp.wait()
        return 0
    lax.fori_loop(0, CLIPS - 1, finish, 0)
    for cp in cps:
        cp.wait()


def device_body(hidden_loc, ln1_gain, ln1_bias, w_q, b_q, w_k, w_v, b_v, w_o, b_o, ln2_gain, ln2_bias, w_fc1, b_fc1, w_fc2, b_fc2, post_gain, post_bias, w_ck, w_cv, b_cv):
    anyspec = pl.BlockSpec(memory_space=pl.ANY)
    vspec = pl.BlockSpec(memory_space=pltpu.VMEM)
    dma = pltpu.SemaphoreType.DMA
    cache = (2, CLIPS, LOC, FRAMES)
    parts = pl.pallas_call(
        kernel,
        out_shape=(
            pltpu.VMEM((CLIPS, FR, D), BF16), pltpu.VMEM(cache, BF16), pltpu.VMEM(cache, BF16),
            pltpu.VMEM((PER_CHIP, 2, 4, FR, D), BF16),
            pltpu.VMEM((4 * LOC, D), BF16),
            pltpu.VMEM((2, LOC, LOC), F32),
        ),
        in_specs=[anyspec] * 21,
        out_specs=(vspec,) * 6,
        scratch_shapes=[
            pltpu.VMEM((LOC,), BF16), pltpu.VMEM((LOC,), BF16), pltpu.VMEM((HID,), BF16), pltpu.VMEM((2, LOC), BF16),
            *([pltpu.VMEM((D,), BF16)] * 8),
            pltpu.VMEM((PER_CHIP, HALF, D), BF16),
            pltpu.VMEM((2, PER_CHIP, FR // 2, D), BF16),
            pltpu.VMEM((PER_CHIP, HALF, D), BF16),
            pltpu.VMEM((PER_CHIP, HALF, D), BF16),
            pltpu.VMEM((3, D, NQ), BF16),
            pltpu.VMEM((NQ, D), BF16),
            pltpu.VMEM((D, NH), BF16),
            pltpu.VMEM((NH, D), BF16),
            pltpu.VMEM((4, 8, LOC), F32),
            pltpu.VMEM((4, FRAMES, NQ), BF16),
            pltpu.VMEM((2, FRAMES, LOC), BF16),
            pltpu.VMEM((2, FRAMES, LOC), BF16),
            pltpu.VMEM((4, FRAMES, HID), BF16),
            pltpu.VMEM((HALF, D), F32),
            pltpu.VMEM((9, 4, 2, FR, D), BF16),
            dma((2, 5)), dma((2, 6)), dma((2, 2)), dma((6, 7)), dma((6, 6)), dma((3,)), dma((3,)),
            dma((2, 3)), dma((2, 3)), dma((2, 3)), dma((2, 3)),
            dma((3, 2)), dma((3, 2)), dma((3, 4)), dma((3, 3, 2)), dma((3, 4)),
            dma((3, 2)), dma((3, 2)), dma((3, 4)), dma((3, 3, 2)), dma((3, 4)),
            dma((4, 2)), dma((12,)), pltpu.SemaphoreType.REGULAR((3,)),
        ],
        compiler_params=pltpu.CompilerParams(collective_id=0, has_side_effects=True, vmem_limit_bytes=48500000),
        name="encoder_layer",
    )(hidden_loc, w_q, w_k, w_v, w_o, w_fc1, w_fc2, w_ck, w_cv,
      b_q, b_v, b_fc1, b_cv, ln1_gain, ln1_bias, ln2_gain, ln2_bias, post_gain, post_bias, b_o, b_fc2)

    enc, kc, vc = pl.pallas_call(
        writer,
        out_shape=(jax.ShapeDtypeStruct((CLIPS, FR, D), BF16), jax.ShapeDtypeStruct(cache, BF16), jax.ShapeDtypeStruct(cache, BF16)),
        in_specs=[vspec] * 6,
        out_specs=(anyspec,) * 3,
        scratch_shapes=[pltpu.VMEM((2, 1, LOC, FRAMES), BF16), pltpu.VMEM((2, 1, LOC, FRAMES), BF16), dma, dma],
        compiler_params=pltpu.CompilerParams(vmem_limit_bytes=8000000),
        name="writer",
    )(*parts)

    def heads_last(cached):
        return cached.reshape(2, CLIPS, LOC // HEAD_DIM, HEAD_DIM, FRAMES).transpose(0, 1, 4, 2, 3)
    return enc, heads_last(kc), heads_last(vc)


def solution(mesh):
    in_specs = (P("dp", "tp", None), P(), P(), P(None, "tp"), P("tp"), P(None, "tp"), P(None, "tp"), P("tp"), P("tp", None), P(), P(), P(), P(None, "tp"), P("tp"), P("tp", None), P(), P(), P(), P(None, None, "tp"), P(None, None, "tp"), P(None, "tp"))
    out_specs = (P("dp", "tp", None), P(None, "dp", None, "tp", None), P(None, "dp", None, "tp", None))
    return jax.shard_map(device_body, mesh=mesh, in_specs=in_specs, out_specs=out_specs, check_vma=False)
```

```python
import functools

import jax
import jax.numpy as jnp
from jax import lax
from jax.experimental import pallas as pl
from jax.experimental.pallas import tpu as pltpu
from jax.sharding import PartitionSpec as P

HEAD_DIM = 64
ATTN_SCALE = HEAD_DIM ** -0.25
LN_EPS = 1e-5
CLIPS = 12
PER_CHIP = 3
FR = 96
HALF = 4 * FR
FRAMES = 8 * FR
D = 1024
LOC = 128
HID = 512
NQ = 4 * LOC
NH = 4 * HID
QROWS = 256
F32, BF16 = jnp.float32, jnp.bfloat16


def ln_rows(values, gain, bias):
    centered = values - jnp.mean(values, axis=-1, keepdims=True)
    row_var = jnp.mean(centered * centered, axis=-1, keepdims=True)
    return (centered * lax.rsqrt(row_var + LN_EPS) * gain + bias).astype(BF16)


def kernel(hid, wq_h, wk_h, wv_h, wo_h, w1_h, w2_h, ck_h, cv_h,
           bq_h, bv_h, b1_h, bcv_h, ln1g_h, ln1b_h, ln2g_h, ln2b_h, postg_h, postb_h, bo_h, bfc2_h,
           enc_o, kc_o, vc_o, am, wct, bct,
           bq_v, bv_v, b1_v, bcv_v, ln1g, ln1b, ln2g, ln2b, postg, postb, bo_v, bfc2, xb, xrel, ex_s, ex_r, wqkv, wo, w1, w2, bias, qkv, kz, vz, g, acc, ea,
           x_r, x_s, xrel_r, w_r, w_s, b_r, b_s, am_r, am_s, ex_rs, ex_ss, ex_x, ex_y, ex_d, ex_f, ex_g, es_x, es_y, es_d, es_f, es_g, c_s, v_s, free):
    t = lax.axis_index("tp")
    c, k = t // 2, t % 2
    cx, cy = c % 2, c // 2
    cxn = 2 * cy + (1 - cx)
    cyn = 2 * (1 - cy) + cx
    cdg = 2 * (1 - cy) + (1 - cx)
    ks = 1 - k
    sib, xn, yn = 2 * c + ks, 2 * cxn + k, 2 * cyn + k

    def remote(src, dst, ssem, rsem, dev):
        return pltpu.make_async_remote_copy(src_ref=src, dst_ref=dst, send_sem=ssem, recv_sem=rsem,
                                            device_id={"tp": dev}, device_id_type=pl.DeviceIdType.MESH)

    def wait_recv(ref, rsem):
        pltpu.make_async_copy(ref, ref, rsem).wait()

    def row(ref):
        return ref[...].astype(F32).reshape(1, ref.shape[0])

    barrier = pltpu.get_barrier_semaphore()
    for peer in (sib, xn, yn):
        pl.semaphore_signal(barrier, inc=1, device_id={"tp": peer}, device_id_type=pl.DeviceIdType.MESH)
    pl.semaphore_wait(barrier, 3)

    def xclips(late):
        return pl.ds(2, 1) if late else pl.ds(0, 2)

    def xslot(chip, late):
        return xb.at[xclips(late), pl.ds(chip * FR, FR), :]

    def xhalf(chip, late, hf):
        return xb.at[xclips(late), pl.ds(chip * FR + hf * (FR // 2), FR // 2), :]

    def xsource(chip, late):
        return hid.at[pl.ds(chip * PER_CHIP + 2, 1) if late else pl.ds(chip * PER_CHIP, 2)]

    def wfull(i, chip):
        if i < 3:
            return wqkv.at[i, :, pl.ds(pl.multiple_of(chip * LOC, LOC), LOC)]
        if i == 3:
            return wo.at[pl.ds(chip * LOC, LOC)]
        if i == 4:
            return w1.at[:, pl.ds(pl.multiple_of(chip * HID, HID), HID)]
        return w2.at[pl.ds(chip * HID, HID)]

    def whalf(i, chip, hf):
        if i < 3:
            return wqkv.at[i, pl.ds(hf * (D // 2), D // 2), pl.ds(pl.multiple_of(chip * LOC, LOC), LOC)]
        if i == 3:
            return wo.at[pl.ds(chip * LOC + hf * (LOC // 2), LOC // 2)]
        if i == 4:
            return w1.at[pl.ds(hf * (D // 2), D // 2), pl.ds(pl.multiple_of(chip * HID, HID), HID)]
        return w2.at[pl.ds(chip * HID + hf * (HID // 2), HID // 2)]

    w_hbm = (wq_h, wk_h, wv_h, wo_h, w1_h, w2_h)
    sends = []

    def go(src, dst, ssem, rsem, dev):
        cp = remote(src, dst, ssem, rsem, dev)
        cp.start()
        sends.append(cp)

    def send_direct(i):
        wait_recv(wfull(i, c), w_r.at[i, 0])
        go(wfull(i, c), wfull(i, c), w_s.at[i, 0], w_r.at[i, 1], xn)
        go(wfull(i, c), wfull(i, c), w_s.at[i, 1], w_r.at[i, 2], yn)

    def send_halves(i, part):
        if part == 0:
            wait_recv(wfull(i, c), w_r.at[i, 0])
        mine_x, mine_y = whalf(i, c, part), whalf(i, c, 1 - part)
        go(mine_x, mine_x, w_s.at[i, 4 * part], w_r.at[i, 1 + 4 * part], xn)
        go(mine_y, mine_y, w_s.at[i, 4 * part + 1], w_r.at[i, 2 + 4 * part], yn)

    def relay(i):
        wait_recv(wfull(i, cxn) if i < 4 else whalf(i, cxn, 0), w_r.at[i, 1])
        go(whalf(i, cxn, 0), whalf(i, cxn, 0), w_s.at[i, 2], w_r.at[i, 3], yn)
        wait_recv(wfull(i, cyn) if i < 4 else whalf(i, cyn, 1), w_r.at[i, 2])
        go(whalf(i, cyn, 1), whalf(i, cyn, 1), w_s.at[i, 3], w_r.at[i, 4], xn)

    def wait_rest(i):
        if i >= 4:
            wait_recv(whalf(i, cxn, 1), w_r.at[i, 5])
            wait_recv(whalf(i, cyn, 0), w_r.at[i, 6])
        wait_recv(whalf(i, cdg, 0), w_r.at[i, 3])
        wait_recv(whalf(i, cdg, 1), w_r.at[i, 4])

    def send_x(late):
        for hf, dev in enumerate((xn, yn)):
            src = xsource(cdg, late).at[:, pl.ds(hf * (FR // 2), FR // 2), :]
            go(src, xrel.at[hf, xclips(late)], x_s.at[late, hf], xrel_r.at[late, hf], dev)
        go(xsource(cxn, late), xslot(c, late), x_s.at[late, 2], x_r.at[late, 1], xn)
        go(xsource(cyn, late), xslot(c, late), x_s.at[late, 3], x_r.at[late, 2], yn)

    def relay_x(late):
        for hf, (chip, dev) in enumerate(((cxn, yn), (cyn, xn))):
            piece = xrel.at[hf, xclips(late)]
            wait_recv(piece, xrel_r.at[late, hf])
            go(piece, xhalf(chip, late, hf), x_s.at[late, 4 + hf], x_r.at[late, 3 + hf], dev)

    def ln1_stage(j):
        def body(b, _):
            vals = xb[j, pl.ds(b * FR, FR), :].astype(F32)
            am[j, k, b] = ln_rows(vals, row(ln1g), row(ln1b))
            return 0
        lax.fori_loop(0, 4, body, 0)
        cp = remote(am.at[j, k], am.at[j, k], am_s.at[0, j], am_r.at[0, j], sib)
        cp.start()
        a_sends.append(cp)

    def wait_x(late):
        for r, chip in ((0, c), (1, cxn), (2, cyn)):
            wait_recv(xslot(chip, late), x_r.at[late, r])
        for hf in range(2):
            wait_recv(xhalf(cdg, late, hf), x_r.at[late, 3 + hf])

    send_x(0)
    vec_copies = [pltpu.make_async_copy(src, dst, v_s.at[i]) for i, (src, dst) in enumerate((
        (bq_h, bq_v), (bv_h, bv_v), (b1_h, b1_v), (bcv_h, bcv_v), (ln1g_h, ln1g), (ln1b_h, ln1b),
        (ln2g_h, ln2g), (ln2b_h, ln2b), (postg_h, postg), (postb_h, postb), (bo_h, bo_v), (bfc2_h, bfc2)))]
    for cp in vec_copies:
        cp.start()
    for i in range(3):
        pltpu.make_async_copy(w_hbm[i], wfull(i, c), w_r.at[i, 0]).start()
    for late in range(2):
        pltpu.make_async_copy(xsource(c, late), xslot(c, late), x_r.at[late, 0]).start()
    for i in range(3, 6):
        pltpu.make_async_copy(w_hbm[i], wfull(i, c), w_r.at[i, 0]).start()
    wc_copies = []
    for i, src in enumerate((ck_h.at[0], ck_h.at[1], cv_h.at[0], cv_h.at[1])):
        for hf in range(2):
            cp = pltpu.make_async_copy(src.at[pl.ds(hf * 512, 512)], qkv.at[i, pl.ds(0, 512), pl.ds(hf * LOC, LOC)], c_s.at[i, hf])
            cp.start()
            wc_copies.append(cp)
    for cp in vec_copies:
        cp.wait()
    bias[c, 0:1, :] = row(bq_v)
    bias[c, 1:2, :] = row(bv_v)
    b1_row = row(b1_v)
    for q in range(4):
        bias[c, 2 + q:3 + q, :] = b1_row[:, q * LOC:(q + 1) * LOC]
    for l in range(2):
        bct[l] = jnp.transpose(jnp.broadcast_to(bcv_v[l:l + 1, :].astype(F32), (LOC, LOC)))
    send_direct(0)
    relay_x(0)
    for r, dev in enumerate((xn, yn)):
        go(bias.at[c], bias.at[c], b_s.at[r], b_r.at[r], dev)
    for i in range(1, 3):
        send_direct(i)

    send_direct(3)
    send_halves(4, 0)
    a_sends = []
    wait_x(0)
    for j in range(2):
        ln1_stage(j)
    for cp in wc_copies:
        cp.wait()
    for i in range(4):
        for hf in range(2):
            wct[i * LOC:(i + 1) * LOC, hf * 512:(hf + 1) * 512] = jnp.transpose(qkv[i, 0:512, hf * LOC:(hf + 1) * LOC])
    for r, chip in enumerate((cxn, cyn, cdg)):
        wait_recv(bias.at[chip], b_r.at[r])
        if r == 0:
            go(bias.at[cxn], bias.at[cxn], b_s.at[2], b_r.at[2], yn)
    for i in range(3):
        relay(i)
    relay(3)
    send_halves(4, 1)
    send_halves(5, 0)
    send_halves(5, 1)
    for i in range(3):
        wait_rest(i)

    def row_of(r):
        return jnp.concatenate([bias[n, r:r + 1, :] for n in range(4)], axis=1)

    lane = lax.broadcasted_iota(jnp.int32, (FRAMES, LOC), 1)

    def attention_stage(j):
        wait_recv(am.at[j, ks], am_r.at[0, j])
        bq, bv = row_of(0), row_of(1)

        def project(r, _):
            rows = pl.ds(r * HALF, HALF)
            a = am[j, r].reshape(HALF, D)
            qkv[0, rows, :] = ((jnp.dot(a, wqkv[0], preferred_element_type=F32) + bq) * ATTN_SCALE).astype(BF16)
            qkv[1, rows, :] = (jnp.dot(a, wqkv[1], preferred_element_type=F32) * ATTN_SCALE).astype(BF16)
            qkv[2, rows, :] = (jnp.dot(a, wqkv[2], preferred_element_type=F32) + bv).astype(BF16)
            return 0
        lax.fori_loop(0, 2, project, 0)

        def pair(p, _):
            cols = pl.ds(pl.multiple_of(p * LOC, LOC), LOC)
            kp, vp = qkv[1, :, cols], qkv[2, :, cols]
            zero = jnp.zeros_like(kp)
            kz[0] = jnp.where(lane < HEAD_DIM, kp, zero)
            kz[1] = jnp.where(lane < HEAD_DIM, zero, kp)
            vz[0] = jnp.where(lane < HEAD_DIM, vp, zero)
            vz[1] = jnp.where(lane < HEAD_DIM, zero, vp)

            def attend(r, _):
                rows = pl.ds(r * QROWS, QROWS)
                qb = qkv[0, rows, cols]
                out = None
                for hh in range(2):
                    s = lax.dot_general(qb, kz[hh], (((1,), (1,)), ((), ())), preferred_element_type=F32)
                    e = jnp.exp(s - jnp.max(s, axis=-1, keepdims=True))
                    prob = (e * (1.0 / jnp.sum(e, axis=-1, keepdims=True))).astype(BF16)
                    part = jnp.dot(prob, vz[hh], preferred_element_type=F32)
                    out = part if out is None else out + part
                qkv[3, rows, cols] = out.astype(BF16)
                return 0
            lax.fori_loop(0, FRAMES // QROWS, attend, 0)
            return 0
        lax.fori_loop(0, 4, pair, 0)

    own = pl.ds(k * HALF, HALF)
    oth = pl.ds(ks * HALF, HALF)

    def swap_partials(phase, j, lhs, weight):
        for n in range(2):
            cols = slice(n * 512, (n + 1) * 512)
            ex_s[j, :, cols] = jnp.dot(lhs(oth), weight[:, cols], preferred_element_type=F32).astype(BF16)
        cp = remote(ex_s.at[j], ex_r.at[j], ex_ss.at[phase, j], ex_rs.at[phase, j], sib)
        cp.start()
        for n in range(2):
            cols = slice(n * 512, (n + 1) * 512)
            acc[:, cols] = jnp.dot(lhs(own), weight[:, cols], preferred_element_type=F32)
        wait_recv(ex_r.at[j], ex_rs.at[phase, j])
        cp.wait_send()

    m_sends = []

    def output_stage(j):
        swap_partials(0, j, lambda rows: qkv[3, rows, :], wo)
        a_sends[j].wait_send()

        def body(b, _):
            rows = pl.ds(b * FR, FR)
            out = (acc[rows, :] + ex_r[j, rows, :].astype(F32) + row(bo_v)).astype(BF16)
            h = (xb[j, rows, :].astype(F32) + out.astype(F32)).astype(BF16)
            xb[j, rows, :] = h
            am[j, k, b] = ln_rows(h.astype(F32), row(ln2g), row(ln2b))
            return 0
        lax.fori_loop(0, 4, body, 0)
        cp = remote(am.at[j, k], am.at[j, k], am_s.at[1, j], am_r.at[1, j], sib)
        cp.start()
        m_sends.append(cp)

    def epiece(group, j, core, hf):
        return ea.at[3 * group + j, pl.ds(2 * hf, 2), core]

    def up_stage(j):
        wait_recv(am.at[j, ks], am_r.at[1, j])

        def up(i, _):
            n, r = i // 2, i % 2
            rows = pl.ds(r * HALF, HALF)
            cols = pl.ds(pl.multiple_of(n * HID, HID), HID)
            b1 = jnp.concatenate([bias[n, 2 + q:3 + q, :] for q in range(4)], axis=1)
            u = jnp.dot(am[j, r].reshape(HALF, D), w1[:, cols], preferred_element_type=F32) + b1
            act = (0.5 * u * (1.0 + lax.erf(u * (2.0 ** -0.5)))).astype(BF16)
            if j == 1:
                qkv[n, rows, :] = act
            else:
                g[n, rows, :] = act
            return 0
        lax.fori_loop(0, 8, up, 0)
        m_sends[j].wait_send()
        for peer in (sib, xn, yn):
            pl.semaphore_signal(free.at[j], inc=1, device_id={"tp": peer}, device_id_type=pl.DeviceIdType.MESH)

    def down_stage(j):
        hidden = qkv if j == 1 else g
        swap_partials(1, j, lambda rows: jnp.concatenate([hidden[n, rows, :] for n in range(4)], axis=1), w2)
        if j == 0:
            relay_x(1)

        def post(b, _):
            rows = pl.ds(b * FR, FR)
            out = (acc[rows, :] + ex_r[j, rows, :].astype(F32) + row(bfc2)).astype(BF16)
            h2 = (xb[j, rows, :].astype(F32) + out.astype(F32)).astype(BF16)
            ea[j, b, k] = ln_rows(h2.astype(F32), row(postg), row(postb))
            return 0
        lax.fori_loop(0, 4, post, 0)
        for hf in range(2):
            go(epiece(0, j, k, hf), epiece(1, j, k, hf), es_x.at[j, hf], ex_x.at[j, hf], xn)
            go(epiece(0, j, k, 1 - hf), epiece(2, j, k, 1 - hf), es_y.at[j, 1 - hf], ex_y.at[j, 1 - hf], yn)
        for hf in range(2):
            go(epiece(0, j, k, hf), epiece(0, j, k, hf), es_f.at[0, j, hf], ex_f.at[0, j, hf], sib)

    def forward(group, j, hf):
        go(epiece(group, j, k, hf), epiece(group, j, k, hf), es_f.at[group, j, hf], ex_f.at[group, j, hf], sib)

    def relay_e(j):
        pl.semaphore_wait(free.at[j], 3)
        wait_recv(epiece(1, j, k, 0), ex_x.at[j, 0])
        for b in range(2):
            go(ea.at[PER_CHIP + j, b, k], am.at[j, k, b], es_d.at[j, b], ex_d.at[j, b], yn)
        forward(1, j, 0)
        wait_recv(epiece(2, j, k, 1), ex_y.at[j, 1])
        for b in range(2, 4):
            go(ea.at[2 * PER_CHIP + j, b, k], am.at[j, k, b], es_d.at[j, b], ex_d.at[j, b], xn)
        forward(2, j, 1)
        wait_recv(epiece(1, j, k, 1), ex_x.at[j, 1])
        forward(1, j, 1)
        wait_recv(epiece(2, j, k, 0), ex_y.at[j, 0])
        forward(2, j, 0)

    def take_diagonal(j):
        for b in (0, 2, 1, 3):
            piece = am.at[j, k, b]
            wait_recv(piece, ex_d.at[j, b])
            go(piece, piece, es_g.at[j, b], ex_g.at[j, b], sib)

    def wait_diagonal(j):
        for b in range(4):
            wait_recv(am.at[j, ks, b], ex_g.at[j, b])

    def write_caches(clip, ec):
        cache_rows(clip, ec, wct, bct, kc_o, vc_o)

    def near_cache(group, j):
        chip = jnp.where(group == 0, c, jnp.where(group == 1, cxn, cyn))
        clip = chip * PER_CHIP + j
        for hf in range(2):
            wait_recv(ea.at[3 * group + j, pl.ds(2 * hf, 2), ks], ex_f.at[group, j, hf])
        enc_o[clip] = ea[3 * group + j, c, k]
        write_caches(clip, ea[3 * group + j].reshape(FRAMES, D))

    def far_cache(j):
        clip = cdg * PER_CHIP + j
        wait_diagonal(j)
        enc_o[clip] = am[j, k, c]
        write_caches(clip, natural_order(am, j))

    attention_stage(0)
    wait_rest(3)
    output_stage(0)
    attention_stage(1)
    relay(4)
    output_stage(1)
    relay(5)
    send_x(1)
    wait_rest(4)
    up_stage(0)
    up_stage(1)
    wait_rest(5)
    down_stage(0)
    down_stage(1)
    wait_x(1)
    ln1_stage(2)
    attention_stage(2)
    relay_e(0)
    output_stage(2)
    up_stage(2)
    down_stage(2)
    relay_e(1)

    def first(i, _):
        near_cache(jnp.where(i < 3, 0, 1 + (i + 1) % 2), jnp.where(i < 3, i, (i - 3) // 2))
        return 0
    lax.fori_loop(0, 7, first, 0)
    take_diagonal(0)
    far_cache(0)
    relay_e(2)

    def second(i, _):
        near_cache(1 + i, 2)
        return 0
    lax.fori_loop(0, 2, second, 0)
    take_diagonal(1)
    far_cache(1)
    take_diagonal(2)
    wait_diagonal(2)
    for cp in sends:
        cp.wait_send()


def natural_order(am, j):
    return jnp.concatenate([am[j, core, b] for b in range(4) for core in range(2)], axis=0)


def cache_rows(clip, ec, wct, bct, k_ref, v_ref):
    r = lax.dot_general(wct[...], ec, (((1,), (1,)), ((), ())), preferred_element_type=F32)
    for i in range(4):
        part = r[i * LOC:(i + 1) * LOC, :]
        if i >= 2:
            part = part + jnp.concatenate([bct[i - 2]] * 6, axis=1)
        (k_ref, v_ref)[i // 2][i % 2, clip] = part.astype(BF16)


def writer(enc_v, kc_v, vc_v, am, wct, bct, enc_o, kc_o, vc_o, kl, vl, sem, last_sem):
    t = lax.axis_index("tp")
    c, k = t // 2, t % 2
    cx, cy = c % 2, c // 2
    cdg = 2 * (1 - cy) + (1 - cx)
    last = cdg * PER_CHIP + 2

    def copies(clip):
        cps = [pltpu.make_async_copy(kc_v.at[l, clip], kc_o.at[l, clip], sem) for l in range(2)]
        cps += [pltpu.make_async_copy(vc_v.at[l, clip], vc_o.at[l, clip], sem) for l in range(2)]
        return cps + [pltpu.make_async_copy(enc_v.at[clip], enc_o.at[clip], sem)]

    def start(i, _):
        for cp in copies(lax.rem(last + 1 + i, CLIPS)):
            cp.start()
        return 0
    lax.fori_loop(0, CLIPS - 1, start, 0)
    cps = [pltpu.make_async_copy(am.at[2, k, c], enc_o.at[last], last_sem)]
    cps[0].start()
    cache_rows(0, natural_order(am, 2), wct, bct, kl, vl)
    for l in range(2):
        cps.append(pltpu.make_async_copy(kl.at[l, 0], kc_o.at[l, last], last_sem))
        cps.append(pltpu.make_async_copy(vl.at[l, 0], vc_o.at[l, last], last_sem))
    for cp in cps[1:]:
        cp.start()

    def finish(i, _):
        for cp in copies(lax.rem(last + 1 + i, CLIPS)):
            cp.wait()
        return 0
    lax.fori_loop(0, CLIPS - 1, finish, 0)
    for cp in cps:
        cp.wait()


def device_body(hidden_loc, ln1_gain, ln1_bias, w_q, b_q, w_k, w_v, b_v, w_o, b_o, ln2_gain, ln2_bias, w_fc1, b_fc1, w_fc2, b_fc2, post_gain, post_bias, w_ck, w_cv, b_cv):
    anyspec = pl.BlockSpec(memory_space=pl.ANY)
    vspec = pl.BlockSpec(memory_space=pltpu.VMEM)
    dma = pltpu.SemaphoreType.DMA
    cache = (2, CLIPS, LOC, FRAMES)
    parts = pl.pallas_call(
        kernel,
        out_shape=(
            pltpu.VMEM((CLIPS, FR, D), BF16), pltpu.VMEM(cache, BF16), pltpu.VMEM(cache, BF16),
            pltpu.VMEM((PER_CHIP, 2, 4, FR, D), BF16),
            pltpu.VMEM((4 * LOC, D), BF16),
            pltpu.VMEM((2, LOC, LOC), F32),
        ),
        in_specs=[anyspec] * 21,
        out_specs=(vspec,) * 6,
        scratch_shapes=[
            pltpu.VMEM((LOC,), BF16), pltpu.VMEM((LOC,), BF16), pltpu.VMEM((HID,), BF16), pltpu.VMEM((2, LOC), BF16),
            *([pltpu.VMEM((D,), BF16)] * 8),
            pltpu.VMEM((PER_CHIP, HALF, D), BF16),
            pltpu.VMEM((2, PER_CHIP, FR // 2, D), BF16),
            pltpu.VMEM((PER_CHIP, HALF, D), BF16),
            pltpu.VMEM((PER_CHIP, HALF, D), BF16),
            pltpu.VMEM((3, D, NQ), BF16),
            pltpu.VMEM((NQ, D), BF16),
            pltpu.VMEM((D, NH), BF16),
            pltpu.VMEM((NH, D), BF16),
            pltpu.VMEM((4, 8, LOC), F32),
            pltpu.VMEM((4, FRAMES, NQ), BF16),
            pltpu.VMEM((2, FRAMES, LOC), BF16),
            pltpu.VMEM((2, FRAMES, LOC), BF16),
            pltpu.VMEM((4, FRAMES, HID), BF16),
            pltpu.VMEM((HALF, D), F32),
            pltpu.VMEM((9, 4, 2, FR, D), BF16),
            dma((2, 5)), dma((2, 6)), dma((2, 2)), dma((6, 7)), dma((6, 6)), dma((3,)), dma((3,)),
            dma((2, 3)), dma((2, 3)), dma((2, 3)), dma((2, 3)),
            dma((3, 2)), dma((3, 2)), dma((3, 4)), dma((3, 3, 2)), dma((3, 4)),
            dma((3, 2)), dma((3, 2)), dma((3, 4)), dma((3, 3, 2)), dma((3, 4)),
            dma((4, 2)), dma((12,)), pltpu.SemaphoreType.REGULAR((3,)),
        ],
        compiler_params=pltpu.CompilerParams(collective_id=0, has_side_effects=True, vmem_limit_bytes=48500000),
        name="encoder_layer",
    )(hidden_loc, w_q, w_k, w_v, w_o, w_fc1, w_fc2, w_ck, w_cv,
      b_q, b_v, b_fc1, b_cv, ln1_gain, ln1_bias, ln2_gain, ln2_bias, post_gain, post_bias, b_o, b_fc2)

    enc, kc, vc = pl.pallas_call(
        writer,
        out_shape=(jax.ShapeDtypeStruct((CLIPS, FR, D), BF16), jax.ShapeDtypeStruct(cache, BF16), jax.ShapeDtypeStruct(cache, BF16)),
        in_specs=[vspec] * 6,
        out_specs=(anyspec,) * 3,
        scratch_shapes=[pltpu.VMEM((2, 1, LOC, FRAMES), BF16), pltpu.VMEM((2, 1, LOC, FRAMES), BF16), dma, dma],
        compiler_params=pltpu.CompilerParams(vmem_limit_bytes=8000000),
        name="writer",
    )(*parts)

    def heads_last(cached):
        return cached.reshape(2, CLIPS, LOC // HEAD_DIM, HEAD_DIM, FRAMES).transpose(0, 1, 4, 2, 3)
    return enc, heads_last(kc), heads_last(vc)


def solution(mesh):
    in_specs = (P("dp", "tp", None), P(), P(), P(None, "tp"), P("tp"), P(None, "tp"), P(None, "tp"), P("tp"), P("tp", None), P(), P(), P(), P(None, "tp"), P("tp"), P("tp", None), P(), P(), P(), P(None, None, "tp"), P(None, None, "tp"), P(None, "tp"))
    out_specs = (P("dp", "tp", None), P(None, "dp", None, "tp", None), P(None, "dp", None, "tp", None))
    return jax.shard_map(device_body, mesh=mesh, in_specs=in_specs, out_specs=out_specs, check_vma=False)
```

```python
import functools

import jax
import jax.numpy as jnp
from jax import lax
from jax.experimental import pallas as pl
from jax.experimental.pallas import tpu as pltpu
from jax.sharding import PartitionSpec as P

HEAD_DIM = 64
ATTN_SCALE = HEAD_DIM ** -0.25
LN_EPS = 1e-5
CLIPS = 12
PER_CHIP = 3
FR = 96
HALF = 4 * FR
FRAMES = 8 * FR
D = 1024
LOC = 128
HID = 512
NQ = 4 * LOC
NH = 4 * HID
QROWS = 256
F32, BF16 = jnp.float32, jnp.bfloat16


def ln_rows(values, gain, bias):
    centered = values - jnp.mean(values, axis=-1, keepdims=True)
    row_var = jnp.mean(centered * centered, axis=-1, keepdims=True)
    return (centered * lax.rsqrt(row_var + LN_EPS) * gain + bias).astype(BF16)


def kernel(hid, wq_h, wk_h, wv_h, wo_h, w1_h, w2_h, ck_h, cv_h,
           bq_h, bv_h, b1_h, bcv_h, ln1g_h, ln1b_h, ln2g_h, ln2b_h, postg_h, postb_h, bo_h, bfc2_h,
           enc_o, kc_o, vc_o, am, wct, bct,
           bq_v, bv_v, b1_v, bcv_v, ln1g, ln1b, ln2g, ln2b, postg, postb, bo_v, bfc2, xb, xrel, ex_s, ex_r, wqkv, wo, w1, w2, bias, qkv, kz, vz, g, acc, ea,
           x_r, x_s, xrel_r, w_r, w_s, b_r, b_s, am_r, am_s, ex_rs, ex_ss, ex_x, ex_y, ex_d, ex_f, ex_g, es_x, es_y, es_d, es_f, es_g, c_s, v_s, free):
    t = lax.axis_index("tp")
    c, k = t // 2, t % 2
    cx, cy = c % 2, c // 2
    cxn = 2 * cy + (1 - cx)
    cyn = 2 * (1 - cy) + cx
    cdg = 2 * (1 - cy) + (1 - cx)
    ks = 1 - k
    sib, xn, yn = 2 * c + ks, 2 * cxn + k, 2 * cyn + k

    def remote(src, dst, ssem, rsem, dev):
        return pltpu.make_async_remote_copy(src_ref=src, dst_ref=dst, send_sem=ssem, recv_sem=rsem,
                                            device_id={"tp": dev}, device_id_type=pl.DeviceIdType.MESH)

    def wait_recv(ref, rsem):
        pltpu.make_async_copy(ref, ref, rsem).wait()

    def row(ref):
        return ref[...].astype(F32).reshape(1, ref.shape[0])

    barrier = pltpu.get_barrier_semaphore()
    for peer in (sib, xn, yn):
        pl.semaphore_signal(barrier, inc=1, device_id={"tp": peer}, device_id_type=pl.DeviceIdType.MESH)
    pl.semaphore_wait(barrier, 3)

    def xclips(late):
        return pl.ds(2, 1) if late else pl.ds(0, 2)

    def xslot(chip, late):
        return xb.at[xclips(late), pl.ds(chip * FR, FR), :]

    def xhalf(chip, late, hf):
        return xb.at[xclips(late), pl.ds(chip * FR + hf * (FR // 2), FR // 2), :]

    def xsource(chip, late):
        return hid.at[pl.ds(chip * PER_CHIP + 2, 1) if late else pl.ds(chip * PER_CHIP, 2)]

    def wfull(i, chip):
        if i < 3:
            return wqkv.at[i, :, pl.ds(pl.multiple_of(chip * LOC, LOC), LOC)]
        if i == 3:
            return wo.at[pl.ds(chip * LOC, LOC)]
        if i == 4:
            return w1.at[:, pl.ds(pl.multiple_of(chip * HID, HID), HID)]
        return w2.at[pl.ds(chip * HID, HID)]

    def whalf(i, chip, hf):
        if i < 3:
            return wqkv.at[i, pl.ds(hf * (D // 2), D // 2), pl.ds(pl.multiple_of(chip * LOC, LOC), LOC)]
        if i == 3:
            return wo.at[pl.ds(chip * LOC + hf * (LOC // 2), LOC // 2)]
        if i == 4:
            return w1.at[pl.ds(hf * (D // 2), D // 2), pl.ds(pl.multiple_of(chip * HID, HID), HID)]
        return w2.at[pl.ds(chip * HID + hf * (HID // 2), HID // 2)]

    w_hbm = (wq_h, wk_h, wv_h, wo_h, w1_h, w2_h)
    sends = []

    def go(src, dst, ssem, rsem, dev):
        cp = remote(src, dst, ssem, rsem, dev)
        cp.start()
        sends.append(cp)

    def send_direct(i):
        wait_recv(wfull(i, c), w_r.at[i, 0])
        go(wfull(i, c), wfull(i, c), w_s.at[i, 0], w_r.at[i, 1], xn)
        go(wfull(i, c), wfull(i, c), w_s.at[i, 1], w_r.at[i, 2], yn)

    def send_halves(i, part):
        if part == 0:
            wait_recv(wfull(i, c), w_r.at[i, 0])
        mine_x, mine_y = whalf(i, c, part), whalf(i, c, 1 - part)
        go(mine_x, mine_x, w_s.at[i, 4 * part], w_r.at[i, 1 + 4 * part], xn)
        go(mine_y, mine_y, w_s.at[i, 4 * part + 1], w_r.at[i, 2 + 4 * part], yn)

    def relay(i):
        wait_recv(wfull(i, cxn) if i < 4 else whalf(i, cxn, 0), w_r.at[i, 1])
        go(whalf(i, cxn, 0), whalf(i, cxn, 0), w_s.at[i, 2], w_r.at[i, 3], yn)
        wait_recv(wfull(i, cyn) if i < 4 else whalf(i, cyn, 1), w_r.at[i, 2])
        go(whalf(i, cyn, 1), whalf(i, cyn, 1), w_s.at[i, 3], w_r.at[i, 4], xn)

    def wait_rest(i):
        if i >= 4:
            wait_recv(whalf(i, cxn, 1), w_r.at[i, 5])
            wait_recv(whalf(i, cyn, 0), w_r.at[i, 6])
        wait_recv(whalf(i, cdg, 0), w_r.at[i, 3])
        wait_recv(whalf(i, cdg, 1), w_r.at[i, 4])

    def send_x(late):
        for hf, dev in enumerate((xn, yn)):
            src = xsource(cdg, late).at[:, pl.ds(hf * (FR // 2), FR // 2), :]
            go(src, xrel.at[hf, xclips(late)], x_s.at[late, hf], xrel_r.at[late, hf], dev)
        go(xsource(cxn, late), xslot(c, late), x_s.at[late, 2], x_r.at[late, 1], xn)
        go(xsource(cyn, late), xslot(c, late), x_s.at[late, 3], x_r.at[late, 2], yn)

    def relay_x(late):
        for hf, (chip, dev) in enumerate(((cxn, yn), (cyn, xn))):
            piece = xrel.at[hf, xclips(late)]
            wait_recv(piece, xrel_r.at[late, hf])
            go(piece, xhalf(chip, late, hf), x_s.at[late, 4 + hf], x_r.at[late, 3 + hf], dev)

    def ln1_stage(j):
        def body(b, _):
            vals = xb[j, pl.ds(b * FR, FR), :].astype(F32)
            am[j, k, b] = ln_rows(vals, row(ln1g), row(ln1b))
            return 0
        lax.fori_loop(0, 4, body, 0)
        cp = remote(am.at[j, k], am.at[j, k], am_s.at[0, j], am_r.at[0, j], sib)
        cp.start()
        a_sends.append(cp)

    def wait_x(late):
        for r, chip in ((0, c), (1, cxn), (2, cyn)):
            wait_recv(xslot(chip, late), x_r.at[late, r])
        for hf in range(2):
            wait_recv(xhalf(cdg, late, hf), x_r.at[late, 3 + hf])

    send_x(0)
    vec_copies = [pltpu.make_async_copy(src, dst, v_s.at[i]) for i, (src, dst) in enumerate((
        (bq_h, bq_v), (bv_h, bv_v), (b1_h, b1_v), (bcv_h, bcv_v), (ln1g_h, ln1g), (ln1b_h, ln1b),
        (ln2g_h, ln2g), (ln2b_h, ln2b), (postg_h, postg), (postb_h, postb), (bo_h, bo_v), (bfc2_h, bfc2)))]
    for cp in vec_copies:
        cp.start()
    for i in range(3):
        pltpu.make_async_copy(w_hbm[i], wfull(i, c), w_r.at[i, 0]).start()
    for late in range(2):
        pltpu.make_async_copy(xsource(c, late), xslot(c, late), x_r.at[late, 0]).start()
    for i in range(3, 6):
        pltpu.make_async_copy(w_hbm[i], wfull(i, c), w_r.at[i, 0]).start()
    wc_copies = []
    for i, src in enumerate((ck_h.at[0], ck_h.at[1], cv_h.at[0], cv_h.at[1])):
        for hf in range(2):
            cp = pltpu.make_async_copy(src.at[pl.ds(hf * 512, 512)], qkv.at[i, pl.ds(0, 512), pl.ds(hf * LOC, LOC)], c_s.at[i, hf])
            cp.start()
            wc_copies.append(cp)
    for cp in vec_copies:
        cp.wait()
    bias[c, 0:1, :] = row(bq_v)
    bias[c, 1:2, :] = row(bv_v)
    b1_row = row(b1_v)
    for q in range(4):
        bias[c, 2 + q:3 + q, :] = b1_row[:, q * LOC:(q + 1) * LOC]
    for l in range(2):
        bct[l] = jnp.transpose(jnp.broadcast_to(bcv_v[l:l + 1, :].astype(F32), (LOC, LOC)))
    send_direct(0)
    relay_x(0)
    for r, dev in enumerate((xn, yn)):
        go(bias.at[c], bias.at[c], b_s.at[r], b_r.at[r], dev)
    for i in range(1, 3):
        send_direct(i)

    send_direct(3)
    send_halves(4, 0)
    a_sends = []
    wait_x(0)
    for j in range(2):
        ln1_stage(j)
    for cp in wc_copies:
        cp.wait()
    for i in range(4):
        for hf in range(2):
            wct[i * LOC:(i + 1) * LOC, hf * 512:(hf + 1) * 512] = jnp.transpose(qkv[i, 0:512, hf * LOC:(hf + 1) * LOC])
    for r, chip in enumerate((cxn, cyn, cdg)):
        wait_recv(bias.at[chip], b_r.at[r])
        if r == 0:
            go(bias.at[cxn], bias.at[cxn], b_s.at[2], b_r.at[2], yn)
    for i in range(3):
        relay(i)
    relay(3)
    send_halves(4, 1)
    send_halves(5, 0)
    for i in range(3):
        wait_rest(i)

    def row_of(r):
        return jnp.concatenate([bias[n, r:r + 1, :] for n in range(4)], axis=1)

    lane = lax.broadcasted_iota(jnp.int32, (FRAMES, LOC), 1)

    def attention_stage(j):
        wait_recv(am.at[j, ks], am_r.at[0, j])
        bq, bv = row_of(0), row_of(1)

        def project(r, _):
            rows = pl.ds(r * HALF, HALF)
            a = am[j, r].reshape(HALF, D)
            qkv[0, rows, :] = ((jnp.dot(a, wqkv[0], preferred_element_type=F32) + bq) * ATTN_SCALE).astype(BF16)
            qkv[1, rows, :] = (jnp.dot(a, wqkv[1], preferred_element_type=F32) * ATTN_SCALE).astype(BF16)
            qkv[2, rows, :] = (jnp.dot(a, wqkv[2], preferred_element_type=F32) + bv).astype(BF16)
            return 0
        lax.fori_loop(0, 2, project, 0)

        def pair(p, _):
            cols = pl.ds(pl.multiple_of(p * LOC, LOC), LOC)
            kp, vp = qkv[1, :, cols], qkv[2, :, cols]
            zero = jnp.zeros_like(kp)
            kz[0] = jnp.where(lane < HEAD_DIM, kp, zero)
            kz[1] = jnp.where(lane < HEAD_DIM, zero, kp)
            vz[0] = jnp.where(lane < HEAD_DIM, vp, zero)
            vz[1] = jnp.where(lane < HEAD_DIM, zero, vp)

            def attend(r, _):
                rows = pl.ds(r * QROWS, QROWS)
                qb = qkv[0, rows, cols]
                out = None
                for hh in range(2):
                    s = lax.dot_general(qb, kz[hh], (((1,), (1,)), ((), ())), preferred_element_type=F32)
                    e = jnp.exp(s - jnp.max(s, axis=-1, keepdims=True))
                    prob = (e * (1.0 / jnp.sum(e, axis=-1, keepdims=True))).astype(BF16)
                    part = jnp.dot(prob, vz[hh], preferred_element_type=F32)
                    out = part if out is None else out + part
                qkv[3, rows, cols] = out.astype(BF16)
                return 0
            lax.fori_loop(0, FRAMES // QROWS, attend, 0)
            return 0
        lax.fori_loop(0, 4, pair, 0)

    own = pl.ds(k * HALF, HALF)
    oth = pl.ds(ks * HALF, HALF)

    def swap_partials(phase, j, lhs, weight):
        for n in range(2):
            cols = slice(n * 512, (n + 1) * 512)
            ex_s[j, :, cols] = jnp.dot(lhs(oth), weight[:, cols], preferred_element_type=F32).astype(BF16)
        cp = remote(ex_s.at[j], ex_r.at[j], ex_ss.at[phase, j], ex_rs.at[phase, j], sib)
        cp.start()
        for n in range(2):
            cols = slice(n * 512, (n + 1) * 512)
            acc[:, cols] = jnp.dot(lhs(own), weight[:, cols], preferred_element_type=F32)
        wait_recv(ex_r.at[j], ex_rs.at[phase, j])
        cp.wait_send()

    m_sends = []

    def output_stage(j):
        swap_partials(0, j, lambda rows: qkv[3, rows, :], wo)
        a_sends[j].wait_send()

        def body(b, _):
            rows = pl.ds(b * FR, FR)
            out = (acc[rows, :] + ex_r[j, rows, :].astype(F32) + row(bo_v)).astype(BF16)
            h = (xb[j, rows, :].astype(F32) + out.astype(F32)).astype(BF16)
            xb[j, rows, :] = h
            am[j, k, b] = ln_rows(h.astype(F32), row(ln2g), row(ln2b))
            return 0
        lax.fori_loop(0, 4, body, 0)
        cp = remote(am.at[j, k], am.at[j, k], am_s.at[1, j], am_r.at[1, j], sib)
        cp.start()
        m_sends.append(cp)

    def epiece(group, j, core, hf):
        return ea.at[3 * group + j, pl.ds(2 * hf, 2), core]

    def up_stage(j):
        wait_recv(am.at[j, ks], am_r.at[1, j])

        def up(i, _):
            n, r = i // 2, i % 2
            rows = pl.ds(r * HALF, HALF)
            cols = pl.ds(pl.multiple_of(n * HID, HID), HID)
            b1 = jnp.concatenate([bias[n, 2 + q:3 + q, :] for q in range(4)], axis=1)
            u = jnp.dot(am[j, r].reshape(HALF, D), w1[:, cols], preferred_element_type=F32) + b1
            act = (0.5 * u * (1.0 + lax.erf(u * (2.0 ** -0.5)))).astype(BF16)
            if j == 1:
                qkv[n, rows, :] = act
            else:
                g[n, rows, :] = act
            return 0
        lax.fori_loop(0, 8, up, 0)
        m_sends[j].wait_send()
        for peer in (sib, xn, yn):
            pl.semaphore_signal(free.at[j], inc=1, device_id={"tp": peer}, device_id_type=pl.DeviceIdType.MESH)

    def down_stage(j):
        hidden = qkv if j == 1 else g
        swap_partials(1, j, lambda rows: jnp.concatenate([hidden[n, rows, :] for n in range(4)], axis=1), w2)
        if j == 0:
            relay_x(1)

        def post(b, _):
            rows = pl.ds(b * FR, FR)
            out = (acc[rows, :] + ex_r[j, rows, :].astype(F32) + row(bfc2)).astype(BF16)
            h2 = (xb[j, rows, :].astype(F32) + out.astype(F32)).astype(BF16)
            ea[j, b, k] = ln_rows(h2.astype(F32), row(postg), row(postb))
            return 0
        lax.fori_loop(0, 4, post, 0)
        for hf in range(2):
            go(epiece(0, j, k, hf), epiece(1, j, k, hf), es_x.at[j, hf], ex_x.at[j, hf], xn)
            go(epiece(0, j, k, 1 - hf), epiece(2, j, k, 1 - hf), es_y.at[j, 1 - hf], ex_y.at[j, 1 - hf], yn)
        for hf in range(2):
            go(epiece(0, j, k, hf), epiece(0, j, k, hf), es_f.at[0, j, hf], ex_f.at[0, j, hf], sib)

    def forward(group, j, hf):
        go(epiece(group, j, k, hf), epiece(group, j, k, hf), es_f.at[group, j, hf], ex_f.at[group, j, hf], sib)

    def relay_e(j):
        pl.semaphore_wait(free.at[j], 3)
        wait_recv(epiece(1, j, k, 0), ex_x.at[j, 0])
        for b in range(2):
            go(ea.at[PER_CHIP + j, b, k], am.at[j, k, b], es_d.at[j, b], ex_d.at[j, b], yn)
        forward(1, j, 0)
        wait_recv(epiece(2, j, k, 1), ex_y.at[j, 1])
        for b in range(2, 4):
            go(ea.at[2 * PER_CHIP + j, b, k], am.at[j, k, b], es_d.at[j, b], ex_d.at[j, b], xn)
        forward(2, j, 1)
        wait_recv(epiece(1, j, k, 1), ex_x.at[j, 1])
        forward(1, j, 1)
        wait_recv(epiece(2, j, k, 0), ex_y.at[j, 0])
        forward(2, j, 0)

    def take_diagonal(j):
        for b in (0, 2, 1, 3):
            piece = am.at[j, k, b]
            wait_recv(piece, ex_d.at[j, b])
            go(piece, piece, es_g.at[j, b], ex_g.at[j, b], sib)

    def wait_diagonal(j):
        for b in range(4):
            wait_recv(am.at[j, ks, b], ex_g.at[j, b])

    def write_caches(clip, ec):
        cache_rows(clip, ec, wct, bct, kc_o, vc_o)

    def near_cache(group, j):
        chip = jnp.where(group == 0, c, jnp.where(group == 1, cxn, cyn))
        clip = chip * PER_CHIP + j
        for hf in range(2):
            wait_recv(ea.at[3 * group + j, pl.ds(2 * hf, 2), ks], ex_f.at[group, j, hf])
        enc_o[clip] = ea[3 * group + j, c, k]
        write_caches(clip, ea[3 * group + j].reshape(FRAMES, D))

    def far_cache(j):
        clip = cdg * PER_CHIP + j
        wait_diagonal(j)
        enc_o[clip] = am[j, k, c]
        write_caches(clip, natural_order(am, j))

    attention_stage(0)
    relay(4)
    send_halves(5, 1)
    wait_rest(3)
    output_stage(0)
    attention_stage(1)
    relay(5)
    output_stage(1)
    wait_rest(4)
    up_stage(0)
    up_stage(1)
    send_x(1)
    wait_rest(5)
    down_stage(0)
    down_stage(1)
    wait_x(1)
    ln1_stage(2)
    attention_stage(2)
    output_stage(2)
    relay_e(0)
    up_stage(2)
    down_stage(2)
    relay_e(1)

    def first(i, _):
        near_cache(jnp.where(i < 3, 0, 1 + (i + 1) % 2), jnp.where(i < 3, i, (i - 3) // 2))
        return 0
    lax.fori_loop(0, 7, first, 0)
    take_diagonal(0)
    far_cache(0)
    relay_e(2)

    def second(i, _):
        near_cache(1 + i, 2)
        return 0
    lax.fori_loop(0, 2, second, 0)
    take_diagonal(1)
    far_cache(1)
    take_diagonal(2)
    wait_diagonal(2)
    for cp in sends:
        cp.wait_send()


def natural_order(am, j):
    return jnp.concatenate([am[j, core, b] for b in range(4) for core in range(2)], axis=0)


def cache_rows(clip, ec, wct, bct, k_ref, v_ref):
    r = lax.dot_general(wct[...], ec, (((1,), (1,)), ((), ())), preferred_element_type=F32)
    for i in range(4):
        part = r[i * LOC:(i + 1) * LOC, :]
        if i >= 2:
            part = part + jnp.concatenate([bct[i - 2]] * 6, axis=1)
        (k_ref, v_ref)[i // 2][i % 2, clip] = part.astype(BF16)


def writer(enc_v, kc_v, vc_v, am, wct, bct, enc_o, kc_o, vc_o, kl, vl, sem, last_sem):
    t = lax.axis_index("tp")
    c, k = t // 2, t % 2
    cx, cy = c % 2, c // 2
    cdg = 2 * (1 - cy) + (1 - cx)
    last = cdg * PER_CHIP + 2

    def copies(clip):
        cps = [pltpu.make_async_copy(kc_v.at[l, clip], kc_o.at[l, clip], sem) for l in range(2)]
        cps += [pltpu.make_async_copy(vc_v.at[l, clip], vc_o.at[l, clip], sem) for l in range(2)]
        return cps + [pltpu.make_async_copy(enc_v.at[clip], enc_o.at[clip], sem)]

    def start(i, _):
        for cp in copies(lax.rem(last + 1 + i, CLIPS)):
            cp.start()
        return 0
    lax.fori_loop(0, CLIPS - 1, start, 0)
    cps = [pltpu.make_async_copy(am.at[2, k, c], enc_o.at[last], last_sem)]
    cps[0].start()
    cache_rows(0, natural_order(am, 2), wct, bct, kl, vl)
    for l in range(2):
        cps.append(pltpu.make_async_copy(kl.at[l, 0], kc_o.at[l, last], last_sem))
        cps.append(pltpu.make_async_copy(vl.at[l, 0], vc_o.at[l, last], last_sem))
    for cp in cps[1:]:
        cp.start()

    def finish(i, _):
        for cp in copies(lax.rem(last + 1 + i, CLIPS)):
            cp.wait()
        return 0
    lax.fori_loop(0, CLIPS - 1, finish, 0)
    for cp in cps:
        cp.wait()


def device_body(hidden_loc, ln1_gain, ln1_bias, w_q, b_q, w_k, w_v, b_v, w_o, b_o, ln2_gain, ln2_bias, w_fc1, b_fc1, w_fc2, b_fc2, post_gain, post_bias, w_ck, w_cv, b_cv):
    anyspec = pl.BlockSpec(memory_space=pl.ANY)
    vspec = pl.BlockSpec(memory_space=pltpu.VMEM)
    dma = pltpu.SemaphoreType.DMA
    cache = (2, CLIPS, LOC, FRAMES)
    parts = pl.pallas_call(
        kernel,
        out_shape=(
            pltpu.VMEM((CLIPS, FR, D), BF16), pltpu.VMEM(cache, BF16), pltpu.VMEM(cache, BF16),
            pltpu.VMEM((PER_CHIP, 2, 4, FR, D), BF16),
            pltpu.VMEM((4 * LOC, D), BF16),
            pltpu.VMEM((2, LOC, LOC), F32),
        ),
        in_specs=[anyspec] * 21,
        out_specs=(vspec,) * 6,
        scratch_shapes=[
            pltpu.VMEM((LOC,), BF16), pltpu.VMEM((LOC,), BF16), pltpu.VMEM((HID,), BF16), pltpu.VMEM((2, LOC), BF16),
            *([pltpu.VMEM((D,), BF16)] * 8),
            pltpu.VMEM((PER_CHIP, HALF, D), BF16),
            pltpu.VMEM((2, PER_CHIP, FR // 2, D), BF16),
            pltpu.VMEM((PER_CHIP, HALF, D), BF16),
            pltpu.VMEM((PER_CHIP, HALF, D), BF16),
            pltpu.VMEM((3, D, NQ), BF16),
            pltpu.VMEM((NQ, D), BF16),
            pltpu.VMEM((D, NH), BF16),
            pltpu.VMEM((NH, D), BF16),
            pltpu.VMEM((4, 8, LOC), F32),
            pltpu.VMEM((4, FRAMES, NQ), BF16),
            pltpu.VMEM((2, FRAMES, LOC), BF16),
            pltpu.VMEM((2, FRAMES, LOC), BF16),
            pltpu.VMEM((4, FRAMES, HID), BF16),
            pltpu.VMEM((HALF, D), F32),
            pltpu.VMEM((9, 4, 2, FR, D), BF16),
            dma((2, 5)), dma((2, 6)), dma((2, 2)), dma((6, 7)), dma((6, 6)), dma((3,)), dma((3,)),
            dma((2, 3)), dma((2, 3)), dma((2, 3)), dma((2, 3)),
            dma((3, 2)), dma((3, 2)), dma((3, 4)), dma((3, 3, 2)), dma((3, 4)),
            dma((3, 2)), dma((3, 2)), dma((3, 4)), dma((3, 3, 2)), dma((3, 4)),
            dma((4, 2)), dma((12,)), pltpu.SemaphoreType.REGULAR((3,)),
        ],
        compiler_params=pltpu.CompilerParams(collective_id=0, has_side_effects=True, vmem_limit_bytes=48500000),
        name="encoder_layer",
    )(hidden_loc, w_q, w_k, w_v, w_o, w_fc1, w_fc2, w_ck, w_cv,
      b_q, b_v, b_fc1, b_cv, ln1_gain, ln1_bias, ln2_gain, ln2_bias, post_gain, post_bias, b_o, b_fc2)

    enc, kc, vc = pl.pallas_call(
        writer,
        out_shape=(jax.ShapeDtypeStruct((CLIPS, FR, D), BF16), jax.ShapeDtypeStruct(cache, BF16), jax.ShapeDtypeStruct(cache, BF16)),
        in_specs=[vspec] * 6,
        out_specs=(anyspec,) * 3,
        scratch_shapes=[pltpu.VMEM((2, 1, LOC, FRAMES), BF16), pltpu.VMEM((2, 1, LOC, FRAMES), BF16), dma, dma],
        compiler_params=pltpu.CompilerParams(vmem_limit_bytes=8000000),
        name="writer",
    )(*parts)

    def heads_last(cached):
        return cached.reshape(2, CLIPS, LOC // HEAD_DIM, HEAD_DIM, FRAMES).transpose(0, 1, 4, 2, 3)
    return enc, heads_last(kc), heads_last(vc)


def solution(mesh):
    in_specs = (P("dp", "tp", None), P(), P(), P(None, "tp"), P("tp"), P(None, "tp"), P(None, "tp"), P("tp"), P("tp", None), P(), P(), P(), P(None, "tp"), P("tp"), P("tp", None), P(), P(), P(), P(None, None, "tp"), P(None, None, "tp"), P(None, "tp"))
    out_specs = (P("dp", "tp", None), P(None, "dp", None, "tp", None), P(None, "dp", None, "tp", None))
    return jax.shard_map(device_body, mesh=mesh, in_specs=in_specs, out_specs=out_specs, check_vma=False)
```

```python
import functools

import jax
import jax.numpy as jnp
from jax import lax
from jax.experimental import pallas as pl
from jax.experimental.pallas import tpu as pltpu
from jax.sharding import PartitionSpec as P

HEAD_DIM = 64
ATTN_SCALE = HEAD_DIM ** -0.25
LN_EPS = 1e-5
CLIPS = 12
PER_CHIP = 3
FR = 96
HALF = 4 * FR
FRAMES = 8 * FR
D = 1024
LOC = 128
HID = 512
NQ = 4 * LOC
NH = 4 * HID
QROWS = 256
F32, BF16 = jnp.float32, jnp.bfloat16


def ln_rows(values, gain, bias):
    centered = values - jnp.mean(values, axis=-1, keepdims=True)
    row_var = jnp.mean(centered * centered, axis=-1, keepdims=True)
    return (centered * lax.rsqrt(row_var + LN_EPS) * gain + bias).astype(BF16)


def kernel(hid, wq_h, wk_h, wv_h, wo_h, w1_h, w2_h, ck_h, cv_h,
           bq_h, bv_h, b1_h, bcv_h, ln1g_h, ln1b_h, ln2g_h, ln2b_h, postg_h, postb_h, bo_h, bfc2_h,
           enc_o, kc_o, vc_o, am, wct, bct,
           bq_v, bv_v, b1_v, bcv_v, ln1g, ln1b, ln2g, ln2b, postg, postb, bo_v, bfc2, xb, xrel, ex_s, ex_r, wqkv, wo, w1, w2, bias, qkv, kz, vz, g, acc, ea,
           x_r, x_s, xrel_r, w_r, w_s, b_r, b_s, am_r, am_s, ex_rs, ex_ss, ex_x, ex_y, ex_d, ex_f, ex_g, es_x, es_y, es_d, es_f, es_g, c_s, v_s, free):
    t = lax.axis_index("tp")
    c, k = t // 2, t % 2
    cx, cy = c % 2, c // 2
    cxn = 2 * cy + (1 - cx)
    cyn = 2 * (1 - cy) + cx
    cdg = 2 * (1 - cy) + (1 - cx)
    ks = 1 - k
    sib, xn, yn = 2 * c + ks, 2 * cxn + k, 2 * cyn + k

    def remote(src, dst, ssem, rsem, dev):
        return pltpu.make_async_remote_copy(src_ref=src, dst_ref=dst, send_sem=ssem, recv_sem=rsem,
                                            device_id={"tp": dev}, device_id_type=pl.DeviceIdType.MESH)

    def wait_recv(ref, rsem):
        pltpu.make_async_copy(ref, ref, rsem).wait()

    def row(ref):
        return ref[...].astype(F32).reshape(1, ref.shape[0])

    barrier = pltpu.get_barrier_semaphore()
    for peer in (sib, xn, yn):
        pl.semaphore_signal(barrier, inc=1, device_id={"tp": peer}, device_id_type=pl.DeviceIdType.MESH)
    pl.semaphore_wait(barrier, 3)

    def xclips(late):
        return pl.ds(2, 1) if late else pl.ds(0, 2)

    def xslot(chip, late):
        return xb.at[xclips(late), pl.ds(chip * FR, FR), :]

    def xhalf(chip, late, hf):
        return xb.at[xclips(late), pl.ds(chip * FR + hf * (FR // 2), FR // 2), :]

    def xsource(chip, late):
        return hid.at[pl.ds(chip * PER_CHIP + 2, 1) if late else pl.ds(chip * PER_CHIP, 2)]

    def wfull(i, chip):
        if i < 3:
            return wqkv.at[i, chip]
        if i == 3:
            return wo.at[pl.ds(chip * LOC, LOC)]
        if i == 4:
            return w1.at[chip]
        return w2.at[pl.ds(chip * HID, HID)]

    def whalf(i, chip, hf):
        if i < 3:
            return wqkv.at[i, chip, pl.ds(hf * (D // 2), D // 2)]
        if i == 3:
            return wo.at[pl.ds(chip * LOC + hf * (LOC // 2), LOC // 2)]
        if i == 4:
            return w1.at[chip, pl.ds(hf * (D // 2), D // 2)]
        return w2.at[pl.ds(chip * HID + hf * (HID // 2), HID // 2)]

    w_hbm = (wq_h, wk_h, wv_h, wo_h, w1_h, w2_h)
    sends = []

    def go(src, dst, ssem, rsem, dev):
        cp = remote(src, dst, ssem, rsem, dev)
        cp.start()
        sends.append(cp)

    def send_direct(i):
        wait_recv(wfull(i, c), w_r.at[i, 0])
        go(wfull(i, c), wfull(i, c), w_s.at[i, 0], w_r.at[i, 1], xn)
        go(wfull(i, c), wfull(i, c), w_s.at[i, 1], w_r.at[i, 2], yn)

    def send_halves(i, part):
        if part == 0:
            wait_recv(wfull(i, c), w_r.at[i, 0])
        mine_x, mine_y = whalf(i, c, part), whalf(i, c, 1 - part)
        go(mine_x, mine_x, w_s.at[i, 4 * part], w_r.at[i, 1 + 4 * part], xn)
        go(mine_y, mine_y, w_s.at[i, 4 * part + 1], w_r.at[i, 2 + 4 * part], yn)

    def relay(i):
        wait_recv(wfull(i, cxn) if i < 4 else whalf(i, cxn, 0), w_r.at[i, 1])
        go(whalf(i, cxn, 0), whalf(i, cxn, 0), w_s.at[i, 2], w_r.at[i, 3], yn)
        wait_recv(wfull(i, cyn) if i < 4 else whalf(i, cyn, 1), w_r.at[i, 2])
        go(whalf(i, cyn, 1), whalf(i, cyn, 1), w_s.at[i, 3], w_r.at[i, 4], xn)

    def wait_rest(i):
        if i >= 4:
            wait_recv(whalf(i, cxn, 1), w_r.at[i, 5])
            wait_recv(whalf(i, cyn, 0), w_r.at[i, 6])
        wait_recv(whalf(i, cdg, 0), w_r.at[i, 3])
        wait_recv(whalf(i, cdg, 1), w_r.at[i, 4])

    def send_x(late):
        for hf, dev in enumerate((xn, yn)):
            src = xsource(cdg, late).at[:, pl.ds(hf * (FR // 2), FR // 2), :]
            go(src, xrel.at[hf, xclips(late)], x_s.at[late, hf], xrel_r.at[late, hf], dev)
        go(xsource(cxn, late), xslot(c, late), x_s.at[late, 2], x_r.at[late, 1], xn)
        go(xsource(cyn, late), xslot(c, late), x_s.at[late, 3], x_r.at[late, 2], yn)

    def relay_x(late):
        for hf, (chip, dev) in enumerate(((cxn, yn), (cyn, xn))):
            piece = xrel.at[hf, xclips(late)]
            wait_recv(piece, xrel_r.at[late, hf])
            go(piece, xhalf(chip, late, hf), x_s.at[late, 4 + hf], x_r.at[late, 3 + hf], dev)

    def ln1_stage(j):
        def body(b, _):
            vals = xb[j, pl.ds(b * FR, FR), :].astype(F32)
            am[j, k, b] = ln_rows(vals, row(ln1g), row(ln1b))
            return 0
        lax.fori_loop(0, 4, body, 0)
        cp = remote(am.at[j, k], am.at[j, k], am_s.at[0, j], am_r.at[0, j], sib)
        cp.start()
        a_sends.append(cp)

    def wait_x(late):
        for r, chip in ((0, c), (1, cxn), (2, cyn)):
            wait_recv(xslot(chip, late), x_r.at[late, r])
        for hf in range(2):
            wait_recv(xhalf(cdg, late, hf), x_r.at[late, 3 + hf])

    send_x(0)
    vec_copies = [pltpu.make_async_copy(src, dst, v_s.at[i]) for i, (src, dst) in enumerate((
        (bq_h, bq_v), (bv_h, bv_v), (b1_h, b1_v), (bcv_h, bcv_v), (ln1g_h, ln1g), (ln1b_h, ln1b),
        (ln2g_h, ln2g), (ln2b_h, ln2b), (postg_h, postg), (postb_h, postb), (bo_h, bo_v), (bfc2_h, bfc2)))]
    for cp in vec_copies:
        cp.start()
    for i in range(3):
        pltpu.make_async_copy(w_hbm[i], wfull(i, c), w_r.at[i, 0]).start()
    for late in range(2):
        pltpu.make_async_copy(xsource(c, late), xslot(c, late), x_r.at[late, 0]).start()
    for i in range(3, 6):
        pltpu.make_async_copy(w_hbm[i], wfull(i, c), w_r.at[i, 0]).start()
    wc_copies = []
    for i, src in enumerate((ck_h.at[0], ck_h.at[1], cv_h.at[0], cv_h.at[1])):
        for hf in range(2):
            cp = pltpu.make_async_copy(src.at[pl.ds(hf * 512, 512)], qkv.at[i, pl.ds(0, 512), pl.ds(hf * LOC, LOC)], c_s.at[i, hf])
            cp.start()
            wc_copies.append(cp)
    for cp in vec_copies:
        cp.wait()
    bias[c, 0:1, :] = row(bq_v)
    bias[c, 1:2, :] = row(bv_v)
    b1_row = row(b1_v)
    for q in range(4):
        bias[c, 2 + q:3 + q, :] = b1_row[:, q * LOC:(q + 1) * LOC]
    for l in range(2):
        bct[l] = jnp.transpose(jnp.broadcast_to(bcv_v[l:l + 1, :].astype(F32), (LOC, LOC)))
    send_direct(0)
    relay_x(0)
    for r, dev in enumerate((xn, yn)):
        go(bias.at[c], bias.at[c], b_s.at[r], b_r.at[r], dev)
    for i in range(1, 3):
        send_direct(i)

    send_direct(3)
    send_halves(4, 0)
    a_sends = []
    wait_x(0)
    for j in range(2):
        ln1_stage(j)
    for cp in wc_copies:
        cp.wait()
    for i in range(4):
        for hf in range(2):
            wct[i * LOC:(i + 1) * LOC, hf * 512:(hf + 1) * 512] = jnp.transpose(qkv[i, 0:512, hf * LOC:(hf + 1) * LOC])
    for r, chip in enumerate((cxn, cyn, cdg)):
        wait_recv(bias.at[chip], b_r.at[r])
        if r == 0:
            go(bias.at[cxn], bias.at[cxn], b_s.at[2], b_r.at[2], yn)
    for i in range(3):
        relay(i)
    relay(3)
    send_halves(4, 1)
    send_halves(5, 0)
    send_halves(5, 1)
    for i in range(3):
        wait_rest(i)

    def row_of(r):
        return jnp.concatenate([bias[n, r:r + 1, :] for n in range(4)], axis=1)

    lane = lax.broadcasted_iota(jnp.int32, (FRAMES, LOC), 1)

    def attention_stage(j):
        wait_recv(am.at[j, ks], am_r.at[0, j])
        bq, bv = row_of(0), row_of(1)

        def columns(i):
            return jnp.concatenate([wqkv[i, n] for n in range(4)], axis=1)

        def project(r, _):
            rows = pl.ds(r * HALF, HALF)
            a = am[j, r].reshape(HALF, D)
            qkv[0, rows, :] = ((jnp.dot(a, columns(0), preferred_element_type=F32) + bq) * ATTN_SCALE).astype(BF16)
            qkv[1, rows, :] = (jnp.dot(a, columns(1), preferred_element_type=F32) * ATTN_SCALE).astype(BF16)
            qkv[2, rows, :] = (jnp.dot(a, columns(2), preferred_element_type=F32) + bv).astype(BF16)
            return 0
        lax.fori_loop(0, 2, project, 0)

        def pair(p, _):
            cols = pl.ds(pl.multiple_of(p * LOC, LOC), LOC)
            kp, vp = qkv[1, :, cols], qkv[2, :, cols]
            zero = jnp.zeros_like(kp)
            kz[0] = jnp.where(lane < HEAD_DIM, kp, zero)
            kz[1] = jnp.where(lane < HEAD_DIM, zero, kp)
            vz[0] = jnp.where(lane < HEAD_DIM, vp, zero)
            vz[1] = jnp.where(lane < HEAD_DIM, zero, vp)

            def attend(r, _):
                rows = pl.ds(r * QROWS, QROWS)
                qb = qkv[0, rows, cols]
                out = None
                for hh in range(2):
                    s = lax.dot_general(qb, kz[hh], (((1,), (1,)), ((), ())), preferred_element_type=F32)
                    e = jnp.exp(s - jnp.max(s, axis=-1, keepdims=True))
                    prob = (e * (1.0 / jnp.sum(e, axis=-1, keepdims=True))).astype(BF16)
                    part = jnp.dot(prob, vz[hh], preferred_element_type=F32)
                    out = part if out is None else out + part
                qkv[3, rows, cols] = out.astype(BF16)
                return 0
            lax.fori_loop(0, FRAMES // QROWS, attend, 0)
            return 0
        lax.fori_loop(0, 4, pair, 0)

    own = pl.ds(k * HALF, HALF)
    oth = pl.ds(ks * HALF, HALF)

    def swap_partials(phase, j, lhs, weight):
        for n in range(2):
            cols = slice(n * 512, (n + 1) * 512)
            ex_s[j, :, cols] = jnp.dot(lhs(oth), weight[:, cols], preferred_element_type=F32).astype(BF16)
        cp = remote(ex_s.at[j], ex_r.at[j], ex_ss.at[phase, j], ex_rs.at[phase, j], sib)
        cp.start()
        for n in range(2):
            cols = slice(n * 512, (n + 1) * 512)
            acc[:, cols] = jnp.dot(lhs(own), weight[:, cols], preferred_element_type=F32)
        wait_recv(ex_r.at[j], ex_rs.at[phase, j])
        cp.wait_send()

    m_sends = []

    def output_stage(j):
        swap_partials(0, j, lambda rows: qkv[3, rows, :], wo)
        a_sends[j].wait_send()

        def body(b, _):
            rows = pl.ds(b * FR, FR)
            out = (acc[rows, :] + ex_r[j, rows, :].astype(F32) + row(bo_v)).astype(BF16)
            h = (xb[j, rows, :].astype(F32) + out.astype(F32)).astype(BF16)
            xb[j, rows, :] = h
            am[j, k, b] = ln_rows(h.astype(F32), row(ln2g), row(ln2b))
            return 0
        lax.fori_loop(0, 4, body, 0)
        cp = remote(am.at[j, k], am.at[j, k], am_s.at[1, j], am_r.at[1, j], sib)
        cp.start()
        m_sends.append(cp)

    def epiece(group, j, core, hf):
        return ea.at[3 * group + j, pl.ds(2 * hf, 2), core]

    def up_stage(j):
        wait_recv(am.at[j, ks], am_r.at[1, j])

        def up(i, _):
            n, r = i // 2, i % 2
            rows = pl.ds(r * HALF, HALF)
            b1 = jnp.concatenate([bias[n, 2 + q:3 + q, :] for q in range(4)], axis=1)
            u = jnp.dot(am[j, r].reshape(HALF, D), w1[n], preferred_element_type=F32) + b1
            act = (0.5 * u * (1.0 + lax.erf(u * (2.0 ** -0.5)))).astype(BF16)
            if j == 1:
                qkv[n, rows, :] = act
            else:
                g[n, rows, :] = act
            return 0
        lax.fori_loop(0, 8, up, 0)
        m_sends[j].wait_send()
        for peer in (sib, xn, yn):
            pl.semaphore_signal(free.at[j], inc=1, device_id={"tp": peer}, device_id_type=pl.DeviceIdType.MESH)

    def down_stage(j):
        hidden = qkv if j == 1 else g
        swap_partials(1, j, lambda rows: jnp.concatenate([hidden[n, rows, :] for n in range(4)], axis=1), w2)
        if j == 0:
            relay_x(1)

        def post(b, _):
            rows = pl.ds(b * FR, FR)
            out = (acc[rows, :] + ex_r[j, rows, :].astype(F32) + row(bfc2)).astype(BF16)
            h2 = (xb[j, rows, :].astype(F32) + out.astype(F32)).astype(BF16)
            ea[j, b, k] = ln_rows(h2.astype(F32), row(postg), row(postb))
            return 0
        lax.fori_loop(0, 4, post, 0)
        for hf in range(2):
            go(epiece(0, j, k, hf), epiece(1, j, k, hf), es_x.at[j, hf], ex_x.at[j, hf], xn)
            go(epiece(0, j, k, 1 - hf), epiece(2, j, k, 1 - hf), es_y.at[j, 1 - hf], ex_y.at[j, 1 - hf], yn)
        for hf in range(2):
            go(epiece(0, j, k, hf), epiece(0, j, k, hf), es_f.at[0, j, hf], ex_f.at[0, j, hf], sib)

    def forward(group, j, hf):
        go(epiece(group, j, k, hf), epiece(group, j, k, hf), es_f.at[group, j, hf], ex_f.at[group, j, hf], sib)

    def relay_e(j):
        pl.semaphore_wait(free.at[j], 3)
        wait_recv(epiece(1, j, k, 0), ex_x.at[j, 0])
        for b in range(2):
            go(ea.at[PER_CHIP + j, b, k], am.at[j, k, b], es_d.at[j, b], ex_d.at[j, b], yn)
        forward(1, j, 0)
        wait_recv(epiece(2, j, k, 1), ex_y.at[j, 1])
        for b in range(2, 4):
            go(ea.at[2 * PER_CHIP + j, b, k], am.at[j, k, b], es_d.at[j, b], ex_d.at[j, b], xn)
        forward(2, j, 1)
        wait_recv(epiece(1, j, k, 1), ex_x.at[j, 1])
        forward(1, j, 1)
        wait_recv(epiece(2, j, k, 0), ex_y.at[j, 0])
        forward(2, j, 0)

    def take_diagonal(j):
        for b in (0, 2, 1, 3):
            piece = am.at[j, k, b]
            wait_recv(piece, ex_d.at[j, b])
            go(piece, piece, es_g.at[j, b], ex_g.at[j, b], sib)

    def wait_diagonal(j):
        for b in range(4):
            wait_recv(am.at[j, ks, b], ex_g.at[j, b])

    def write_caches(clip, ec):
        cache_rows(clip, ec, wct, bct, kc_o, vc_o)

    def near_cache(group, j):
        chip = jnp.where(group == 0, c, jnp.where(group == 1, cxn, cyn))
        clip = chip * PER_CHIP + j
        for hf in range(2):
            wait_recv(ea.at[3 * group + j, pl.ds(2 * hf, 2), ks], ex_f.at[group, j, hf])
        enc_o[clip] = ea[3 * group + j, c, k]
        write_caches(clip, ea[3 * group + j].reshape(FRAMES, D))

    def far_cache(j):
        clip = cdg * PER_CHIP + j
        wait_diagonal(j)
        enc_o[clip] = am[j, k, c]
        write_caches(clip, natural_order(am, j))

    attention_stage(0)
    wait_rest(3)
    output_stage(0)
    attention_stage(1)
    relay(4)
    output_stage(1)
    relay(5)
    send_x(1)
    wait_rest(4)
    up_stage(0)
    up_stage(1)
    wait_rest(5)
    down_stage(0)
    down_stage(1)
    wait_x(1)
    ln1_stage(2)
    attention_stage(2)
    relay_e(0)
    output_stage(2)
    up_stage(2)
    down_stage(2)
    relay_e(1)

    def first(i, _):
        near_cache(jnp.where(i < 3, 0, 1 + (i + 1) % 2), jnp.where(i < 3, i, (i - 3) // 2))
        return 0
    lax.fori_loop(0, 7, first, 0)
    take_diagonal(0)
    far_cache(0)
    relay_e(2)

    def second(i, _):
        near_cache(1 + i, 2)
        return 0
    lax.fori_loop(0, 2, second, 0)
    take_diagonal(1)
    far_cache(1)
    take_diagonal(2)
    wait_diagonal(2)
    for cp in sends:
        cp.wait_send()


def natural_order(am, j):
    return jnp.concatenate([am[j, core, b] for b in range(4) for core in range(2)], axis=0)


def cache_rows(clip, ec, wct, bct, k_ref, v_ref):
    r = lax.dot_general(wct[...], ec, (((1,), (1,)), ((), ())), preferred_element_type=F32)
    for i in range(4):
        part = r[i * LOC:(i + 1) * LOC, :]
        if i >= 2:
            part = part + jnp.concatenate([bct[i - 2]] * 6, axis=1)
        (k_ref, v_ref)[i // 2][i % 2, clip] = part.astype(BF16)


def writer(enc_v, kc_v, vc_v, am, wct, bct, enc_o, kc_o, vc_o, kl, vl, sem, last_sem):
    t = lax.axis_index("tp")
    c, k = t // 2, t % 2
    cx, cy = c % 2, c // 2
    cdg = 2 * (1 - cy) + (1 - cx)
    last = cdg * PER_CHIP + 2

    def copies(clip):
        cps = [pltpu.make_async_copy(kc_v.at[l, clip], kc_o.at[l, clip], sem) for l in range(2)]
        cps += [pltpu.make_async_copy(vc_v.at[l, clip], vc_o.at[l, clip], sem) for l in range(2)]
        return cps + [pltpu.make_async_copy(enc_v.at[clip], enc_o.at[clip], sem)]

    def start(i, _):
        for cp in copies(lax.rem(last + 1 + i, CLIPS)):
            cp.start()
        return 0
    lax.fori_loop(0, CLIPS - 1, start, 0)
    cps = [pltpu.make_async_copy(am.at[2, k, c], enc_o.at[last], last_sem)]
    cps[0].start()
    cache_rows(0, natural_order(am, 2), wct, bct, kl, vl)
    for l in range(2):
        cps.append(pltpu.make_async_copy(kl.at[l, 0], kc_o.at[l, last], last_sem))
        cps.append(pltpu.make_async_copy(vl.at[l, 0], vc_o.at[l, last], last_sem))
    for cp in cps[1:]:
        cp.start()

    def finish(i, _):
        for cp in copies(lax.rem(last + 1 + i, CLIPS)):
            cp.wait()
        return 0
    lax.fori_loop(0, CLIPS - 1, finish, 0)
    for cp in cps:
        cp.wait()


def device_body(hidden_loc, ln1_gain, ln1_bias, w_q, b_q, w_k, w_v, b_v, w_o, b_o, ln2_gain, ln2_bias, w_fc1, b_fc1, w_fc2, b_fc2, post_gain, post_bias, w_ck, w_cv, b_cv):
    anyspec = pl.BlockSpec(memory_space=pl.ANY)
    vspec = pl.BlockSpec(memory_space=pltpu.VMEM)
    dma = pltpu.SemaphoreType.DMA
    cache = (2, CLIPS, LOC, FRAMES)
    parts = pl.pallas_call(
        kernel,
        out_shape=(
            pltpu.VMEM((CLIPS, FR, D), BF16), pltpu.VMEM(cache, BF16), pltpu.VMEM(cache, BF16),
            pltpu.VMEM((PER_CHIP, 2, 4, FR, D), BF16),
            pltpu.VMEM((4 * LOC, D), BF16),
            pltpu.VMEM((2, LOC, LOC), F32),
        ),
        in_specs=[anyspec] * 21,
        out_specs=(vspec,) * 6,
        scratch_shapes=[
            pltpu.VMEM((LOC,), BF16), pltpu.VMEM((LOC,), BF16), pltpu.VMEM((HID,), BF16), pltpu.VMEM((2, LOC), BF16),
            *([pltpu.VMEM((D,), BF16)] * 8),
            pltpu.VMEM((PER_CHIP, HALF, D), BF16),
            pltpu.VMEM((2, PER_CHIP, FR // 2, D), BF16),
            pltpu.VMEM((PER_CHIP, HALF, D), BF16),
            pltpu.VMEM((PER_CHIP, HALF, D), BF16),
            pltpu.VMEM((3, 4, D, LOC), BF16),
            pltpu.VMEM((NQ, D), BF16),
            pltpu.VMEM((4, D, HID), BF16),
            pltpu.VMEM((NH, D), BF16),
            pltpu.VMEM((4, 8, LOC), F32),
            pltpu.VMEM((4, FRAMES, NQ), BF16),
            pltpu.VMEM((2, FRAMES, LOC), BF16),
            pltpu.VMEM((2, FRAMES, LOC), BF16),
            pltpu.VMEM((4, FRAMES, HID), BF16),
            pltpu.VMEM((HALF, D), F32),
            pltpu.VMEM((9, 4, 2, FR, D), BF16),
            dma((2, 5)), dma((2, 6)), dma((2, 2)), dma((6, 7)), dma((6, 6)), dma((3,)), dma((3,)),
            dma((2, 3)), dma((2, 3)), dma((2, 3)), dma((2, 3)),
            dma((3, 2)), dma((3, 2)), dma((3, 4)), dma((3, 3, 2)), dma((3, 4)),
            dma((3, 2)), dma((3, 2)), dma((3, 4)), dma((3, 3, 2)), dma((3, 4)),
            dma((4, 2)), dma((12,)), pltpu.SemaphoreType.REGULAR((3,)),
        ],
        compiler_params=pltpu.CompilerParams(collective_id=0, has_side_effects=True, vmem_limit_bytes=48500000),
        name="encoder_layer",
    )(hidden_loc, w_q, w_k, w_v, w_o, w_fc1, w_fc2, w_ck, w_cv,
      b_q, b_v, b_fc1, b_cv, ln1_gain, ln1_bias, ln2_gain, ln2_bias, post_gain, post_bias, b_o, b_fc2)

    enc, kc, vc = pl.pallas_call(
        writer,
        out_shape=(jax.ShapeDtypeStruct((CLIPS, FR, D), BF16), jax.ShapeDtypeStruct(cache, BF16), jax.ShapeDtypeStruct(cache, BF16)),
        in_specs=[vspec] * 6,
        out_specs=(anyspec,) * 3,
        scratch_shapes=[pltpu.VMEM((2, 1, LOC, FRAMES), BF16), pltpu.VMEM((2, 1, LOC, FRAMES), BF16), dma, dma],
        compiler_params=pltpu.CompilerParams(vmem_limit_bytes=8000000),
        name="writer",
    )(*parts)

    def heads_last(cached):
        return cached.reshape(2, CLIPS, LOC // HEAD_DIM, HEAD_DIM, FRAMES).transpose(0, 1, 4, 2, 3)
    return enc, heads_last(kc), heads_last(vc)


def solution(mesh):
    in_specs = (P("dp", "tp", None), P(), P(), P(None, "tp"), P("tp"), P(None, "tp"), P(None, "tp"), P("tp"), P("tp", None), P(), P(), P(), P(None, "tp"), P("tp"), P("tp", None), P(), P(), P(), P(None, None, "tp"), P(None, None, "tp"), P(None, "tp"))
    out_specs = (P("dp", "tp", None), P(None, "dp", None, "tp", None), P(None, "dp", None, "tp", None))
    return jax.shard_map(device_body, mesh=mesh, in_specs=in_specs, out_specs=out_specs, check_vma=False)
```

```python
import functools

import jax
import jax.numpy as jnp
from jax import lax
from jax.experimental import pallas as pl
from jax.experimental.pallas import tpu as pltpu
from jax.sharding import PartitionSpec as P

HEAD_DIM = 64
ATTN_SCALE = HEAD_DIM ** -0.25
LN_EPS = 1e-5
CLIPS = 12
PER_CHIP = 3
FR = 96
HALF = 4 * FR
FRAMES = 8 * FR
D = 1024
LOC = 128
HID = 512
NQ = 4 * LOC
NH = 4 * HID
QROWS = 256
F32, BF16 = jnp.float32, jnp.bfloat16


def ln_rows(values, gain, bias):
    centered = values - jnp.mean(values, axis=-1, keepdims=True)
    row_var = jnp.mean(centered * centered, axis=-1, keepdims=True)
    return (centered * lax.rsqrt(row_var + LN_EPS) * gain + bias).astype(BF16)


def kernel(hid, wq_h, wk_h, wv_h, wo_h, w1_h, w2_h, ck_h, cv_h,
           bq_h, bv_h, b1_h, bcv_h, ln1g_h, ln1b_h, ln2g_h, ln2b_h, postg_h, postb_h, bo_h, bfc2_h,
           enc_o, kc_o, vc_o, am, wct, bct,
           bq_v, bv_v, b1_v, bcv_v, ln1g, ln1b, ln2g, ln2b, postg, postb, bo_v, bfc2, xb, xrel, ex_s, ex_r, wqkv, wo, w1, w2, bias, qkv, kz, vz, g, acc, ea,
           x_r, x_s, xrel_r, w_r, w_s, b_r, b_s, am_r, am_s, ex_rs, ex_ss, ex_x, ex_y, ex_d, ex_f, ex_g, es_x, es_y, es_d, es_f, es_g, c_s, v_s, free):
    t = lax.axis_index("tp")
    c, k = t // 2, t % 2
    cx, cy = c % 2, c // 2
    cxn = 2 * cy + (1 - cx)
    cyn = 2 * (1 - cy) + cx
    cdg = 2 * (1 - cy) + (1 - cx)
    ks = 1 - k
    sib, xn, yn = 2 * c + ks, 2 * cxn + k, 2 * cyn + k

    def remote(src, dst, ssem, rsem, dev):
        return pltpu.make_async_remote_copy(src_ref=src, dst_ref=dst, send_sem=ssem, recv_sem=rsem,
                                            device_id={"tp": dev}, device_id_type=pl.DeviceIdType.MESH)

    def wait_recv(ref, rsem):
        pltpu.make_async_copy(ref, ref, rsem).wait()

    def row(ref):
        return ref[...].astype(F32).reshape(1, ref.shape[0])

    barrier = pltpu.get_barrier_semaphore()
    for peer in (sib, xn, yn):
        pl.semaphore_signal(barrier, inc=1, device_id={"tp": peer}, device_id_type=pl.DeviceIdType.MESH)
    pl.semaphore_wait(barrier, 3)

    def xclips(late):
        return pl.ds(2, 1) if late else pl.ds(0, 2)

    def xslot(chip, late):
        return xb.at[xclips(late), pl.ds(chip * FR, FR), :]

    def xhalf(chip, late, hf):
        return xb.at[xclips(late), pl.ds(chip * FR + hf * (FR // 2), FR // 2), :]

    def xsource(chip, late):
        return hid.at[pl.ds(chip * PER_CHIP + 2, 1) if late else pl.ds(chip * PER_CHIP, 2)]

    def wfull(i, chip):
        if i < 3:
            return wqkv.at[i, chip]
        if i == 3:
            return wo.at[pl.ds(chip * LOC, LOC)]
        if i == 4:
            return w1.at[chip]
        return w2.at[pl.ds(chip * HID, HID)]

    def whalf(i, chip, hf):
        if i < 3:
            return wqkv.at[i, chip, pl.ds(hf * (D // 2), D // 2)]
        if i == 3:
            return wo.at[pl.ds(chip * LOC + hf * (LOC // 2), LOC // 2)]
        if i == 4:
            return w1.at[chip, pl.ds(hf * (D // 2), D // 2)]
        return w2.at[pl.ds(chip * HID + hf * (HID // 2), HID // 2)]

    w_hbm = (wq_h, wk_h, wv_h, wo_h, w1_h, w2_h)
    sends = []

    def go(src, dst, ssem, rsem, dev):
        cp = remote(src, dst, ssem, rsem, dev)
        cp.start()
        sends.append(cp)

    def send_direct(i):
        wait_recv(wfull(i, c), w_r.at[i, 0])
        go(wfull(i, c), wfull(i, c), w_s.at[i, 0], w_r.at[i, 1], xn)
        go(wfull(i, c), wfull(i, c), w_s.at[i, 1], w_r.at[i, 2], yn)

    def send_halves(i, part):
        if part == 0:
            wait_recv(wfull(i, c), w_r.at[i, 0])
        mine_x, mine_y = whalf(i, c, part), whalf(i, c, 1 - part)
        go(mine_x, mine_x, w_s.at[i, 4 * part], w_r.at[i, 1 + 4 * part], xn)
        go(mine_y, mine_y, w_s.at[i, 4 * part + 1], w_r.at[i, 2 + 4 * part], yn)

    def relay(i):
        wait_recv(wfull(i, cxn) if i < 4 else whalf(i, cxn, 0), w_r.at[i, 1])
        go(whalf(i, cxn, 0), whalf(i, cxn, 0), w_s.at[i, 2], w_r.at[i, 3], yn)
        wait_recv(wfull(i, cyn) if i < 4 else whalf(i, cyn, 1), w_r.at[i, 2])
        go(whalf(i, cyn, 1), whalf(i, cyn, 1), w_s.at[i, 3], w_r.at[i, 4], xn)

    def wait_rest(i):
        if i >= 4:
            wait_recv(whalf(i, cxn, 1), w_r.at[i, 5])
            wait_recv(whalf(i, cyn, 0), w_r.at[i, 6])
        wait_recv(whalf(i, cdg, 0), w_r.at[i, 3])
        wait_recv(whalf(i, cdg, 1), w_r.at[i, 4])

    def send_x(late):
        for hf, dev in enumerate((xn, yn)):
            src = xsource(cdg, late).at[:, pl.ds(hf * (FR // 2), FR // 2), :]
            go(src, xrel.at[hf, xclips(late)], x_s.at[late, hf], xrel_r.at[late, hf], dev)
        go(xsource(cxn, late), xslot(c, late), x_s.at[late, 2], x_r.at[late, 1], xn)
        go(xsource(cyn, late), xslot(c, late), x_s.at[late, 3], x_r.at[late, 2], yn)

    def relay_x(late):
        for hf, (chip, dev) in enumerate(((cxn, yn), (cyn, xn))):
            piece = xrel.at[hf, xclips(late)]
            wait_recv(piece, xrel_r.at[late, hf])
            go(piece, xhalf(chip, late, hf), x_s.at[late, 4 + hf], x_r.at[late, 3 + hf], dev)

    def ln1_stage(j):
        def body(b, _):
            vals = xb[j, pl.ds(b * FR, FR), :].astype(F32)
            am[j, k, b] = ln_rows(vals, row(ln1g), row(ln1b))
            return 0
        lax.fori_loop(0, 4, body, 0)
        cp = remote(am.at[j, k], am.at[j, k], am_s.at[0, j], am_r.at[0, j], sib)
        cp.start()
        a_sends.append(cp)

    def wait_x(late):
        for r, chip in ((0, c), (1, cxn), (2, cyn)):
            wait_recv(xslot(chip, late), x_r.at[late, r])
        for hf in range(2):
            wait_recv(xhalf(cdg, late, hf), x_r.at[late, 3 + hf])

    send_x(0)
    vec_copies = [pltpu.make_async_copy(src, dst, v_s.at[i]) for i, (src, dst) in enumerate((
        (bq_h, bq_v), (bv_h, bv_v), (b1_h, b1_v), (bcv_h, bcv_v), (ln1g_h, ln1g), (ln1b_h, ln1b),
        (ln2g_h, ln2g), (ln2b_h, ln2b), (postg_h, postg), (postb_h, postb), (bo_h, bo_v), (bfc2_h, bfc2)))]
    for cp in vec_copies:
        cp.start()
    for i in range(3):
        pltpu.make_async_copy(w_hbm[i], wfull(i, c), w_r.at[i, 0]).start()
    for late in range(2):
        pltpu.make_async_copy(xsource(c, late), xslot(c, late), x_r.at[late, 0]).start()
    for i in range(3, 6):
        pltpu.make_async_copy(w_hbm[i], wfull(i, c), w_r.at[i, 0]).start()
    wc_copies = []
    for i, src in enumerate((ck_h.at[0], ck_h.at[1], cv_h.at[0], cv_h.at[1])):
        for hf in range(2):
            cp = pltpu.make_async_copy(src.at[pl.ds(hf * 512, 512)], qkv.at[i, pl.ds(0, 512), pl.ds(hf * LOC, LOC)], c_s.at[i, hf])
            cp.start()
            wc_copies.append(cp)
    for cp in vec_copies:
        cp.wait()
    bias[c, 0:1, :] = row(bq_v)
    bias[c, 1:2, :] = row(bv_v)
    b1_row = row(b1_v)
    for q in range(4):
        bias[c, 2 + q:3 + q, :] = b1_row[:, q * LOC:(q + 1) * LOC]
    for l in range(2):
        bct[l] = jnp.transpose(jnp.broadcast_to(bcv_v[l:l + 1, :].astype(F32), (LOC, LOC)))
    send_direct(0)
    relay_x(0)
    for r, dev in enumerate((xn, yn)):
        go(bias.at[c], bias.at[c], b_s.at[r], b_r.at[r], dev)
    for i in range(1, 3):
        send_direct(i)

    send_direct(3)
    send_halves(4, 0)
    a_sends = []
    wait_x(0)
    for j in range(2):
        ln1_stage(j)
    for cp in wc_copies:
        cp.wait()
    for i in range(4):
        for hf in range(2):
            wct[i * LOC:(i + 1) * LOC, hf * 512:(hf + 1) * 512] = jnp.transpose(qkv[i, 0:512, hf * LOC:(hf + 1) * LOC])
    for r, chip in enumerate((cxn, cyn, cdg)):
        wait_recv(bias.at[chip], b_r.at[r])
        if r == 0:
            go(bias.at[cxn], bias.at[cxn], b_s.at[2], b_r.at[2], yn)
    for i in range(3):
        relay(i)
    relay(3)
    send_halves(4, 1)
    send_halves(5, 0)
    send_halves(5, 1)
    for i in range(3):
        wait_rest(i)

    def row_of(r):
        return jnp.concatenate([bias[n, r:r + 1, :] for n in range(4)], axis=1)

    lane = lax.broadcasted_iota(jnp.int32, (FRAMES, LOC), 1)

    def attention_stage(j):
        wait_recv(am.at[j, ks], am_r.at[0, j])
        bq, bv = row_of(0), row_of(1)

        def columns(i):
            return jnp.concatenate([wqkv[i, n] for n in range(4)], axis=1)

        def project(r, _):
            rows = pl.ds(r * HALF, HALF)
            a = am[j, r].reshape(HALF, D)
            qkv[0, rows, :] = ((jnp.dot(a, columns(0), preferred_element_type=F32) + bq) * ATTN_SCALE).astype(BF16)
            qkv[1, rows, :] = (jnp.dot(a, columns(1), preferred_element_type=F32) * ATTN_SCALE).astype(BF16)
            qkv[2, rows, :] = (jnp.dot(a, columns(2), preferred_element_type=F32) + bv).astype(BF16)
            return 0
        lax.fori_loop(0, 2, project, 0)

        def pair(p, _):
            cols = pl.ds(pl.multiple_of(p * LOC, LOC), LOC)
            kp, vp = qkv[1, :, cols], qkv[2, :, cols]
            zero = jnp.zeros_like(kp)
            kz[0] = jnp.where(lane < HEAD_DIM, kp, zero)
            kz[1] = jnp.where(lane < HEAD_DIM, zero, kp)
            vz[0] = jnp.where(lane < HEAD_DIM, vp, zero)
            vz[1] = jnp.where(lane < HEAD_DIM, zero, vp)

            def attend(r, _):
                rows = pl.ds(r * QROWS, QROWS)
                qb = qkv[0, rows, cols]
                out = None
                for hh in range(2):
                    s = lax.dot_general(qb, kz[hh], (((1,), (1,)), ((), ())), preferred_element_type=F32)
                    e = jnp.exp(s - jnp.max(s, axis=-1, keepdims=True))
                    prob = (e * (1.0 / jnp.sum(e, axis=-1, keepdims=True))).astype(BF16)
                    part = jnp.dot(prob, vz[hh], preferred_element_type=F32)
                    out = part if out is None else out + part
                qkv[3, rows, cols] = out.astype(BF16)
                return 0
            lax.fori_loop(0, FRAMES // QROWS, attend, 0)
            return 0
        lax.fori_loop(0, 4, pair, 0)

    own = pl.ds(k * HALF, HALF)
    oth = pl.ds(ks * HALF, HALF)

    def swap_partials(phase, j, lhs, weight):
        for n in range(2):
            cols = slice(n * 512, (n + 1) * 512)
            ex_s[j, :, cols] = jnp.dot(lhs(oth), weight[:, cols], preferred_element_type=F32).astype(BF16)
        cp = remote(ex_s.at[j], ex_r.at[j], ex_ss.at[phase, j], ex_rs.at[phase, j], sib)
        cp.start()
        for n in range(2):
            cols = slice(n * 512, (n + 1) * 512)
            acc[:, cols] = jnp.dot(lhs(own), weight[:, cols], preferred_element_type=F32)
        wait_recv(ex_r.at[j], ex_rs.at[phase, j])
        cp.wait_send()

    m_sends = []

    def output_stage(j):
        swap_partials(0, j, lambda rows: qkv[3, rows, :], wo)
        a_sends[j].wait_send()

        def body(b, _):
            rows = pl.ds(b * FR, FR)
            out = (acc[rows, :] + ex_r[j, rows, :].astype(F32) + row(bo_v)).astype(BF16)
            h = (xb[j, rows, :].astype(F32) + out.astype(F32)).astype(BF16)
            xb[j, rows, :] = h
            am[j, k, b] = ln_rows(h.astype(F32), row(ln2g), row(ln2b))
            return 0
        lax.fori_loop(0, 4, body, 0)
        cp = remote(am.at[j, k], am.at[j, k], am_s.at[1, j], am_r.at[1, j], sib)
        cp.start()
        m_sends.append(cp)

    def epiece(group, j, core, hf):
        return ea.at[3 * group + j, pl.ds(2 * hf, 2), core]

    def up_stage(j):
        wait_recv(am.at[j, ks], am_r.at[1, j])

        def up(i, _):
            n, r = i // 2, i % 2
            rows = pl.ds(r * HALF, HALF)
            b1 = jnp.concatenate([bias[n, 2 + q:3 + q, :] for q in range(4)], axis=1)
            u = jnp.dot(am[j, r].reshape(HALF, D), w1[n], preferred_element_type=F32) + b1
            act = (0.5 * u * (1.0 + lax.erf(u * (2.0 ** -0.5)))).astype(BF16)
            if j == 1:
                qkv[n, rows, :] = act
            else:
                g[n, rows, :] = act
            return 0
        lax.fori_loop(0, 8, up, 0)
        m_sends[j].wait_send()
        for peer in (sib, xn, yn):
            pl.semaphore_signal(free.at[j], inc=1, device_id={"tp": peer}, device_id_type=pl.DeviceIdType.MESH)

    def down_stage(j):
        hidden = qkv if j == 1 else g
        swap_partials(1, j, lambda rows: jnp.concatenate([hidden[n, rows, :] for n in range(4)], axis=1), w2)
        if j == 0:
            relay_x(1)

        def post(b, _):
            rows = pl.ds(b * FR, FR)
            out = (acc[rows, :] + ex_r[j, rows, :].astype(F32) + row(bfc2)).astype(BF16)
            h2 = (xb[j, rows, :].astype(F32) + out.astype(F32)).astype(BF16)
            ea[j, b, k] = ln_rows(h2.astype(F32), row(postg), row(postb))
            return 0
        lax.fori_loop(0, 4, post, 0)
        for hf in range(2):
            go(epiece(0, j, k, hf), epiece(1, j, k, hf), es_x.at[j, hf], ex_x.at[j, hf], xn)
            go(epiece(0, j, k, 1 - hf), epiece(2, j, k, 1 - hf), es_y.at[j, 1 - hf], ex_y.at[j, 1 - hf], yn)
        for hf in range(2):
            go(epiece(0, j, k, hf), epiece(0, j, k, hf), es_f.at[0, j, hf], ex_f.at[0, j, hf], sib)

    def forward(group, j, hf):
        go(epiece(group, j, k, hf), epiece(group, j, k, hf), es_f.at[group, j, hf], ex_f.at[group, j, hf], sib)

    def relay_e(j):
        pl.semaphore_wait(free.at[j], 3)
        wait_recv(epiece(1, j, k, 0), ex_x.at[j, 0])
        for b in range(2):
            go(ea.at[PER_CHIP + j, b, k], am.at[j, k, b], es_d.at[j, b], ex_d.at[j, b], yn)
        forward(1, j, 0)
        wait_recv(epiece(2, j, k, 1), ex_y.at[j, 1])
        for b in range(2, 4):
            go(ea.at[2 * PER_CHIP + j, b, k], am.at[j, k, b], es_d.at[j, b], ex_d.at[j, b], xn)
        forward(2, j, 1)
        wait_recv(epiece(1, j, k, 1), ex_x.at[j, 1])
        forward(1, j, 1)
        wait_recv(epiece(2, j, k, 0), ex_y.at[j, 0])
        forward(2, j, 0)

    def take_diagonal(j):
        for b in (0, 2, 1, 3):
            piece = am.at[j, k, b]
            wait_recv(piece, ex_d.at[j, b])
            go(piece, piece, es_g.at[j, b], ex_g.at[j, b], sib)

    def wait_diagonal(j):
        for b in range(4):
            wait_recv(am.at[j, ks, b], ex_g.at[j, b])

    def write_caches(clip, ec):
        cache_rows(clip, ec, wct, bct, kc_o, vc_o)

    def near_cache(group, j):
        chip = jnp.where(group == 0, c, jnp.where(group == 1, cxn, cyn))
        clip = chip * PER_CHIP + j
        for hf in range(2):
            wait_recv(ea.at[3 * group + j, pl.ds(2 * hf, 2), ks], ex_f.at[group, j, hf])
        enc_o[clip] = ea[3 * group + j, c, k]
        write_caches(clip, ea[3 * group + j].reshape(FRAMES, D))

    def far_cache(j):
        clip = cdg * PER_CHIP + j
        wait_diagonal(j)
        enc_o[clip] = am[j, k, c]
        write_caches(clip, natural_order(am, j))

    attention_stage(0)
    wait_rest(3)
    output_stage(0)
    attention_stage(1)
    relay(4)
    output_stage(1)
    relay(5)
    send_x(1)
    wait_rest(4)
    up_stage(0)
    up_stage(1)
    wait_rest(5)
    down_stage(0)
    down_stage(1)
    wait_x(1)
    ln1_stage(2)
    attention_stage(2)
    relay_e(0)
    output_stage(2)
    up_stage(2)
    down_stage(2)
    relay_e(1)

    def first(i, _):
        near_cache(jnp.where(i < 3, 0, 1 + (i + 1) % 2), jnp.where(i < 3, i, (i - 3) // 2))
        return 0
    lax.fori_loop(0, 7, first, 0)
    relay_e(2)
    take_diagonal(0)
    far_cache(0)

    def second(i, _):
        near_cache(1 + i, 2)
        return 0
    lax.fori_loop(0, 2, second, 0)
    take_diagonal(1)
    take_diagonal(2)
    far_cache(1)
    wait_diagonal(2)
    for cp in sends:
        cp.wait_send()


def natural_order(am, j):
    return jnp.concatenate([am[j, core, b] for b in range(4) for core in range(2)], axis=0)


def cache_rows(clip, ec, wct, bct, k_ref, v_ref):
    r = lax.dot_general(wct[...], ec, (((1,), (1,)), ((), ())), preferred_element_type=F32)
    for i in range(4):
        part = r[i * LOC:(i + 1) * LOC, :]
        if i >= 2:
            part = part + jnp.concatenate([bct[i - 2]] * 6, axis=1)
        (k_ref, v_ref)[i // 2][i % 2, clip] = part.astype(BF16)


def writer(enc_v, kc_v, vc_v, am, wct, bct, enc_o, kc_o, vc_o, kl, vl, sem, last_sem):
    t = lax.axis_index("tp")
    c, k = t // 2, t % 2
    cx, cy = c % 2, c // 2
    cdg = 2 * (1 - cy) + (1 - cx)
    last = cdg * PER_CHIP + 2

    def copies(clip):
        cps = [pltpu.make_async_copy(kc_v.at[l, clip], kc_o.at[l, clip], sem) for l in range(2)]
        cps += [pltpu.make_async_copy(vc_v.at[l, clip], vc_o.at[l, clip], sem) for l in range(2)]
        return cps + [pltpu.make_async_copy(enc_v.at[clip], enc_o.at[clip], sem)]

    def start(i, _):
        for cp in copies(lax.rem(last + 1 + i, CLIPS)):
            cp.start()
        return 0
    lax.fori_loop(0, CLIPS - 1, start, 0)
    cps = [pltpu.make_async_copy(am.at[2, k, c], enc_o.at[last], last_sem)]
    cps[0].start()
    cache_rows(0, natural_order(am, 2), wct, bct, kl, vl)
    for l in range(2):
        cps.append(pltpu.make_async_copy(kl.at[l, 0], kc_o.at[l, last], last_sem))
        cps.append(pltpu.make_async_copy(vl.at[l, 0], vc_o.at[l, last], last_sem))
    for cp in cps[1:]:
        cp.start()

    def finish(i, _):
        for cp in copies(lax.rem(last + 1 + i, CLIPS)):
            cp.wait()
        return 0
    lax.fori_loop(0, CLIPS - 1, finish, 0)
    for cp in cps:
        cp.wait()


def device_body(hidden_loc, ln1_gain, ln1_bias, w_q, b_q, w_k, w_v, b_v, w_o, b_o, ln2_gain, ln2_bias, w_fc1, b_fc1, w_fc2, b_fc2, post_gain, post_bias, w_ck, w_cv, b_cv):
    anyspec = pl.BlockSpec(memory_space=pl.ANY)
    vspec = pl.BlockSpec(memory_space=pltpu.VMEM)
    dma = pltpu.SemaphoreType.DMA
    cache = (2, CLIPS, LOC, FRAMES)
    parts = pl.pallas_call(
        kernel,
        out_shape=(
            pltpu.VMEM((CLIPS, FR, D), BF16), pltpu.VMEM(cache, BF16), pltpu.VMEM(cache, BF16),
            pltpu.VMEM((PER_CHIP, 2, 4, FR, D), BF16),
            pltpu.VMEM((4 * LOC, D), BF16),
            pltpu.VMEM((2, LOC, LOC), F32),
        ),
        in_specs=[anyspec] * 21,
        out_specs=(vspec,) * 6,
        scratch_shapes=[
            pltpu.VMEM((LOC,), BF16), pltpu.VMEM((LOC,), BF16), pltpu.VMEM((HID,), BF16), pltpu.VMEM((2, LOC), BF16),
            *([pltpu.VMEM((D,), BF16)] * 8),
            pltpu.VMEM((PER_CHIP, HALF, D), BF16),
            pltpu.VMEM((2, PER_CHIP, FR // 2, D), BF16),
            pltpu.VMEM((PER_CHIP, HALF, D), BF16),
            pltpu.VMEM((PER_CHIP, HALF, D), BF16),
            pltpu.VMEM((3, 4, D, LOC), BF16),
            pltpu.VMEM((NQ, D), BF16),
            pltpu.VMEM((4, D, HID), BF16),
            pltpu.VMEM((NH, D), BF16),
            pltpu.VMEM((4, 8, LOC), F32),
            pltpu.VMEM((4, FRAMES, NQ), BF16),
            pltpu.VMEM((2, FRAMES, LOC), BF16),
            pltpu.VMEM((2, FRAMES, LOC), BF16),
            pltpu.VMEM((4, FRAMES, HID), BF16),
            pltpu.VMEM((HALF, D), F32),
            pltpu.VMEM((9, 4, 2, FR, D), BF16),
            dma((2, 5)), dma((2, 6)), dma((2, 2)), dma((6, 7)), dma((6, 6)), dma((3,)), dma((3,)),
            dma((2, 3)), dma((2, 3)), dma((2, 3)), dma((2, 3)),
            dma((3, 2)), dma((3, 2)), dma((3, 4)), dma((3, 3, 2)), dma((3, 4)),
            dma((3, 2)), dma((3, 2)), dma((3, 4)), dma((3, 3, 2)), dma((3, 4)),
            dma((4, 2)), dma((12,)), pltpu.SemaphoreType.REGULAR((3,)),
        ],
        compiler_params=pltpu.CompilerParams(collective_id=0, has_side_effects=True, vmem_limit_bytes=48500000),
        name="encoder_layer",
    )(hidden_loc, w_q, w_k, w_v, w_o, w_fc1, w_fc2, w_ck, w_cv,
      b_q, b_v, b_fc1, b_cv, ln1_gain, ln1_bias, ln2_gain, ln2_bias, post_gain, post_bias, b_o, b_fc2)

    enc, kc, vc = pl.pallas_call(
        writer,
        out_shape=(jax.ShapeDtypeStruct((CLIPS, FR, D), BF16), jax.ShapeDtypeStruct(cache, BF16), jax.ShapeDtypeStruct(cache, BF16)),
        in_specs=[vspec] * 6,
        out_specs=(anyspec,) * 3,
        scratch_shapes=[pltpu.VMEM((2, 1, LOC, FRAMES), BF16), pltpu.VMEM((2, 1, LOC, FRAMES), BF16), dma, dma],
        compiler_params=pltpu.CompilerParams(vmem_limit_bytes=8000000),
        name="writer",
    )(*parts)

    def heads_last(cached):
        return cached.reshape(2, CLIPS, LOC // HEAD_DIM, HEAD_DIM, FRAMES).transpose(0, 1, 4, 2, 3)
    return enc, heads_last(kc), heads_last(vc)


def solution(mesh):
    in_specs = (P("dp", "tp", None), P(), P(), P(None, "tp"), P("tp"), P(None, "tp"), P(None, "tp"), P("tp"), P("tp", None), P(), P(), P(), P(None, "tp"), P("tp"), P("tp", None), P(), P(), P(), P(None, None, "tp"), P(None, None, "tp"), P(None, "tp"))
    out_specs = (P("dp", "tp", None), P(None, "dp", None, "tp", None), P(None, "dp", None, "tp", None))
    return jax.shard_map(device_body, mesh=mesh, in_specs=in_specs, out_specs=out_specs, check_vma=False)
```
